16 devices in a mesh: col: 2 (over z), row: 8 (over y, x, core).
Axes of the slice: x: 2, y: 2, z: 2, core: 2. Of those that a mesh axis runs over, the one named last changes fastest.
Arguments:
- vel_u: float32 [20, 1024, 1024], P(None, 'row', 'col')
- vel_v: float32 [20, 1024, 1024], P(None, 'row', 'col')
- temperature: float32 [20, 1024, 1024], P(None, 'row', 'col')
- salinity: float32 [20, 1024, 1024], P(None, 'row', 'col')
- sea_level: float32 [1024, 1024], P('row', 'col')
- trans_u: float32 [1024, 1024], P('row', 'col')
- trans_v: float32 [1024, 1024], P('row', 'col')
- bathymetry: float32 [1024, 1024], P('row', 'col')
- kmt_levels: int32 [1024, 1024], P('row', 'col')
- tide_force: float32 [20, 2], replicated
Outputs:
- output 1: float32 [1024, 1024], P('row', 'col')
- output 2: float32 [1024, 1024], P('row', 'col')
- output 3: float32 [1024, 1024], P('row', 'col')
- output 4: float32 [20, 1024, 1024], P(None, 'row', 'col')
- output 5: float32 [20, 1024, 1024], P(None, 'row', 'col')
- output 6: float32 [20, 1024, 1024], P(None, 'row', 'col')
- output 7: float32 [20, 1024, 1024], P(None, 'row', 'col')
All inputs are finite; a program needn't handle non-finite values.
Results may differ from the reference program's by a relative error of at most 0.001.
Values sent between devices are 32-bit elements.
A program may use at most 1 GiB of HBM per device.

```python
import jax
import jax.numpy as jnp
from jax import lax

LEVELS = 20
SUBCYCLES = 20
GRID_NY = 1024
GRID_NX = 1024

GRAVITY = 1.0
GRID_DX = 1.0
TIME_STEP = 4.0
ALPHA_T = 0.02
BETA_S = 0.015
T_REF = 1.0
S_REF = 1.0
VISC_KV = 0.001
DIFF_KT = 0.0005


def pad_halo(field):
    wrapped = jnp.concatenate([field[..., -1:], field, field[..., :1]], axis=-1)
    walls = jnp.zeros_like(wrapped[..., :1, :])
    return jnp.concatenate([walls, wrapped, walls], axis=-2)


def level_mask(count, n_levels):
    levels = jnp.arange(n_levels, dtype=jnp.int32)[:, None, None]
    return (levels < count[None]).astype(jnp.float32)


def interface_coef(count, thick, kappa, n_levels):
    levels = jnp.arange(n_levels - 1, dtype=jnp.int32)[:, None, None]
    active = (levels + 1 < count[None]).astype(jnp.float32)
    safe = jnp.where(count > 0, thick, 1.0)
    return active * (TIME_STEP * kappa / (safe * safe))[None]


def column_solve(source, couple):
    edge = jnp.zeros_like(source[:1])
    upper = jnp.concatenate([couple, edge], axis=0)
    lower = jnp.concatenate([edge, couple], axis=0)
    diag = 1.0 + upper + lower

    def forward(carry, slab):
        gain_prev, part_prev = carry
        lower_k, diag_k, upper_k, source_k = slab
        pivot = diag_k - lower_k * gain_prev
        gain = upper_k / pivot
        part = (source_k + lower_k * part_prev) / pivot
        return (gain, part), (gain, part)

    start = (jnp.zeros_like(source[0]), jnp.zeros_like(source[0]))
    _, (gains, parts) = lax.scan(forward, start, (lower, diag, upper, source))

    def backward(below, slab):
        gain, part = slab
        here = part + gain * below
        return here, here

    _, profile = lax.scan(backward, jnp.zeros_like(source[0]), (gains, parts), reverse=True)
    return profile


def geometry(kmt_ext, depth_ext):
    kmt_cell = kmt_ext[1:-1, 1:-1]
    thick_ext = depth_ext / jnp.maximum(kmt_ext, 1).astype(jnp.float32)
    thick_cell = thick_ext[1:-1, 1:-1]
    return {"k_cell": kmt_cell, "k_u": jnp.minimum(kmt_cell, kmt_ext[1:-1, 2:]), "k_v": jnp.minimum(kmt_cell, kmt_ext[2:, 1:-1]), "dz_cell": thick_cell, "dz_u": 0.5 * (thick_cell + thick_ext[1:-1, 2:]), "dz_v": 0.5 * (thick_cell + thick_ext[2:, 1:-1])}


def surface_fields(layout):
    k_faces = jnp.stack([layout["k_u"], layout["k_v"]])
    face_depth = k_faces.astype(jnp.float32) * jnp.stack([layout["dz_u"], layout["dz_v"]])
    face_wet = (k_faces > 0).astype(jnp.float32)
    wet_cell = (layout["k_cell"] > 0).astype(jnp.float32)
    return face_depth, face_wet, wet_cell


def momentum_tend(u_ext, v_ext, p_ext):
    cen_u = 0.5 * (u_ext[:, 1:-1, :-1] + u_ext[:, 1:-1, 1:])
    corner_v = 0.5 * (v_ext[:, :-1, 1:-1] + v_ext[:, :-1, 2:])
    corner_u = 0.5 * (u_ext[:, :-1, 1:-1] + u_ext[:, 1:, 1:-1])
    flux_uu = cen_u * cen_u
    flux_vu = corner_v * corner_u
    tend_u = -(flux_uu[:, :, 1:] - flux_uu[:, :, :-1] + flux_vu[:, 1:, :] - flux_vu[:, :-1, :] + p_ext[:, 1:-1, 2:] - p_ext[:, 1:-1, 1:-1]) / GRID_DX
    cen_v = 0.5 * (v_ext[:, :-1, 1:-1] + v_ext[:, 1:, 1:-1])
    side_u = 0.5 * (u_ext[:, 1:-1, :-1] + u_ext[:, 2:, :-1])
    side_v = 0.5 * (v_ext[:, 1:-1, :-1] + v_ext[:, 1:-1, 1:])
    flux_vv = cen_v * cen_v
    flux_uv = side_u * side_v
    tend_v = -(flux_vv[:, 1:, :] - flux_vv[:, :-1, :] + flux_uv[:, :, 1:] - flux_uv[:, :, :-1] + p_ext[:, 2:, 1:-1] - p_ext[:, 1:-1, 1:-1]) / GRID_DX
    return tend_u, tend_v


def baroclinic_predict(vel_u, vel_v, temperature, salinity, layout, halo_fn):
    n_levels = vel_u.shape[0]
    mask_c = level_mask(layout["k_cell"], n_levels)
    mask_u = level_mask(layout["k_u"], n_levels)
    mask_v = level_mask(layout["k_v"], n_levels)
    vel_um = vel_u * mask_u
    vel_vm = vel_v * mask_v
    density = mask_c * (BETA_S * (salinity - S_REF) - ALPHA_T * (temperature - T_REF))
    pressure = GRAVITY * layout["dz_cell"] * (jnp.cumsum(density, axis=0) - 0.5 * density)
    cell_coef = interface_coef(layout["k_cell"], layout["dz_cell"], DIFF_KT, n_levels)
    temp_mix = column_solve(temperature * mask_c, cell_coef)
    salt_mix = column_solve(salinity * mask_c, cell_coef)
    edges = halo_fn(jnp.stack([vel_um, vel_vm, pressure, temp_mix, salt_mix]))
    tend_u, tend_v = momentum_tend(edges[0], edges[1], edges[2])
    u_star = column_solve(mask_u * (vel_um + TIME_STEP * tend_u), interface_coef(layout["k_u"], layout["dz_u"], VISC_KV, n_levels))
    v_star = column_solve(mask_v * (vel_vm + TIME_STEP * tend_v), interface_coef(layout["k_v"], layout["dz_v"], VISC_KV, n_levels))
    forcing = jnp.stack([jnp.sum(layout["dz_u"] * (u_star - vel_um), axis=0), jnp.sum(layout["dz_v"] * (v_star - vel_vm), axis=0)]) / TIME_STEP
    return u_star, v_star, forcing, edges[3:], (mask_c, mask_u, mask_v)


def barotropic(eta_start, trans_start, face_depth, face_wet, wet_cell, forcing, tide_force, halo_fn):
    n_sub = tide_force.shape[0]
    dt_sub = TIME_STEP / n_sub
    weight_norm = 6.0 / (n_sub * (n_sub + 1) * (n_sub + 2))

    def substep(step, carry):
        eta_now, trans_now, trans_avg = carry
        trans_ext = halo_fn(trans_now)
        divergence = (trans_now[0] - trans_ext[0, 1:-1, :-2] + trans_now[1] - trans_ext[1, :-2, 1:-1]) / GRID_DX
        eta_next = wet_cell * (eta_now - dt_sub * divergence)
        eta_ext = halo_fn(eta_next)
        slope = jnp.stack([eta_ext[1:-1, 2:] - eta_next, eta_ext[2:, 1:-1] - eta_next]) / GRID_DX
        tide_now = lax.dynamic_index_in_dim(tide_force, step, 0, keepdims=False)
        trans_next = face_wet * (trans_now + dt_sub * (face_depth * (tide_now[:, None, None] - GRAVITY * slope) + forcing))
        weight = weight_norm * ((step + 1) * (n_sub - step)).astype(jnp.float32)
        return eta_next, trans_next, trans_avg + weight * trans_next

    return lax.fori_loop(0, n_sub, substep, (eta_start, trans_start, jnp.zeros_like(trans_start)))


def correct_velocity(star, dz_face, depth_face, mean_trans, mask):
    safe = jnp.where(depth_face > 0, depth_face, 1.0)
    return mask * (star + ((mean_trans - jnp.sum(dz_face * star, axis=0)) / safe)[None])


def advect_tracers(tracer_ext, flow_ext, mask_c):
    flux_x = flow_ext[0, :, 1:-1, :-1] * (0.5 * (tracer_ext[..., 1:-1, :-1] + tracer_ext[..., 1:-1, 1:]))
    flux_y = flow_ext[1, :, :-1, 1:-1] * (0.5 * (tracer_ext[..., :-1, 1:-1] + tracer_ext[..., 1:, 1:-1]))
    divergence = (flux_x[..., 1:] - flux_x[..., :-1] + flux_y[..., 1:, :] - flux_y[..., :-1, :]) / GRID_DX
    return mask_c * (tracer_ext[..., 1:-1, 1:-1] - TIME_STEP * divergence)


def baroclinic_finish(u_star, v_star, trans_avg, face_depth, layout, tracer_ext, masks, halo_fn):
    mask_c, mask_u, mask_v = masks
    vel_uc = correct_velocity(u_star, layout["dz_u"], face_depth[0], trans_avg[0], mask_u)
    vel_vc = correct_velocity(v_star, layout["dz_v"], face_depth[1], trans_avg[1], mask_v)
    flows = halo_fn(jnp.stack([vel_uc, vel_vc]))
    tracers = advect_tracers(tracer_ext, flows, mask_c)
    return vel_uc, vel_vc, tracers[0], tracers[1]


def ocean_step(vel_u, vel_v, temperature, salinity, sea_level, trans_u, trans_v, bathymetry, kmt_levels, tide_force, halo_fn):
    layout = geometry(halo_fn(kmt_levels), halo_fn(bathymetry))
    u_star, v_star, forcing, tracer_ext, masks = baroclinic_predict(vel_u, vel_v, temperature, salinity, layout, halo_fn)
    face_depth, face_wet, wet_cell = surface_fields(layout)
    eta_new, trans_new, trans_avg = barotropic(wet_cell * sea_level, face_wet * jnp.stack([trans_u, trans_v]), face_depth, face_wet, wet_cell, forcing, tide_force, halo_fn)
    vel_uc, vel_vc, temp_new, salt_new = baroclinic_finish(u_star, v_star, trans_avg, face_depth, layout, tracer_ext, masks, halo_fn)
    return eta_new, trans_new[0], trans_new[1], vel_uc, vel_vc, temp_new, salt_new


def draw_levels(key):
    key_count, key_land = jax.random.split(key)
    counts = jax.random.randint(key_count, (GRID_NY, GRID_NX), (LEVELS + 2) // 3, LEVELS + 1)
    land = jax.random.randint(key_land, (GRID_NY, GRID_NX), 0, 12) == 0
    levels = jnp.where(land, 0, counts).astype(jnp.int32)
    return levels.at[0, 0].set(0).at[GRID_NY - 1, GRID_NX - 1].set(LEVELS)


def setup_inputs(seed: int = 0) -> dict:
    keys = jax.random.split(jax.random.key(seed), 10)
    shape_cube = (LEVELS, GRID_NY, GRID_NX)
    shape_plane = (GRID_NY, GRID_NX)
    depth_frac = jnp.arange(LEVELS, dtype=jnp.float32)[:, None, None] / LEVELS
    return {
        "vel_u": 0.1 * jax.random.normal(keys[0], shape_cube, jnp.float32),
        "vel_v": 0.1 * jax.random.normal(keys[1], shape_cube, jnp.float32),
        "temperature": 2.0 * (1.0 - depth_frac) + 0.5 * jax.random.normal(keys[2], shape_cube, jnp.float32),
        "salinity": 1.0 + depth_frac + 0.3 * jax.random.normal(keys[3], shape_cube, jnp.float32),
        "sea_level": 0.05 * jax.random.normal(keys[4], shape_plane, jnp.float32),
        "trans_u": 0.05 * jax.random.normal(keys[5], shape_plane, jnp.float32),
        "trans_v": 0.05 * jax.random.normal(keys[6], shape_plane, jnp.float32),
        "bathymetry": 0.6 + 0.8 * jax.random.uniform(keys[7], shape_plane, jnp.float32),
        "kmt_levels": draw_levels(keys[8]),
        "tide_force": 0.01 + 0.01 * jax.random.normal(keys[9], (SUBCYCLES, 2), jnp.float32),
    }


def reference(vel_u, vel_v, temperature, salinity, sea_level, trans_u, trans_v, bathymetry, kmt_levels, tide_force):
    return ocean_step(vel_u, vel_v, temperature, salinity, sea_level, trans_u, trans_v, bathymetry, kmt_levels, tide_force, pad_halo)
```

```python
import functools

import jax
import jax.numpy as jnp
from jax import lax
from jax.experimental import pallas as pl
from jax.experimental.pallas import tpu as pltpu
from jax.sharding import PartitionSpec as P

TIME_STEP = 4.0
ALPHA_T = 0.02
BETA_S = 0.015
VISC_KV = 0.001
DIFF_KT = 0.0005

NL = 20
NSUB = 20
NR, NC = 128, 512
HR = 24
ER, EC = NR + 2 * HR, NC + 128
NCH = 4
CH = NR // NCH
DTB = TIME_STEP / NSUB
F32 = jnp.float32
ZERO = 0.0
BODY = slice(0, NC)
LEFT = slice(0, 128)
RIGHT = slice(NC - 128, NC)
GHOST = slice(NC, EC)
KMT, DZ, ETA, TU, TV, FX, FY, SV, SU = range(9)
WIDE = 42
MESH = pl.DeviceIdType.MESH


def rows(r, off=0):
    start = 8 * r + off
    if isinstance(start, int):
        return pl.ds(start, 8)
    return pl.ds(pl.multiple_of(start, 8), 8)


def iota(shape, axis):
    return lax.broadcasted_iota(jnp.int32, shape, axis)


def east(x):
    return pltpu.roll(x, x.shape[1] - 1, 1)


def west(x):
    return pltpu.roll(x, 1, 1)


def north(here, above):
    return pltpu.roll(jnp.where(iota(here.shape, 0) == 0, above, here), 7, 0)


def south(here, below):
    return pltpu.roll(jnp.where(iota(here.shape, 0) == 7, below, here), 1, 0)


def lane_of(slot, k):
    return 2 * k + 40 * slot


def unpack(ghost, slot, k):
    shift = (128 - lane_of(slot, k)) % 128
    return pltpu.roll(ghost, shift, 1) if shift else ghost


def pack(tiles):
    lane = iota((8, 128), 1)
    acc = None
    first = None
    for slot, k, low, high in tiles:
        both = jnp.where(lane == 127, high, low)
        at = lane_of(slot, k)
        moved = pltpu.roll(both, at, 1) if at else both
        if acc is None:
            acc = moved
            if at == 0:
                first = moved
        else:
            acc = jnp.where(lane >= at - 1, moved, acc)
    if first is not None:
        acc = jnp.where(lane == 127, first, acc)
    return acc


def pack_wide(planes):
    lane = iota((8, 128), 1)
    acc = None
    for q, x in enumerate(planes):
        edge = jnp.where(lane < 64, x[:, LEFT], x[:, RIGHT])
        if acc is None:
            acc = edge
        else:
            acc = jnp.where(lane >= WIDE * q - WIDE // 2, pltpu.roll(edge, WIDE * q, 1), acc)
    if len(planes) == 1:
        return acc
    first = jnp.where(lane < 64, planes[0][:, LEFT], planes[0][:, RIGHT])
    return jnp.where(lane >= 128 - WIDE // 2, first, acc)


def unpack_wide(tile, q):
    lane = iota((8, 128), 1)
    moved = pltpu.roll(tile, 128 - WIDE * q, 1) if q else tile
    return jnp.where((lane < WIDE // 2) | (lane >= 128 - WIDE // 2), moved, ZERO)


def solve(refs, masked, count, coef, gains, at):
    low = gain = None
    parts = [None] * len(refs)
    for k in range(NL):
        up = jnp.where(count > k + 1.0, coef, ZERO) if k < NL - 1 else None
        if k == 0:
            pivot = 1.0 + up
        elif k < NL - 1:
            pivot = (1.0 + up) + low * (1.0 - gain)
        else:
            pivot = 1.0 + low * (1.0 - gain)
        inv = 1.0 / pivot
        for i, ref in enumerate(refs):
            src = ref[k, at, :]
            if not masked:
                src = jnp.where(count > k, src, ZERO)
            parts[i] = src * inv if k == 0 else (src + low * parts[i]) * inv
            if k < NL - 1:
                ref[k, at, :] = parts[i]
        if k < NL - 1:
            gain = up * inv
            gains[k] = gain
        low = up
    for i, ref in enumerate(refs):
        ref[NL - 1, at, :] = parts[i]
    for k in range(NL - 2, -1, -1):
        gain = gains[k]
        for i, ref in enumerate(refs):
            parts[i] = ref[k, at, :] + gain * parts[i]
            ref[k, at, :] = parts[i]


def predict_kernel(
    u_h, v_h, t_h, s_h, eta_h, tu_h, tv_h, dep_h, kmt_h,
    su_o, sv_o, tm_o, sm_o, ext_o, gts_o, gu_o, grts_o, grtn_o, grv_o,
    ub, vb, pb, tb, sb, su, sv, ext, ktmp, htmp, pa, pb_, pc, ga, gb, gc, ug, vg, pg, dup, sp, gx, prn, prs, grs, grn, sts, trn, trs, sug, vrn, fp, gains, gains2,
    load_sem, small_sem, out_sem, outs_sem, send_sem, recv_sem,
):
    col = lax.axis_index("col")
    row = lax.axis_index("row")
    n_row = 8
    side = 1 - col
    up_row = lax.rem(row + 1, n_row)
    down_row = lax.rem(row + n_row - 1, n_row)
    to_x = {"col": side, "row": row}
    to_n = {"col": col, "row": up_row}
    to_s = {"col": col, "row": down_row}
    to_dn = {"col": side, "row": up_row}
    to_ds = {"col": side, "row": down_row}

    barrier = pltpu.get_barrier_semaphore()
    for dev in (to_x, to_n, to_s, to_dn, to_ds):
        pl.semaphore_signal(barrier, inc=1, device_id=dev, device_id_type=MESH)

    small = [
        pltpu.make_async_copy(kmt_h, ktmp, small_sem.at[0]),
        pltpu.make_async_copy(dep_h, htmp, small_sem.at[1]),
        pltpu.make_async_copy(eta_h, ext.at[2, pl.ds(HR, NR), pl.ds(0, NC)], small_sem.at[2]),
        pltpu.make_async_copy(tu_h, ext.at[3, pl.ds(HR, NR), pl.ds(0, NC)], small_sem.at[3]),
        pltpu.make_async_copy(tv_h, ext.at[4, pl.ds(HR, NR), pl.ds(0, NC)], small_sem.at[4]),
    ]
    for c in small:
        c.start()

    def load(i, c):
        src = (t_h, s_h, u_h, v_h)[i]
        dst = (tb, sb, ub, vb)[i]
        at = pl.ds(pl.multiple_of(c * CH, CH), CH)
        to = pl.ds(pl.multiple_of(c * CH + (8 if i >= 2 else 0), 8), CH)
        return pltpu.make_async_copy(src.at[:, at, :], dst.at[:, to, :], load_sem.at[i, c])

    def start_loads(pair):
        def body(c, _):
            for i in pair:
                load(i, c).start()
            return 0

        lax.fori_loop(0, NCH, body, 0)

    start_loads((0, 1))
    start_loads((2, 3))

    def send(src, dst, idx, dev):
        c = pltpu.make_async_remote_copy(
            src_ref=src, dst_ref=dst, send_sem=send_sem.at[idx], recv_sem=recv_sem.at[idx], device_id=dev, device_id_type=MESH
        )
        c.start()
        return c

    for c in small:
        c.wait()
    def stage(r, _):
        kf = ktmp[rows(r), :].astype(F32)
        dz = htmp[rows(r), :] / jnp.maximum(kf, 1.0)
        ext[KMT, rows(r, HR), BODY] = kf
        ext[DZ, rows(r, HR), BODY] = dz
        eta, tu, tv = (ext[f, rows(r, HR), BODY] for f in (ETA, TU, TV))
        pa[rows(r), :] = pack_wide((kf, dz, eta))
        pb_[rows(r), :] = pack_wide((tu, tv))
        return 0

    lax.fori_loop(0, NR // 8, stage, 0)
    pl.semaphore_wait(barrier, 5)

    def send_ext(lo, n, tile, ghost, base):
        at = pl.ds(lo, n)
        low, high, mid = pl.ds(0, HR), pl.ds(HR + NR, HR), pl.ds(HR, NR)
        body = pl.ds(0, NC)
        return [
            send(tile, ghost.at[mid, :], base, to_x),
            send(ext.at[at, pl.ds(NR, HR), body], ext.at[at, low, body], base + 1, to_n),
            send(ext.at[at, pl.ds(HR, HR), body], ext.at[at, high, body], base + 2, to_s),
            send(tile.at[pl.ds(NR - HR, HR), :], ghost.at[low, :], base + 3, to_dn),
            send(tile.at[low, :], ghost.at[high, :], base + 4, to_ds),
        ]

    def receive_ext(copies, ghost, fields):
        for c in copies:
            c.wait()

        def body(t, _):
            g = ghost[rows(t), :]
            for q, f in enumerate(fields):
                ext[f, rows(t), GHOST] = unpack_wide(g, q)
            return 0

        lax.fori_loop(0, ER // 8, body, 0)

    first = send_ext(KMT, 3, pa, ga, 0)
    later = send_ext(TU, 2, pb_, gb, 5)

    def pressure(r, _):
        kc = ext[KMT, rows(r, HR), BODY]
        dz = ext[DZ, rows(r, HR), BODY]
        total = jnp.zeros((8, NC), F32)
        for k in range(NL):
            dens = BETA_S * (sb[k, rows(r), :] - 1.0) - ALPHA_T * (tb[k, rows(r), :] - 1.0)
            dens = jnp.where(kc > k, dens, ZERO)
            total = total + dens
            pb[k, rows(r, 8), :] = dz * (total - 0.5 * dens)
        return 0

    def pressure_chunk(c, _):
        load(0, c).wait()
        load(1, c).wait()
        lax.fori_loop(c * (CH // 8), (c + 1) * (CH // 8), pressure, 0)
        return 0

    lax.fori_loop(0, NCH, pressure_chunk, 0)

    receive_ext(first, ga, (KMT, DZ, ETA))
    has_south = (row > 0).astype(F32)
    has_north = (row < n_row - 1).astype(F32)
    ext[KMT, 0:HR, :] = ext[KMT, 0:HR, :] * has_south
    ext[KMT, HR + NR :, :] = ext[KMT, HR + NR :, :] * has_north

    def count_u(r):
        kc = ext[KMT, rows(r, HR), :]
        return jnp.minimum(kc, east(kc))[:, BODY]

    def count_v(r):
        kc = ext[KMT, rows(r, HR), BODY]
        return jnp.minimum(kc, north(kc, ext[KMT, rows(r, HR + 8), BODY]))

    def mask_pack(r, _):
        counts = (count_u(r), count_v(r))
        tiles = []
        for slot, ref in enumerate((ub, vb, pb)):
            for k in range(NL):
                x = ref[k, rows(r, 8), :]
                if slot < 2:
                    x = jnp.where(counts[slot] > k, x, ZERO)
                    ref[k, rows(r, 8), :] = x
                tiles.append((slot, k, x[:, LEFT], x[:, RIGHT]))
        sp[rows(r), :] = pack(tiles)
        return 0

    def mask_chunk(c, _):
        load(2, c).wait()
        load(3, c).wait()
        lax.fori_loop(c * (CH // 8), (c + 1) * (CH // 8), mask_pack, 0)
        return 0

    lax.fori_loop(0, NCH, mask_chunk, 0)

    def edge_row(dst, i, k, ref, at):
        dst[24 * i + k : 24 * i + k + 1, :] = ref[k, at : at + 1, :]

    def ghost_row(ref, k, at, src, i):
        ref[k, at : at + 1, :] = src[24 * i + k : 24 * i + k + 1, :]

    for k in range(NL):
        for i, ref in enumerate((ub, vb, pb)):
            edge_row(prs, i, k, ref, 8)
        for i, ref in enumerate((ub, vb)):
            edge_row(prn, i, k, ref, NR + 7)
    second = [
        send(sp, gx.at[pl.ds(8, NR), :], 10, to_x),
        send(prn, grs, 11, to_n),
        send(prs, grn, 12, to_s),
        send(sp.at[pl.ds(NR - 8, 8), :], gx.at[pl.ds(0, 8), :], 13, to_dn),
        send(sp.at[pl.ds(0, 8), :], gx.at[pl.ds(NR + 8, 8), :], 14, to_ds),
    ]

    def out_copy(i, c):
        src = (tb, sb, su, sv)[i]
        dst = (tm_o, sm_o, su_o, sv_o)[i]
        at = pl.ds(pl.multiple_of(c * CH, CH), CH)
        return pltpu.make_async_copy(src.at[:, at, :], dst.at[:, at, :], out_sem.at[i, c])

    def mix(r, _):
        kc = ext[KMT, rows(r, HR), BODY]
        dz = ext[DZ, rows(r, HR), BODY]
        solve((tb, sb), False, kc, (TIME_STEP * DIFF_KT) / (dz * dz), gains, rows(r))
        tiles = []
        for slot, ref in enumerate((tb, sb)):
            for k in range(NL):
                tiles.append((slot, k, ref[k, rows(r), LEFT], ref[k, rows(r), RIGHT]))
        sts[rows(r), :] = pack(tiles)
        return 0

    def mix_chunk(c, _):
        lax.fori_loop(c * (CH // 8), (c + 1) * (CH // 8), mix, 0)
        out_copy(0, c).start()
        out_copy(1, c).start()
        return 0

    lax.fori_loop(0, NCH, mix_chunk, 0)
    for k in range(NL):
        for i, ref in enumerate((tb, sb)):
            edge_row(trs, i, k, ref, 0)
            edge_row(trn, i, k, ref, NR - 1)
    third = [send(sts, gts_o, 15, to_x), send(trn, grts_o, 16, to_n), send(trs, grtn_o, 17, to_s)]

    for c in second:
        c.wait()

    def spread(s, _):
        g = gx[rows(s), :]
        for k in range(NL):
            for slot, ref in enumerate((ug, vg, pg)):
                ref[k, rows(s), :] = unpack(g, slot, k)
        return 0

    lax.fori_loop(0, NR // 8 + 2, spread, 0)
    for k in range(NL):
        for i, ref in enumerate((ub, vb)):
            ghost_row(ref, k, 7, grs, i)
        for i, ref in enumerate((ub, vb, pb)):
            ghost_row(ref, k, NR + 8, grn, i)

    def corner(r, k):
        here, above = ub[k, rows(r, 8), :], ub[k, rows(r, 16), :]
        g_here, g_above = ug[k, rows(r, 8), :], ug[k, rows(r, 16), :]
        u_e = jnp.concatenate([here, g_here], 1)
        un_e = jnp.concatenate([north(here, above), north(g_here, g_above)], 1)
        v = vb[k, rows(r, 8), :]
        v_e = jnp.concatenate([v, vg[k, rows(r, 8), :]], 1)
        f_e = 0.25 * ((v_e + east(v_e)) * (u_e + un_e))
        return u_e, v, f_e

    for k in range(NL):
        fp[k] = corner(-1, k)[2]

    def tendency(r, _):
        for k in range(NL):
            u_e, v, f_e = corner(r, k)
            f = f_e[:, BODY]
            f_s = south(f, fp[k, :, BODY])
            fp[k] = f_e
            p = pb[k, rows(r, 8), :]
            p_e = east(jnp.concatenate([p, pg[k, rows(r, 8), :]], 1))[:, BODY]
            p_n = north(p, pb[k, rows(r, 16), :])
            du = 0.5 * (u_e + east(u_e))
            du = du * du
            dup[k] = du
            hi = 0.5 * (v + north(v, vb[k, rows(r, 16), :]))
            lo = 0.5 * (v + south(v, vb[k, rows(r), :]))
            su[k, rows(r), :] = (f_s - f) + ((p - p_e) - du[:, BODY])
            sv[k, rows(r), :] = (lo * lo - hi * hi) + ((p - p_n) - f)
        k_u, k_v = count_u(r), count_v(r)
        acc_u = acc_v = sum_u = sum_v = jnp.zeros((8, NC), F32)
        for k in range(NL):
            u, v = ub[k, rows(r, 8), :], vb[k, rows(r, 8), :]
            t_u = jnp.where(k_u > k, su[k, rows(r), :] + west(dup[k])[:, BODY], ZERO)
            t_v = jnp.where(k_v > k, sv[k, rows(r), :] + west(fp[k])[:, BODY], ZERO)
            su[k, rows(r), :] = u + TIME_STEP * t_u
            sv[k, rows(r), :] = v + TIME_STEP * t_v
            acc_u, acc_v = acc_u + t_u, acc_v + t_v
            sum_u, sum_v = sum_u + u, sum_v + v
        dz_u, dz_v = face_dz(r)
        f_x, f_y = dz_u * acc_u, dz_v * acc_v
        s_u = dz_u * (sum_u + TIME_STEP * acc_u)
        ext[FX, rows(r, HR), BODY] = f_x
        ext[FY, rows(r, HR), BODY] = f_y
        ext[SU, rows(r, HR), BODY] = s_u
        ext[SV, rows(r, HR), BODY] = dz_v * (sum_v + TIME_STEP * acc_v)
        pc[rows(r), :] = pack_wide((f_x, f_y, s_u))
        return 0

    def face_dz(r):
        dz_e = ext[DZ, rows(r, HR), :]
        dz = dz_e[:, BODY]
        dz_u = 0.5 * (dz + east(dz_e)[:, BODY])
        dz_v = 0.5 * (dz + north(dz, ext[DZ, rows(r, HR + 8), BODY]))
        return dz_u, dz_v

    lax.fori_loop(0, NR // 8, tendency, 0)
    fourth = send_ext(FX, 3, pc, gc, 18)
    receive_ext(later, gb, (TU, TV))
    out_ext0 = pltpu.make_async_copy(ext.at[pl.ds(0, 5)], ext_o.at[pl.ds(0, 5)], outs_sem.at[0])
    out_ext0.start()

    def momentum(r, _):
        dz_u, dz_v = face_dz(r)
        solve((su,), True, count_u(r), (TIME_STEP * VISC_KV) / (dz_u * dz_u), gains, rows(r))
        solve((sv,), True, count_v(r), (TIME_STEP * VISC_KV) / (dz_v * dz_v), gains2, rows(r))
        sug[rows(r), :] = pack([(0, k, su[k, rows(r), LEFT], su[k, rows(r), RIGHT]) for k in range(NL)])
        return 0

    def momentum_chunk(c, _):
        lax.fori_loop(c * (CH // 8), (c + 1) * (CH // 8), momentum, 0)
        out_copy(2, c).start()
        out_copy(3, c).start()
        return 0

    lax.fori_loop(0, NCH, momentum_chunk, 0)
    for k in range(NL):
        edge_row(vrn, 0, k, sv, NR - 1)
    fifth = [send(sug, gu_o, 23, to_x), send(vrn, grv_o, 24, to_n)]
    receive_ext(fourth, gc, (FX, FY, SU))
    out_ext1 = pltpu.make_async_copy(ext.at[pl.ds(5, 4)], ext_o.at[pl.ds(5, 4)], outs_sem.at[1])
    out_ext1.start()

    def drain(c, _):
        for i in range(4):
            out_copy(i, c).wait()
        return 0

    lax.fori_loop(0, NCH, drain, 0)
    for c in third:
        c.wait()
    for c in fifth:
        c.wait()
    out_ext0.wait()
    out_ext1.wait()


def finish_kernel(
    tide, su_h, sv_h, tm_h, sm_h, ext_h, gts_h, gu_h, grts_h, grtn_h, grv_h,
    eta_o, tu_o, tv_o, u_o, v_o, t_o, s_o,
    ub, vb, tb, sb, ext, cof, avg, gts, gu, grts, grtn, grv, fpt, fps, fxt, fxs, ug, tg, sg,
    load_sem, small_sem, out_sem, outs_sem,
):
    early = pltpu.make_async_copy(ext_h, ext, small_sem.at[0])
    early.start()
    small = [
        pltpu.make_async_copy(a, b, small_sem.at[i + 1])
        for i, (a, b) in enumerate(((gts_h, gts), (gu_h, gu), (grts_h, grts), (grtn_h, grtn), (grv_h, grv)))
    ]
    for c in small:
        c.start()
    big = [
        pltpu.make_async_copy(su_h, ub, load_sem.at[0]),
        pltpu.make_async_copy(sv_h, vb.at[:, pl.ds(8, NR), :], load_sem.at[1]),
        pltpu.make_async_copy(tm_h, tb.at[:, pl.ds(8, NR), :], load_sem.at[2]),
        pltpu.make_async_copy(sm_h, sb.at[:, pl.ds(8, NR), :], load_sem.at[3]),
    ]
    for c in big:
        c.start()
    early.wait()

    def faces(at, above):
        kc, kn = ext[KMT, at, :], ext[KMT, above, :]
        dz, dn = ext[DZ, at, :], ext[DZ, above, :]
        k_u = jnp.minimum(kc, east(kc))
        k_v = jnp.minimum(kc, north(kc, kn))
        return kc, k_u, k_v, k_u * (0.5 * (dz + east(dz))), k_v * (0.5 * (dz + north(dz, dn)))

    def prepare(t, _):
        at = rows(t)
        kc, k_u, k_v, h_u, h_v = faces(at, rows(jnp.minimum(t + 1, ER // 8 - 1)))
        cof[0, at, :] = (DTB * DTB) * h_u
        cof[1, at, :] = (DTB * DTB) * h_v
        for f in (FX, FY):
            ext[f, at, :] = (DTB * DTB) * ext[f, at, :]
        for f, count, scale in ((ETA, kc, 1.0), (TU, k_u, DTB), (TV, k_v, DTB)):
            ext[f, at, :] = jnp.where(count > ZERO, scale * ext[f, at, :], ZERO)
        for i in range(2):
            avg[i, at, :] = jnp.zeros((8, EC), F32)
        return 0

    lax.fori_loop(0, ER // 8, prepare, 0)

    norm = 6.0 / (NSUB * (NSUB + 1) * (NSUB + 2)) / DTB

    def subcycle(n, _, lo, hi):
        tide_x, tide_y = tide[n, 0], tide[n, 1]
        weight = norm * ((n + 1) * (NSUB - n)).astype(F32)
        v_prev = ext[TV, rows(max(lo - 1, 0)), :]
        eta_prev = None
        u_keep = v_keep = None
        for t in range(lo, hi + 1):
            if t < hi:
                at = rows(t)
                u, v = ext[TU, at, :], ext[TV, at, :]
                eta = ext[ETA, at, :] - ((u - west(u)) + (v - south(v, v_prev)))
                ext[ETA, at, :] = eta
            if t > lo:
                b = rows(t - 1)
                slope_x = east(eta_prev) - eta_prev
                slope_y = north(eta_prev, eta) - eta_prev
                u_new = u_keep + (cof[0, b, :] * (tide_x - slope_x) + ext[FX, b, :])
                v_new = v_keep + (cof[1, b, :] * (tide_y - slope_y) + ext[FY, b, :])
                ext[TU, b, :] = u_new
                ext[TV, b, :] = v_new
                if 2 <= t - 1 < 19:
                    avg[0, b, :] = avg[0, b, :] + weight * u_new
                    avg[1, b, :] = avg[1, b, :] + weight * v_new
            eta_prev, u_keep, v_keep, v_prev = eta, u, v, v
        return 0

    tiles = ER // 8
    lax.fori_loop(0, 4, functools.partial(subcycle, lo=0, hi=tiles), 0)
    lax.fori_loop(4, 12, functools.partial(subcycle, lo=1, hi=tiles - 1), 0)
    lax.fori_loop(12, NSUB, functools.partial(subcycle, lo=2, hi=tiles - 2), 0)

    def unscale(r, _):
        at = rows(r, HR)
        for f in (TU, TV):
            ext[f, at, :] = (1.0 / DTB) * ext[f, at, :]
        return 0

    lax.fori_loop(0, NR // 8, unscale, 0)
    planes = [
        pltpu.make_async_copy(ext.at[2 + i, pl.ds(HR, NR), pl.ds(0, NC)], o, outs_sem.at[i])
        for i, o in enumerate((eta_o, tu_o, tv_o))
    ]
    for c in planes:
        c.start()
    for c in small:
        c.wait()
    for c in big:
        c.wait()
    for k in range(NL):
        vb[k, 7:8, :] = grv[k : k + 1, :]
        for i, ref in enumerate((tb, sb)):
            ref[k, 7:8, :] = grts[24 * i + k : 24 * i + k + 1, :]
            ref[k, NR + 8 : NR + 9, :] = grtn[24 * i + k : 24 * i + k + 1, :]

    def strip(r):
        at, above = rows(r, HR), rows(r, HR + 8)
        kc, k_u, k_v, h_u, h_v = faces(at, above)
        d_u = (avg[0, at, :] - ext[SU, at, :]) / jnp.where(h_u > ZERO, h_u, 1.0)
        d_v = (avg[1, at, BODY] - ext[SV, at, BODY]) / jnp.where(h_v > ZERO, h_v, 1.0)[:, BODY]
        return kc[:, BODY], k_u, k_v[:, BODY], d_u, d_v

    def flux_y(r, k, k_v, d_v):
        vc = jnp.where(k_v > k, vb[k, rows(r, 8), :] + d_v, ZERO)
        out = [vc]
        for ref in (tb, sb):
            here = ref[k, rows(r, 8), :]
            out.append(here)
            out.append(vc * (here + north(here, ref[k, rows(r, 16), :])))
        return out

    _, _, k_v, _, d_v = strip(-1)
    for k in range(NL):
        _, _, a, _, b = flux_y(-1, k, k_v, d_v)
        fpt[k] = a
        fps[k] = b

    def spread(r, _):
        g_u, g_ts = gu[rows(r), :], gts[rows(r), :]
        for k in range(NL):
            ug[k, rows(r), :] = unpack(g_u, 0, k)
            tg[k, rows(r), :] = unpack(g_ts, 0, k)
            sg[k, rows(r), :] = unpack(g_ts, 1, k)
        return 0

    lax.fori_loop(0, NR // 8, spread, 0)

    def advect(r, _):
        kc, k_u, k_v, d_u, d_v = strip(r)
        for k in range(NL):
            vc, t, y_t, s, y_s = flux_y(r, k, k_v, d_v)
            vb[k, rows(r, 8), :] = vc
            uc = jnp.where(k_u > k, jnp.concatenate([ub[k, rows(r), :], ug[k, rows(r), :]], 1) + d_u, ZERO)
            ub[k, rows(r), :] = uc[:, BODY]
            for ref, ghost, prev, keep, x, y in ((tb, tg, fpt, fxt, t, y_t), (sb, sg, fps, fxs, s, y_s)):
                x_e = jnp.concatenate([x, ghost[k, rows(r), :]], 1)
                fx = uc * (x_e + east(x_e))
                keep[k] = fx
                ref[k, rows(r, 8), :] = x - (0.5 * TIME_STEP) * (fx[:, BODY] + (y - south(y, prev[k])))
                prev[k] = y
        for k in range(NL):
            for ref, keep in ((tb, fxt), (sb, fxs)):
                x = ref[k, rows(r, 8), :] + (0.5 * TIME_STEP) * west(keep[k])[:, BODY]
                ref[k, rows(r, 8), :] = jnp.where(kc > k, x, ZERO)
        return 0

    def out_copy(i, c):
        src = (ub, vb, tb, sb)[i]
        dst = (u_o, v_o, t_o, s_o)[i]
        at = pl.ds(pl.multiple_of(c * CH, CH), CH)
        frm = pl.ds(pl.multiple_of(c * CH + (8 if i else 0), 8), CH)
        return pltpu.make_async_copy(src.at[:, frm, :], dst.at[:, at, :], out_sem.at[i, c])

    def advect_chunk(c, _):
        lax.fori_loop(c * (CH // 8), (c + 1) * (CH // 8), advect, 0)
        for i in range(4):
            out_copy(i, c).start()
        return 0

    lax.fori_loop(0, NCH, advect_chunk, 0)

    def drain(c, _):
        for i in range(4):
            out_copy(i, c).wait()
        return 0

    lax.fori_loop(0, NCH, drain, 0)
    for c in planes:
        c.wait()


def vmem(*shape):
    return pltpu.VMEM(shape, F32)


def solution(mesh):
    any_spec = pl.BlockSpec(memory_space=pl.ANY)
    cube = jax.ShapeDtypeStruct((NL, NR, NC), F32)
    plane = jax.ShapeDtypeStruct((NR, NC), F32)

    tile, ghost, strip = vmem(NR, 128), vmem(ER, 128), vmem(NL, 8, NC)

    def arr(*shape):
        return jax.ShapeDtypeStruct(shape, F32)

    def local_step(vel_u, vel_v, temperature, salinity, sea_level, trans_u, trans_v, bathymetry, kmt_levels, tide_force):
        mid = pl.pallas_call(
            predict_kernel,
            name="predict",
            out_shape=(
                cube, cube, cube, cube, arr(9, ER, EC), arr(NR, 128), arr(NR, 128), arr(48, NC), arr(48, NC), arr(24, NC),
            ),
            in_specs=[any_spec] * 9,
            out_specs=(any_spec,) * 10,
            scratch_shapes=[
                *([vmem(NL, NR + 16, NC)] * 3), *([vmem(NL, NR, NC)] * 4),
                vmem(9, ER, EC), pltpu.VMEM((NR, NC), jnp.int32), vmem(NR, NC),
                *([tile] * 3), *([ghost] * 3), *([vmem(NL, NR + 16, 128)] * 3), vmem(NL, 8, EC), tile, vmem(NR + 16, 128),
                vmem(48, NC), vmem(72, NC), vmem(48, NC), vmem(72, NC),
                tile, vmem(48, NC), vmem(48, NC), tile, vmem(24, NC), vmem(NL, 8, EC), strip, strip,
                pltpu.SemaphoreType.DMA((4, NCH)), pltpu.SemaphoreType.DMA((5,)), pltpu.SemaphoreType.DMA((4, NCH)),
                pltpu.SemaphoreType.DMA((2,)), pltpu.SemaphoreType.DMA((25,)), pltpu.SemaphoreType.DMA((25,)),
            ],
            compiler_params=pltpu.CompilerParams(collective_id=0, has_side_effects=True, vmem_limit_bytes=63 * 2**20),
        )(vel_u, vel_v, temperature, salinity, sea_level, trans_u, trans_v, bathymetry, kmt_levels)
        return pl.pallas_call(
            finish_kernel,
            name="finish",
            out_shape=(plane, plane, plane, cube, cube, cube, cube),
            in_specs=[pl.BlockSpec(memory_space=pltpu.SMEM)] + [any_spec] * 10,
            out_specs=(any_spec,) * 7,
            scratch_shapes=[
                vmem(NL, NR, NC), vmem(NL, NR + 8, NC), vmem(NL, NR + 16, NC), vmem(NL, NR + 16, NC),
                vmem(9, ER, EC), vmem(2, ER, EC), vmem(2, ER, EC),
                vmem(NR, 128), vmem(NR, 128), vmem(48, NC), vmem(48, NC), vmem(24, NC), strip, strip,
                *([vmem(NL, 8, EC)] * 2), *([vmem(NL, NR, 128)] * 3),
                pltpu.SemaphoreType.DMA((4,)), pltpu.SemaphoreType.DMA((6,)), pltpu.SemaphoreType.DMA((4, NCH)),
                pltpu.SemaphoreType.DMA((3,)),
            ],
            compiler_params=pltpu.CompilerParams(vmem_limit_bytes=60 * 2**20),
        )(tide_force, *mid)

    spec_cube = P(None, "row", "col")
    spec_plane = P("row", "col")
    return jax.shard_map(
        local_step,
        mesh=mesh,
        in_specs=(spec_cube,) * 4 + (spec_plane,) * 5 + (P(None, None),),
        out_specs=(spec_plane,) * 3 + (spec_cube,) * 4,
        check_vma=False,
    )
```

```python
import functools

import jax
import jax.numpy as jnp
from jax import lax
from jax.experimental import pallas as pl
from jax.experimental.pallas import tpu as pltpu
from jax.sharding import PartitionSpec as P

TIME_STEP = 4.0
ALPHA_T = 0.02
BETA_S = 0.015
VISC_KV = 0.001
DIFF_KT = 0.0005

NL = 20
NSUB = 20
NR, NC = 128, 512
HR = 24
ER, EC = NR + 2 * HR, NC + 128
NCH = 8
CH = NR // NCH
EARLY = NCH // 2
DTB = TIME_STEP / NSUB
F32 = jnp.float32
ZERO = 0.0
BODY = slice(0, NC)
LEFT = slice(0, 128)
RIGHT = slice(NC - 128, NC)
GHOST = slice(NC, EC)
KMT, DZ, ETA, TU, TV, FX, FY, SV, SU = range(9)
KU, KV, DU, DV = range(4)
WIDE = 42
MESH = pl.DeviceIdType.MESH


def rows(r, off=0):
    start = 8 * r + off
    if isinstance(start, int):
        return pl.ds(start, 8)
    return pl.ds(pl.multiple_of(start, 8), 8)


def iota(shape, axis):
    return lax.broadcasted_iota(jnp.int32, shape, axis)


def east(x):
    return pltpu.roll(x, x.shape[1] - 1, 1)


def west(x):
    return pltpu.roll(x, 1, 1)


def north(here, above):
    return pltpu.roll(jnp.where(iota(here.shape, 0) == 0, above, here), 7, 0)


def south(here, below):
    return pltpu.roll(jnp.where(iota(here.shape, 0) == 7, below, here), 1, 0)


def lane_of(slot, k):
    return 2 * k + 40 * slot


def unpack(ghost, slot, k):
    shift = (128 - lane_of(slot, k)) % 128
    return pltpu.roll(ghost, shift, 1) if shift else ghost


def pack(tiles):
    lane = iota((8, 128), 1)
    acc = None
    first = None
    for slot, k, low, high in tiles:
        both = jnp.where(lane == 127, high, low)
        at = lane_of(slot, k)
        moved = pltpu.roll(both, at, 1) if at else both
        if acc is None:
            acc = moved
            if at == 0:
                first = moved
        else:
            acc = jnp.where(lane >= at - 1, moved, acc)
    if first is not None:
        acc = jnp.where(lane == 127, first, acc)
    return acc


def pack_wide(planes):
    lane = iota((8, 128), 1)
    acc = None
    for q, x in enumerate(planes):
        edge = jnp.where(lane < 64, x[:, LEFT], x[:, RIGHT])
        if acc is None:
            acc = edge
        else:
            acc = jnp.where(lane >= WIDE * q - WIDE // 2, pltpu.roll(edge, WIDE * q, 1), acc)
    if len(planes) == 1:
        return acc
    first = jnp.where(lane < 64, planes[0][:, LEFT], planes[0][:, RIGHT])
    return jnp.where(lane >= 128 - WIDE // 2, first, acc)


def unpack_wide(tile, q):
    lane = iota(tile.shape, 1)
    moved = pltpu.roll(tile, 128 - WIDE * q, 1) if q else tile
    return jnp.where((lane < WIDE // 2) | (lane >= 128 - WIDE // 2), moved, ZERO)


def solve(refs, masked, count, coef, gains, at):
    low = None
    rest = 1.0
    parts = [None] * len(refs)
    for k in range(NL):
        up = jnp.where(count > k + 1.0, coef, ZERO) if k < NL - 1 else ZERO
        inv = 1.0 / (rest + up)
        for i, ref in enumerate(refs):
            src = ref[k, at, :]
            if not masked:
                src = jnp.where(count > k, src, ZERO)
            parts[i] = src * inv if k == 0 else (src + low * parts[i]) * inv
            if k < NL - 1:
                ref[k, at, :] = parts[i]
        if k < NL - 1:
            gain = up * inv
            gains[k] = gain
            rest = 1.0 + gain * rest
        low = up
    for i, ref in enumerate(refs):
        ref[NL - 1, at, :] = parts[i]
    for k in range(NL - 2, -1, -1):
        gain = gains[k]
        for i, ref in enumerate(refs):
            parts[i] = ref[k, at, :] + gain * parts[i]
            ref[k, at, :] = parts[i]


def predict_kernel(
    u_h, v_h, t_h, s_h, eta_h, tu_h, tv_h, dep_h, kmt_h,
    su_o, sv_o, tm_o, sm_o, ext_o, gts_o, gu_o, grts_o, grtn_o, grv_o,
    ub, vb, pb, tb, sb, su, sv, ext, ktmp, htmp, pa, pb_, pc, ga, gb, gc, ug, vg, pg, dup, sp, gx, prn, prs, grs, grn, sts, trn, trs, sug, vrn, fp, fsp, csp, geo, tot, gains, gains2,
    load_sem, small_sem, out_sem, outs_sem, send_sem, recv_sem,
):
    col = lax.axis_index("col")
    row = lax.axis_index("row")
    n_row = 8
    side = 1 - col
    up_row = lax.rem(row + 1, n_row)
    down_row = lax.rem(row + n_row - 1, n_row)
    to_x = {"col": side, "row": row}
    to_n = {"col": col, "row": up_row}
    to_s = {"col": col, "row": down_row}
    to_dn = {"col": side, "row": up_row}
    to_ds = {"col": side, "row": down_row}

    barrier = pltpu.get_barrier_semaphore()
    for dev in (to_x, to_n, to_s, to_dn, to_ds):
        pl.semaphore_signal(barrier, inc=1, device_id=dev, device_id_type=MESH)

    small = [
        pltpu.make_async_copy(kmt_h, ktmp, small_sem.at[0]),
        pltpu.make_async_copy(dep_h, htmp, small_sem.at[1]),
        pltpu.make_async_copy(eta_h, ext.at[2, pl.ds(HR, NR), pl.ds(0, NC)], small_sem.at[2]),
        pltpu.make_async_copy(tu_h, ext.at[3, pl.ds(HR, NR), pl.ds(0, NC)], small_sem.at[3]),
        pltpu.make_async_copy(tv_h, ext.at[4, pl.ds(HR, NR), pl.ds(0, NC)], small_sem.at[4]),
    ]
    for c in small:
        c.start()

    def load(i, c):
        src = (t_h, s_h, u_h, v_h)[i]
        dst = (tb, sb, ub, vb)[i]
        at = pl.ds(pl.multiple_of(c * CH, CH), CH)
        to = pl.ds(pl.multiple_of(c * CH + (8 if i >= 2 else 0), 8), CH)
        return pltpu.make_async_copy(src.at[:, at, :], dst.at[:, to, :], load_sem.at[i, c])

    def start_loads(pair):
        def body(c, _):
            for i in pair:
                load(i, c).start()
            return 0

        lax.fori_loop(0, NCH, body, 0)

    start_loads((0, 1))
    start_loads((2, 3))

    def send(src, dst, idx, dev):
        c = pltpu.make_async_remote_copy(
            src_ref=src, dst_ref=dst, send_sem=send_sem.at[idx], recv_sem=recv_sem.at[idx], device_id=dev, device_id_type=MESH
        )
        c.start()
        return c

    for c in small:
        c.wait()
    for r in range(NR // 8):
        kf = ktmp[rows(r), :].astype(F32)
        dz = htmp[rows(r), :] / jnp.maximum(kf, 1.0)
        ext[KMT, rows(r, HR), BODY] = kf
        ext[DZ, rows(r, HR), BODY] = dz
        eta, tu, tv = (ext[f, rows(r, HR), BODY] for f in (ETA, TU, TV))
        pa[rows(r), :] = pack_wide((kf, dz, eta))
        pb_[rows(r), :] = pack_wide((tu, tv))
    pl.semaphore_wait(barrier, 5)

    def send_ext(lo, n, tile, ghost, base):
        at = pl.ds(lo, n)
        low, high, mid = pl.ds(0, HR), pl.ds(HR + NR, HR), pl.ds(HR, NR)
        body = pl.ds(0, NC)
        return [
            send(tile, ghost.at[mid, :], base, to_x),
            send(ext.at[at, pl.ds(NR, HR), body], ext.at[at, low, body], base + 1, to_n),
            send(ext.at[at, pl.ds(HR, HR), body], ext.at[at, high, body], base + 2, to_s),
            send(tile.at[pl.ds(NR - HR, HR), :], ghost.at[low, :], base + 3, to_dn),
            send(tile.at[low, :], ghost.at[high, :], base + 4, to_ds),
        ]

    def receive_ext(copies, ghost, fields):
        for c in copies:
            c.wait()

        for q, f in enumerate(fields):
            ext[f, :, GHOST] = unpack_wide(ghost[...], q)

    first = send_ext(KMT, 3, pa, ga, 0)
    later = send_ext(TU, 2, pb_, gb, 5)

    def pressure(r, _):
        kc = ext[KMT, rows(r, HR), BODY]
        dz = ext[DZ, rows(r, HR), BODY]
        total = jnp.zeros((8, NC), F32)
        scale = TIME_STEP * dz
        for k in range(NL):
            half = (0.5 * BETA_S) * (sb[k, rows(r), :] - 1.0) - (0.5 * ALPHA_T) * (tb[k, rows(r), :] - 1.0)
            half = jnp.where(kc > k, half, ZERO)
            middle = total + half
            total = middle + half
            pb[k, rows(r, 8), :] = scale * middle
        return 0

    def pressure_chunk(c, _):
        load(0, c).wait()
        load(1, c).wait()
        lax.fori_loop(c * (CH // 8), (c + 1) * (CH // 8), pressure, 0)
        return 0

    lax.fori_loop(0, NCH, pressure_chunk, 0)

    def out_copy(i, c):
        src = (tb, sb, su, sv)[i]
        dst = (tm_o, sm_o, su_o, sv_o)[i]
        at = pl.ds(pl.multiple_of(c * CH, CH), CH)
        return pltpu.make_async_copy(src.at[:, at, :], dst.at[:, at, :], out_sem.at[i, c])

    def pack_ts(r):
        tiles = []
        for slot, ref in enumerate((tb, sb)):
            for k in range(NL):
                tiles.append((slot, k, ref[k, rows(r), LEFT], ref[k, rows(r), RIGHT]))
        sts[rows(r), :] = pack(tiles)

    def mix(r, _):
        pack_ts(jnp.maximum(r - 1, 0))
        kc = ext[KMT, rows(r, HR), BODY]
        dz = ext[DZ, rows(r, HR), BODY]
        solve((tb, sb), False, kc, (TIME_STEP * DIFF_KT) / (dz * dz), gains, rows(r))
        return 0

    def mix_chunk(c, _):
        lax.fori_loop(c * (CH // 8), (c + 1) * (CH // 8), mix, 0)
        out_copy(0, c).start()
        out_copy(1, c).start()
        return 0

    lax.fori_loop(0, EARLY, mix_chunk, 0)

    receive_ext(first, ga, (KMT, DZ, ETA))
    has_south = (row > 0).astype(F32)
    has_north = (row < n_row - 1).astype(F32)
    ext[KMT, 0:HR, :] = ext[KMT, 0:HR, :] * has_south
    ext[KMT, HR + NR :, :] = ext[KMT, HR + NR :, :] * has_north

    for r in range(NR // 8):
        at, above = rows(r, HR), rows(r, HR + 8)
        kc, dz = ext[KMT, at, :], ext[DZ, at, :]
        k_c, dz_c = kc[:, BODY], dz[:, BODY]
        geo[KU, rows(r), :] = jnp.minimum(k_c, east(kc)[:, BODY])
        geo[KV, rows(r), :] = jnp.minimum(k_c, north(k_c, ext[KMT, above, BODY]))
        geo[DU, rows(r), :] = 0.5 * (dz_c + east(dz)[:, BODY])
        geo[DV, rows(r), :] = 0.5 * (dz_c + north(dz_c, ext[DZ, above, BODY]))

    def pack_uvp(r):
        tiles = []
        for slot, ref in enumerate((ub, vb, pb)):
            for k in range(NL):
                tiles.append((slot, k, ref[k, rows(r, 8), LEFT], ref[k, rows(r, 8), RIGHT]))
        sp[rows(r), :] = pack(tiles)

    def mask_pack(r, _):
        pack_uvp(jnp.maximum(r - 1, 0))
        for slot, ref in enumerate((ub, vb)):
            count = geo[slot, rows(r), :]
            total = jnp.zeros((8, NC), F32)
            for k in range(NL):
                x = jnp.where(count > k, ref[k, rows(r, 8), :], ZERO)
                ref[k, rows(r, 8), :] = x
                total = total + x
            tot[slot, rows(r), :] = total
        return 0

    def mask_chunk(c, _):
        load(2, c).wait()
        load(3, c).wait()
        lax.fori_loop(c * (CH // 8), (c + 1) * (CH // 8), mask_pack, 0)
        return 0

    lax.fori_loop(0, NCH, mask_chunk, 0)
    pack_uvp(NR // 8 - 1)

    def edge_row(dst, i, k, ref, at):
        dst[24 * i + k : 24 * i + k + 1, :] = ref[k, at : at + 1, :]

    def ghost_row(ref, k, at, src, i):
        ref[k, at : at + 1, :] = src[24 * i + k : 24 * i + k + 1, :]

    for k in range(NL):
        for i, ref in enumerate((ub, vb, pb)):
            edge_row(prs, i, k, ref, 8)
        for i, ref in enumerate((ub, vb)):
            edge_row(prn, i, k, ref, NR + 7)
    second = [
        send(sp, gx.at[pl.ds(8, NR), :], 10, to_x),
        send(prn, grs, 11, to_n),
        send(prs, grn, 12, to_s),
        send(sp.at[pl.ds(NR - 8, 8), :], gx.at[pl.ds(0, 8), :], 13, to_dn),
        send(sp.at[pl.ds(0, 8), :], gx.at[pl.ds(NR + 8, 8), :], 14, to_ds),
    ]

    lax.fori_loop(EARLY, NCH, mix_chunk, 0)
    pack_ts(NR // 8 - 1)
    for k in range(NL):
        for i, ref in enumerate((tb, sb)):
            edge_row(trs, i, k, ref, 0)
            edge_row(trn, i, k, ref, NR - 1)
    third = [send(sts, gts_o, 15, to_x), send(trn, grts_o, 16, to_n), send(trs, grtn_o, 17, to_s)]

    for c in second:
        c.wait()

    def spread(i, _):
        for j in range(3):
            at = rows(3 * i + j)
            g = gx[at, :]
            for k in range(NL):
                for slot, ref in enumerate((ug, vg, pg)):
                    ref[k, at, :] = unpack(g, slot, k)
        return 0

    lax.fori_loop(0, (NR // 8 + 2) // 3, spread, 0)
    for k in range(NL):
        for i, ref in enumerate((ub, vb)):
            ghost_row(ref, k, 7, grs, i)
        for i, ref in enumerate((ub, vb, pb)):
            ghost_row(ref, k, NR + 8, grn, i)

    def corner(r, k):
        here, below = rows(r, 8), rows(r)
        u_e = jnp.concatenate([ub[k, here, :], ug[k, here, :]], 1)
        v = vb[k, here, :]
        u_s = south(u_e, jnp.concatenate([ub[k, below, :], ug[k, below, :]], 1))
        v_s = south(
            jnp.concatenate([v, vg[k, here, :]], 1), jnp.concatenate([vb[k, below, :], vg[k, below, :]], 1)
        )
        f_s = (v_s + east(v_s)) * (u_s + u_e)
        p = pb[k, here, :]
        c = v + v_s[:, BODY]
        c = c * c + p
        return u_e, p, f_s, c

    for k in range(NL):
        fsp[k], csp[k] = corner(NR // 8, k)[2:]

    def tendency(i, _):
        r = NR // 8 - 1 - i
        at = rows(r)
        for k in range(NL):
            u_e, p, f_s, c = corner(r, k)
            f = north(f_s, fsp[k])
            c_n = north(c, csp[k])
            fsp[k], csp[k] = f_s, c
            d = u_e + west(u_e)
            d = d * d + jnp.concatenate([p, pg[k, rows(r, 8), :]], 1)
            fp[k], dup[k] = f, d
            su[k, at, :] = (f_s - f)[:, BODY] + d[:, BODY]
            sv[k, at, :] = (c - c_n) - f[:, BODY]
        k_u, k_v = geo[KU, at, :], geo[KV, at, :]
        sum_u = sum_v = jnp.zeros((8, NC), F32)
        for k in range(NL):
            t_u = su[k, at, :] - east(dup[k])[:, BODY]
            t_v = sv[k, at, :] + west(fp[k])[:, BODY]
            u = jnp.where(k_u > k, ub[k, rows(r, 8), :] + t_u, ZERO)
            v = jnp.where(k_v > k, vb[k, rows(r, 8), :] + t_v, ZERO)
            su[k, at, :], sv[k, at, :] = u, v
            sum_u, sum_v = sum_u + u, sum_v + v
        dz_u, dz_v = geo[DU, at, :], geo[DV, at, :]
        ext[FX, rows(r, HR), BODY] = (dz_u / TIME_STEP) * (sum_u - tot[KU, at, :])
        ext[FY, rows(r, HR), BODY] = (dz_v / TIME_STEP) * (sum_v - tot[KV, at, :])
        ext[SU, rows(r, HR), BODY] = dz_u * sum_u
        ext[SV, rows(r, HR), BODY] = dz_v * sum_v
        return 0

    lax.fori_loop(0, NR // 8, tendency, 0)
    for r in range(NR // 8):
        pc[rows(r), :] = pack_wide([ext[f, rows(r, HR), BODY] for f in (FX, FY, SU)])
    fourth = send_ext(FX, 3, pc, gc, 18)
    receive_ext(later, gb, (TU, TV))
    out_ext0 = pltpu.make_async_copy(ext.at[pl.ds(0, 5)], ext_o.at[pl.ds(0, 5)], outs_sem.at[0])
    out_ext0.start()

    def pack_su(r):
        sug[rows(r), :] = pack([(0, k, su[k, rows(r), LEFT], su[k, rows(r), RIGHT]) for k in range(NL)])

    def momentum(r, _):
        pack_su(jnp.maximum(r - 1, 0))
        for i, (ref, keep) in enumerate(((su, gains), (sv, gains2))):
            dz = geo[DU + i, rows(r), :]
            solve((ref,), True, geo[i, rows(r), :], (TIME_STEP * VISC_KV) / (dz * dz), keep, rows(r))
        return 0

    def momentum_chunk(c, _):
        lax.fori_loop(c * (CH // 8), (c + 1) * (CH // 8), momentum, 0)
        out_copy(2, c).start()
        out_copy(3, c).start()
        return 0

    lax.fori_loop(0, NCH, momentum_chunk, 0)
    pack_su(NR // 8 - 1)
    for k in range(NL):
        edge_row(vrn, 0, k, sv, NR - 1)
    fifth = [send(sug, gu_o, 23, to_x), send(vrn, grv_o, 24, to_n)]
    receive_ext(fourth, gc, (FX, FY, SU))
    out_ext1 = pltpu.make_async_copy(ext.at[pl.ds(5, 4)], ext_o.at[pl.ds(5, 4)], outs_sem.at[1])
    out_ext1.start()

    def drain(c, _):
        for i in range(4):
            out_copy(i, c).wait()
        return 0

    lax.fori_loop(0, NCH, drain, 0)
    for c in third:
        c.wait()
    for c in fifth:
        c.wait()
    out_ext0.wait()
    out_ext1.wait()


def finish_kernel(
    tide, su_h, sv_h, tm_h, sm_h, ext_h, gts_h, gu_h, grts_h, grtn_h, grv_h,
    eta_o, tu_o, tv_o, u_o, v_o, t_o, s_o,
    ub, vb, tb, sb, ext, cof, cnt, avg, gts, gu, grts, grtn, grv, fpt, fps, fxt, fxs, ug, tg, sg,
    load_sem, small_sem, out_sem, outs_sem,
):
    early = pltpu.make_async_copy(ext_h, ext, small_sem.at[0])
    early.start()
    small = [
        pltpu.make_async_copy(a, b, small_sem.at[i + 1])
        for i, (a, b) in enumerate(((gts_h, gts), (gu_h, gu), (grts_h, grts), (grtn_h, grtn), (grv_h, grv)))
    ]
    for c in small:
        c.start()
    big = [
        pltpu.make_async_copy(su_h, ub, load_sem.at[0]),
        pltpu.make_async_copy(sv_h, vb.at[:, pl.ds(8, NR), :], load_sem.at[1]),
        pltpu.make_async_copy(tm_h, tb.at[:, pl.ds(8, NR), :], load_sem.at[2]),
        pltpu.make_async_copy(sm_h, sb.at[:, pl.ds(8, NR), :], load_sem.at[3]),
    ]
    for c in big:
        c.start()
    early.wait()

    def faces(at, above):
        kc, kn = ext[KMT, at, :], ext[KMT, above, :]
        dz, dn = ext[DZ, at, :], ext[DZ, above, :]
        k_u = jnp.minimum(kc, east(kc))
        k_v = jnp.minimum(kc, north(kc, kn))
        return kc, k_u, k_v, k_u * (0.5 * (dz + east(dz))), k_v * (0.5 * (dz + north(dz, dn)))

    for t in range(ER // 8):
        at = rows(t)
        kc, k_u, k_v, h_u, h_v = faces(at, rows(min(t + 1, ER // 8 - 1)))
        for i, (count, h) in enumerate(((k_u, h_u), (k_v, h_v))):
            cof[i, at, :] = (DTB * DTB) * h
            cnt[i, at, :] = count
            ext[FX + i, at, :] = (DTB * DTB) * ext[FX + i, at, :]
            avg[i, at, :] = jnp.zeros((8, EC), F32)
        for f, count, scale in ((ETA, kc, 1.0), (TU, k_u, DTB), (TV, k_v, DTB)):
            ext[f, at, :] = jnp.where(count > ZERO, scale * ext[f, at, :], ZERO)

    norm = 6.0 / (NSUB * (NSUB + 1) * (NSUB + 2)) / DTB

    def subcycle(n, _, lo, hi):
        tide_x, tide_y = tide[0, n], tide[1, n]
        weight = norm * ((n + 1) * (NSUB - n)).astype(F32)
        v_prev = ext[TV, rows(max(lo - 1, 0)), :]
        eta_prev = None
        u_keep = v_keep = None
        for t in range(lo, hi + 1):
            if t < hi:
                at = rows(t)
                u, v = ext[TU, at, :], ext[TV, at, :]
                eta = ext[ETA, at, :] - ((u - west(u)) + (v - south(v, v_prev)))
                ext[ETA, at, :] = eta
            if t > lo:
                b = rows(t - 1)
                slope_x = east(eta_prev) - eta_prev
                slope_y = north(eta_prev, eta) - eta_prev
                u_new = u_keep + (cof[0, b, :] * (tide_x - slope_x) + ext[FX, b, :])
                v_new = v_keep + (cof[1, b, :] * (tide_y - slope_y) + ext[FY, b, :])
                ext[TU, b, :] = u_new
                ext[TV, b, :] = v_new
                if 2 <= t - 1 < 19:
                    avg[0, b, :] = avg[0, b, :] + weight * u_new
                    avg[1, b, :] = avg[1, b, :] + weight * v_new
            eta_prev, u_keep, v_keep, v_prev = eta, u, v, v
        return 0

    tiles = ER // 8
    lax.fori_loop(0, 4, functools.partial(subcycle, lo=0, hi=tiles), 0)
    lax.fori_loop(4, 12, functools.partial(subcycle, lo=1, hi=tiles - 1), 0)
    lax.fori_loop(12, NSUB, functools.partial(subcycle, lo=2, hi=tiles - 2), 0)

    for r in range(NR // 8):
        at = rows(r, HR)
        for f in (TU, TV):
            ext[f, at, :] = (1.0 / DTB) * ext[f, at, :]
    planes = [
        pltpu.make_async_copy(ext.at[2 + i, pl.ds(HR, NR), pl.ds(0, NC)], o, outs_sem.at[i])
        for i, o in enumerate((eta_o, tu_o, tv_o))
    ]
    for c in planes:
        c.start()
    for c in small:
        c.wait()
    for c in big:
        c.wait()
    for k in range(NL):
        vb[k, 7:8, :] = grv[k : k + 1, :]
        for i, ref in enumerate((tb, sb)):
            ref[k, 7:8, :] = grts[24 * i + k : 24 * i + k + 1, :]
            ref[k, NR + 8 : NR + 9, :] = grtn[24 * i + k : 24 * i + k + 1, :]

    for r in range(-1, NR // 8):
        at = rows(r, HR)
        for i, f in enumerate((SU, SV)):
            h = cof[i, at, :]
            avg[i, at, :] = (DTB * DTB) * (avg[i, at, :] - ext[f, at, :]) / jnp.where(h > ZERO, h, 1.0)

    def strip(r):
        at = rows(r, HR)
        return ext[KMT, at, BODY], cnt[0, at, :], cnt[1, at, BODY], avg[0, at, :], avg[1, at, BODY]

    def flux_y(r, k, k_v, d_v):
        vc = jnp.where(k_v > k, vb[k, rows(r, 8), :] + d_v, ZERO)
        out = [vc]
        for ref in (tb, sb):
            here = ref[k, rows(r, 8), :]
            out.append(here)
            out.append(vc * (here + north(here, ref[k, rows(r, 16), :])))
        return out

    _, _, k_v, _, d_v = strip(-1)
    for k in range(NL):
        _, _, a, _, b = flux_y(-1, k, k_v, d_v)
        fpt[k] = a
        fps[k] = b

    def spread(i, _):
        for j in range(4):
            at = rows(4 * i + j)
            g_u, g_ts = gu[at, :], gts[at, :]
            for k in range(NL):
                for ref, g, slot in ((ug, g_u, 0), (tg, g_ts, 0), (sg, g_ts, 1)):
                    ref[k, at, :] = unpack(g, slot, k)
        return 0

    lax.fori_loop(0, NR // 8 // 4, spread, 0)

    def advect(r, _):
        kc, k_u, k_v, d_u, d_v = strip(r)
        for k in range(NL):
            vc, t, y_t, s, y_s = flux_y(r, k, k_v, d_v)
            vb[k, rows(r, 8), :] = vc
            uc = jnp.where(k_u > k, jnp.concatenate([ub[k, rows(r), :], ug[k, rows(r), :]], 1) + d_u, ZERO)
            ub[k, rows(r), :] = uc[:, BODY]
            for ref, ghost, prev, keep, x, y in ((tb, tg, fpt, fxt, t, y_t), (sb, sg, fps, fxs, s, y_s)):
                x_e = jnp.concatenate([x, ghost[k, rows(r), :]], 1)
                fx = uc * (x_e + east(x_e))
                keep[k] = fx
                ref[k, rows(r, 8), :] = x - (0.5 * TIME_STEP) * (fx[:, BODY] + (y - south(y, prev[k])))
                prev[k] = y
        for k in range(NL):
            for ref, keep in ((tb, fxt), (sb, fxs)):
                x = ref[k, rows(r, 8), :] + (0.5 * TIME_STEP) * west(keep[k])[:, BODY]
                ref[k, rows(r, 8), :] = jnp.where(kc > k, x, ZERO)
        return 0

    def out_copy(i, c):
        src = (ub, vb, tb, sb)[i]
        dst = (u_o, v_o, t_o, s_o)[i]
        at = pl.ds(pl.multiple_of(c * CH, CH), CH)
        frm = pl.ds(pl.multiple_of(c * CH + (8 if i else 0), 8), CH)
        return pltpu.make_async_copy(src.at[:, frm, :], dst.at[:, at, :], out_sem.at[i, c])

    def advect_chunk(c, _):
        lax.fori_loop(c * (CH // 8), (c + 1) * (CH // 8), advect, 0)
        for i in range(4):
            out_copy(i, c).start()
        return 0

    lax.fori_loop(0, NCH, advect_chunk, 0)

    def drain(c, _):
        for i in range(4):
            out_copy(i, c).wait()
        return 0

    lax.fori_loop(0, NCH, drain, 0)
    for c in planes:
        c.wait()


def vmem(*shape):
    return pltpu.VMEM(shape, F32)


def solution(mesh):
    any_spec = pl.BlockSpec(memory_space=pl.ANY)
    cube = jax.ShapeDtypeStruct((NL, NR, NC), F32)
    plane = jax.ShapeDtypeStruct((NR, NC), F32)

    tile, ghost, strip = vmem(NR, 128), vmem(ER, 128), vmem(NL, 8, NC)

    def arr(*shape):
        return jax.ShapeDtypeStruct(shape, F32)

    def local_step(vel_u, vel_v, temperature, salinity, sea_level, trans_u, trans_v, bathymetry, kmt_levels, tide_force):
        mid = pl.pallas_call(
            predict_kernel,
            name="predict",
            out_shape=(
                cube, cube, cube, cube, arr(9, ER, EC), arr(NR, 128), arr(NR, 128), arr(48, NC), arr(48, NC), arr(24, NC),
            ),
            in_specs=[any_spec] * 9,
            out_specs=(any_spec,) * 10,
            scratch_shapes=[
                *([vmem(NL, NR + 16, NC)] * 3), *([vmem(NL, NR, NC)] * 4),
                vmem(9, ER, EC), pltpu.VMEM((NR, NC), jnp.int32), vmem(NR, NC),
                *([tile] * 3), *([ghost] * 3), *([vmem(NL, NR + 16, 128)] * 3), vmem(NL, 8, EC), tile, vmem(NR + 16, 128),
                vmem(48, NC), vmem(72, NC), vmem(48, NC), vmem(72, NC),
                tile, vmem(48, NC), vmem(48, NC), tile, vmem(24, NC), *([vmem(NL, 8, EC)] * 2), strip, vmem(4, NR, NC), vmem(2, NR, NC), strip, strip,
                pltpu.SemaphoreType.DMA((4, NCH)), pltpu.SemaphoreType.DMA((5,)), pltpu.SemaphoreType.DMA((4, NCH)),
                pltpu.SemaphoreType.DMA((2,)), pltpu.SemaphoreType.DMA((25,)), pltpu.SemaphoreType.DMA((25,)),
            ],
            compiler_params=pltpu.CompilerParams(collective_id=0, has_side_effects=True, vmem_limit_bytes=63 * 2**20),
        )(vel_u, vel_v, temperature, salinity, sea_level, trans_u, trans_v, bathymetry, kmt_levels)
        return pl.pallas_call(
            finish_kernel,
            name="finish",
            out_shape=(plane, plane, plane, cube, cube, cube, cube),
            in_specs=[pl.BlockSpec(memory_space=pltpu.SMEM)] + [any_spec] * 10,
            out_specs=(any_spec,) * 7,
            scratch_shapes=[
                vmem(NL, NR, NC), vmem(NL, NR + 8, NC), vmem(NL, NR + 16, NC), vmem(NL, NR + 16, NC),
                vmem(9, ER, EC), *([vmem(2, ER, EC)] * 3),
                vmem(NR, 128), vmem(NR, 128), vmem(48, NC), vmem(48, NC), vmem(24, NC), strip, strip,
                *([vmem(NL, 8, EC)] * 2), *([vmem(NL, NR, 128)] * 3),
                pltpu.SemaphoreType.DMA((4,)), pltpu.SemaphoreType.DMA((6,)), pltpu.SemaphoreType.DMA((4, NCH)),
                pltpu.SemaphoreType.DMA((3,)),
            ],
            compiler_params=pltpu.CompilerParams(vmem_limit_bytes=60 * 2**20),
        )(tide_force.T, *mid)

    spec_cube = P(None, "row", "col")
    spec_plane = P("row", "col")
    return jax.shard_map(
        local_step,
        mesh=mesh,
        in_specs=(spec_cube,) * 4 + (spec_plane,) * 5 + (P(None, None),),
        out_specs=(spec_plane,) * 3 + (spec_cube,) * 4,
        check_vma=False,
    )
```

```python
import functools

import jax
import jax.numpy as jnp
from jax import lax
from jax.experimental import pallas as pl
from jax.experimental.pallas import tpu as pltpu
from jax.sharding import PartitionSpec as P

TIME_STEP = 4.0
ALPHA_T = 0.02
BETA_S = 0.015
VISC_KV = 0.001
DIFF_KT = 0.0005

NL = 20
NSUB = 20
NR, NC = 128, 512
HR = 24
ER, EC = NR + 2 * HR, NC + 128
NCH = 8
CH = NR // NCH
STRIPS, PER, TILES = (n // 8 for n in (NR, CH, ER))
EARLY = NCH // 2
DTB = TIME_STEP / NSUB
F32 = jnp.float32
ZERO = 0.0
BODY = slice(0, NC)
LEFT = slice(0, 128)
RIGHT = slice(NC - 128, NC)
GHOST = slice(NC, EC)
KMT, DZ, ETA, TU, TV, FX, FY, SV, SU = range(9)
KU, KV, DU, DV = range(4)
WIDE = 42
MESH = pl.DeviceIdType.MESH


def loop(lo, hi, body):
    def step(i, carry):
        body(i)
        return carry

    lax.fori_loop(lo, hi, step, 0)


def rows(r, off=0):
    start = 8 * r + off
    if isinstance(start, int):
        return pl.ds(start, 8)
    return pl.ds(pl.multiple_of(start, 8), 8)


def iota(shape, axis):
    return lax.broadcasted_iota(jnp.int32, shape, axis)


def east(x):
    return pltpu.roll(x, x.shape[1] - 1, 1)


def west(x):
    return pltpu.roll(x, 1, 1)


def north(here, above):
    return pltpu.roll(jnp.where(iota(here.shape, 0) == 0, above, here), 7, 0)


def south(here, below):
    return pltpu.roll(jnp.where(iota(here.shape, 0) == 7, below, here), 1, 0)


def lane_tiles(x):
    return [x[:, 128 * c : 128 * (c + 1)] for c in range(NC // 128)]


def east_of(x, ghost):
    moved = [pltpu.roll(t, 127, 1) for t in lane_tiles(x)] + [ghost]
    last = iota((8, 128), 1) == 127
    return jnp.concatenate([jnp.where(last, b, a) for a, b in zip(moved, moved[1:])], 1)


def west_of(x, ghost):
    moved = [ghost] + [pltpu.roll(t, 1, 1) for t in lane_tiles(x)]
    first = iota((8, 128), 1) == 0
    return jnp.concatenate([jnp.where(first, a, b) for a, b in zip(moved, moved[1:])], 1)


def turn(x, by):
    return pltpu.roll(x, by % 128, 1)


def even_odd(a, b):
    return jnp.where(iota((8, 128), 1) % 2 == 0, a, b)


def lane_of(slot, k):
    return 2 * k + 40 * slot


def unpack(ghost, slot, k):
    shift = (128 - lane_of(slot, k)) % 128
    return pltpu.roll(ghost, shift, 1) if shift else ghost


def pack(tiles):
    lane = iota((8, 128), 1)
    acc = None
    first = None
    for slot, k, low, high in tiles:
        both = jnp.where(lane == 127, high, low)
        at = lane_of(slot, k)
        moved = pltpu.roll(both, at, 1) if at else both
        if acc is None:
            acc = moved
            if at == 0:
                first = moved
        else:
            acc = jnp.where(lane >= at - 1, moved, acc)
    if first is not None:
        acc = jnp.where(lane == 127, first, acc)
    return acc


def pack_wide(planes):
    lane = iota((8, 128), 1)
    acc = None
    for q, x in enumerate(planes):
        edge = jnp.where(lane < 64, x[:, LEFT], x[:, RIGHT])
        if acc is None:
            acc = edge
        else:
            acc = jnp.where(lane >= WIDE * q - WIDE // 2, pltpu.roll(edge, WIDE * q, 1), acc)
    if len(planes) == 1:
        return acc
    first = jnp.where(lane < 64, planes[0][:, LEFT], planes[0][:, RIGHT])
    return jnp.where(lane >= 128 - WIDE // 2, first, acc)


def unpack_wide(tile, q):
    lane = iota(tile.shape, 1)
    moved = pltpu.roll(tile, 128 - WIDE * q, 1) if q else tile
    return jnp.where((lane < WIDE // 2) | (lane >= 128 - WIDE // 2), moved, ZERO)


def solve(refs, masked, count, coef, gains, at):
    low = None
    rest = 1.0
    parts = [None] * len(refs)
    for k in range(NL):
        up = jnp.where(count > k + 1.0, coef, ZERO) if k < NL - 1 else ZERO
        inv = 1.0 / (rest + up)
        for i, ref in enumerate(refs):
            src = ref[k, at, :]
            if not masked:
                src = jnp.where(count > k, src, ZERO)
            parts[i] = src * inv if k == 0 else (src + low * parts[i]) * inv
            if k < NL - 1:
                ref[k, at, :] = parts[i]
        if k < NL - 1:
            gain = up * inv
            gains[k] = gain
            rest = 1.0 + gain * rest
        low = up
    for i, ref in enumerate(refs):
        ref[NL - 1, at, :] = parts[i]
    for k in range(NL - 2, -1, -1):
        gain = gains[k]
        for i, ref in enumerate(refs):
            parts[i] = ref[k, at, :] + gain * parts[i]
            ref[k, at, :] = parts[i]


def predict_kernel(
    u_h, v_h, t_h, s_h, eta_h, tu_h, tv_h, dep_h, kmt_h,
    su_o, sv_o, tm_o, sm_o, ext_o, gts_o, gu_o, grts_o, grtn_o, grv_o, sts_o,
    ub, vb, pb, tb, sb, su, sv, ext, ktmp, htmp, pa, pb_, pc, ga, gb, gc, pka, pkb, ga2, gb2, dup, sp, gx, prn, prs, grs, grn, sts, trn, trs, sug, vrn, fp, fsp, csp, geo, tot, gains, gains2,
    load_sem, small_sem, out_sem, outs_sem, send_sem, recv_sem,
):
    col = lax.axis_index("col")
    row = lax.axis_index("row")
    n_row = 8
    side = 1 - col
    up_row = lax.rem(row + 1, n_row)
    down_row = lax.rem(row + n_row - 1, n_row)
    to_x = {"col": side, "row": row}
    to_n = {"col": col, "row": up_row}
    to_s = {"col": col, "row": down_row}
    to_dn = {"col": side, "row": up_row}
    to_ds = {"col": side, "row": down_row}

    barrier = pltpu.get_barrier_semaphore()
    for dev in (to_x, to_n, to_s, to_dn, to_ds):
        pl.semaphore_signal(barrier, inc=1, device_id=dev, device_id_type=MESH)

    small = [
        pltpu.make_async_copy(kmt_h, ktmp, small_sem.at[0]),
        pltpu.make_async_copy(dep_h, htmp, small_sem.at[1]),
        pltpu.make_async_copy(eta_h, ext.at[2, pl.ds(HR, NR), pl.ds(0, NC)], small_sem.at[2]),
        pltpu.make_async_copy(tu_h, ext.at[3, pl.ds(HR, NR), pl.ds(0, NC)], small_sem.at[3]),
        pltpu.make_async_copy(tv_h, ext.at[4, pl.ds(HR, NR), pl.ds(0, NC)], small_sem.at[4]),
    ]
    for c in small:
        c.start()

    def load(i, c):
        src = (t_h, s_h, u_h, v_h)[i]
        dst = (tb, sb, ub, vb)[i]
        at = pl.ds(pl.multiple_of(c * CH, CH), CH)
        to = pl.ds(pl.multiple_of(c * CH + (8 if i >= 2 else 0), 8), CH)
        return pltpu.make_async_copy(src.at[:, at, :], dst.at[:, to, :], load_sem.at[i, c])

    def start_loads(pair):
        def body(c):
            for i in pair:
                load(i, c).start()

        loop(0, NCH, body)

    start_loads((0, 1))
    start_loads((2, 3))

    def send(src, dst, idx, dev):
        c = pltpu.make_async_remote_copy(
            src_ref=src, dst_ref=dst, send_sem=send_sem.at[idx], recv_sem=recv_sem.at[idx], device_id=dev, device_id_type=MESH
        )
        c.start()
        return c

    for c in small:
        c.wait()
    for r in range(STRIPS):
        kf = ktmp[rows(r), :].astype(F32)
        dz = htmp[rows(r), :] / jnp.maximum(kf, 1.0)
        ext[KMT, rows(r, HR), BODY] = kf
        ext[DZ, rows(r, HR), BODY] = dz
        eta, tu, tv = (ext[f, rows(r, HR), BODY] for f in (ETA, TU, TV))
        pa[rows(r), :] = pack_wide((kf, dz, eta))
        pb_[rows(r), :] = pack_wide((tu, tv))
    pl.semaphore_wait(barrier, 5)

    def send_ext(lo, n, tile, ghost, base):
        at = pl.ds(lo, n)
        low, high, mid = pl.ds(0, HR), pl.ds(HR + NR, HR), pl.ds(HR, NR)
        body = pl.ds(0, NC)
        return [
            send(tile, ghost.at[mid, :], base, to_x),
            send(ext.at[at, pl.ds(NR, HR), body], ext.at[at, low, body], base + 1, to_n),
            send(ext.at[at, pl.ds(HR, HR), body], ext.at[at, high, body], base + 2, to_s),
            send(tile.at[pl.ds(NR - HR, HR), :], ghost.at[low, :], base + 3, to_dn),
            send(tile.at[low, :], ghost.at[high, :], base + 4, to_ds),
        ]

    def receive_ext(copies, ghost, fields):
        for c in copies:
            c.wait()

        for q, f in enumerate(fields):
            ext[f, :, GHOST] = unpack_wide(ghost[...], q)

    first = send_ext(KMT, 3, pa, ga, 0)
    later = send_ext(TU, 2, pb_, gb, 5)

    def pressure(r):
        kc = ext[KMT, rows(r, HR), BODY]
        dz = ext[DZ, rows(r, HR), BODY]
        total = jnp.zeros((8, NC), F32)
        scale = TIME_STEP * dz
        for k in range(NL):
            half = (0.5 * BETA_S) * (sb[k, rows(r), :] - 1.0) - (0.5 * ALPHA_T) * (tb[k, rows(r), :] - 1.0)
            half = jnp.where(kc > k, half, ZERO)
            middle = total + half
            total = middle + half
            pb[k, rows(r, 8), :] = scale * middle

    def pressure_chunk(c):
        load(0, c).wait()
        load(1, c).wait()
        loop(c * (PER), (c + 1) * (PER), pressure)

    loop(0, NCH, pressure_chunk)

    def out_copy(i, c):
        src = (tb, sb, su, sv)[i]
        dst = (tm_o, sm_o, su_o, sv_o)[i]
        at = pl.ds(pl.multiple_of(c * CH, CH), CH)
        return pltpu.make_async_copy(src.at[:, at, :], dst.at[:, at, :], out_sem.at[i, c])

    def pack_ts(r):
        tiles = []
        for slot, ref in enumerate((tb, sb)):
            for k in range(NL):
                tiles.append((slot, k, ref[k, rows(r), LEFT], ref[k, rows(r), RIGHT]))
        sts[rows(r), :] = pack(tiles)

    def mix(r):
        pack_ts(jnp.maximum(r - 1, 0))
        kc = ext[KMT, rows(r, HR), BODY]
        dz = ext[DZ, rows(r, HR), BODY]
        solve((tb, sb), False, kc, (TIME_STEP * DIFF_KT) / (dz * dz), gains, rows(r))

    def mix_chunk(c):
        loop(c * (PER), (c + 1) * (PER), mix)
        out_copy(0, c).start()
        out_copy(1, c).start()

    loop(0, EARLY, mix_chunk)

    receive_ext(first, ga, (KMT, DZ, ETA))
    has_south = (row > 0).astype(F32)
    has_north = (row < n_row - 1).astype(F32)
    ext[KMT, 0:HR, :] = ext[KMT, 0:HR, :] * has_south
    ext[KMT, HR + NR :, :] = ext[KMT, HR + NR :, :] * has_north

    for r in range(STRIPS):
        at, above = rows(r, HR), rows(r, HR + 8)
        kc, dz = ext[KMT, at, :], ext[DZ, at, :]
        k_c, dz_c = kc[:, BODY], dz[:, BODY]
        geo[KU, rows(r), :] = jnp.minimum(k_c, east(kc)[:, BODY])
        geo[KV, rows(r), :] = jnp.minimum(k_c, north(k_c, ext[KMT, above, BODY]))
        geo[DU, rows(r), :] = 0.5 * (dz_c + east(dz)[:, BODY])
        geo[DV, rows(r), :] = 0.5 * (dz_c + north(dz_c, ext[DZ, above, BODY]))

    def pack_uvp(r):
        tiles = []
        for slot, ref in enumerate((ub, vb, pb)):
            for k in range(NL):
                x = [ref[k, rows(r, 8), LEFT], ref[k, rows(r, 8), RIGHT]]
                if slot < 2:
                    x = [jnp.where(geo[slot, rows(r), at] > k, t, ZERO) for t, at in zip(x, (LEFT, RIGHT))]
                tiles.append((slot, k, *x))
        sp[rows(r, 8), :] = pack(tiles)

    def pack_chunk(c):
        load(2, c).wait()
        load(3, c).wait()
        loop(c * (PER), (c + 1) * (PER), pack_uvp)

    loop(0, NCH, pack_chunk)

    def edge_row(dst, i, k, ref, at):
        dst[24 * i + k : 24 * i + k + 1, :] = ref[k, at : at + 1, :]

    def ghost_row(ref, k, at, src, i):
        ref[k, at : at + 1, :] = src[24 * i + k : 24 * i + k + 1, :]

    def masked_row(dst, i, k, ref, r):
        dst[24 * i + k : 24 * i + k + 1, :] = jnp.where(geo[i, r : r + 1, :] > k, ref[k, r + 8 : r + 9, :], ZERO)

    for k in range(NL):
        for i, ref in enumerate((ub, vb)):
            masked_row(prs, i, k, ref, 0)
            masked_row(prn, i, k, ref, NR - 1)
        edge_row(prs, 2, k, pb, 8)
    low, high = pl.ds(8, 8), pl.ds(NR, 8)
    second = [
        send(sp.at[pl.ds(8, NR), :], gx.at[pl.ds(8, NR), :], 10, to_x),
        send(prn, grs, 11, to_n),
        send(prs, grn, 12, to_s),
        send(sp.at[high, :], gx.at[pl.ds(0, 8), :], 13, to_dn),
        send(sp.at[low, :], gx.at[pl.ds(NR + 8, 8), :], 14, to_ds),
        send(sp.at[high, :], sp.at[pl.ds(0, 8), :], 25, to_n),
    ]

    def mask(r):
        for slot, ref in enumerate((ub, vb)):
            count = geo[slot, rows(r), :]
            total = jnp.zeros((8, NC), F32)
            for k in range(NL):
                x = jnp.where(count > k, ref[k, rows(r, 8), :], ZERO)
                ref[k, rows(r, 8), :] = x
                total = total + x
            tot[slot, rows(r), :] = total

    loop(0, STRIPS, mask)
    loop(EARLY, NCH, mix_chunk)
    pack_ts(STRIPS - 1)
    for k in range(NL):
        for i, ref in enumerate((tb, sb)):
            edge_row(trs, i, k, ref, 0)
            edge_row(trn, i, k, ref, NR - 1)
    third = [send(sts, gts_o, 15, to_x), send(trn, grts_o, 16, to_n), send(trs, grtn_o, 17, to_s)]

    for c in second:
        c.wait()

    corner_w = None
    for t in range(STRIPS + 1, 0, -1):
        g, own = gx[rows(t), :], sp[rows(t), :]
        g_s, own_s = south(g, gx[rows(t - 1), :]), south(own, sp[rows(t - 1), :])
        pka[rows(t - 1), :] = even_odd(turn(g, 1), turn(g_s, -41))
        flux = (turn(g_s, -39) + turn(own_s, -40)) * turn(g_s + g, 1)
        if corner_w is not None:
            d = own + turn(g, -1)
            pkb[rows(t - 1), :] = even_odd(north(flux, corner_w), d * d + turn(g, -81))
        corner_w = flux

    def spread(i):
        for j in range(4):
            at = rows(4 * i + j)
            a, b = pka[at, :], pkb[at, :]
            for k in range(NL):
                ga2[k, at, :] = unpack(a, 0, k)
                gb2[k, at, :] = unpack(b, 0, k)

    loop(0, STRIPS // 4, spread)
    for k in range(NL):
        for i, ref in enumerate((ub, vb)):
            ghost_row(ref, k, 7, grs, i)
        for i, ref in enumerate((ub, vb, pb)):
            ghost_row(ref, k, NR + 8, grn, i)

    def corner(r, k, ghost):
        u, v, p = (ref[k, rows(r, 8), :] for ref in (ub, vb, pb))
        u_s = south(u, ub[k, rows(r), :])
        v_s = south(v, vb[k, rows(r), :])
        f_s = (v_s + east_of(v_s, ghost)) * (u_s + u)
        c = v + v_s
        return u, p, f_s, c * c + p

    for k in range(NL):
        fsp[k], csp[k] = corner(STRIPS, k, unpack(pka[NR : NR + 8, :], 0, k))[2:]

    def tendency(i):
        r = STRIPS - 1 - i
        at = rows(r)
        for k in range(NL):
            ghost = ga2[k, at, :]
            u, p, f_s, c = corner(r, k, ghost)
            f = north(f_s, fsp[k])
            c_n = north(c, csp[k])
            fsp[k], csp[k] = f_s, c
            d = u + west_of(u, ghost)
            d = d * d + p
            fp[k], dup[k] = f, d
            su[k, at, :] = (f_s - f) + d
            sv[k, at, :] = (c - c_n) - f
        k_u, k_v = geo[KU, at, :], geo[KV, at, :]
        sum_u = sum_v = jnp.zeros((8, NC), F32)
        for k in range(NL):
            ghost = gb2[k, at, :]
            t_u = su[k, at, :] - east_of(dup[k], ghost)
            t_v = sv[k, at, :] + west_of(fp[k], ghost)
            u = jnp.where(k_u > k, ub[k, rows(r, 8), :] + t_u, ZERO)
            v = jnp.where(k_v > k, vb[k, rows(r, 8), :] + t_v, ZERO)
            su[k, at, :], sv[k, at, :] = u, v
            sum_u, sum_v = sum_u + u, sum_v + v
        dz_u, dz_v = geo[DU, at, :], geo[DV, at, :]
        ext[FX, rows(r, HR), BODY] = (dz_u / TIME_STEP) * (sum_u - tot[KU, at, :])
        ext[FY, rows(r, HR), BODY] = (dz_v / TIME_STEP) * (sum_v - tot[KV, at, :])
        ext[SU, rows(r, HR), BODY] = dz_u * sum_u
        ext[SV, rows(r, HR), BODY] = dz_v * sum_v

    loop(0, STRIPS, tendency)
    for r in range(STRIPS):
        pc[rows(r), :] = pack_wide([ext[f, rows(r, HR), BODY] for f in (FX, FY, SU)])
    fourth = send_ext(FX, 3, pc, gc, 18)
    receive_ext(later, gb, (TU, TV))
    out_ext0 = pltpu.make_async_copy(ext.at[pl.ds(0, 5)], ext_o.at[pl.ds(0, 5)], outs_sem.at[0])
    out_ext0.start()

    def implicit(i, ref, keep, r):
        dz = geo[DU + i, rows(r), :]
        solve((ref,), True, geo[i, rows(r), :], (TIME_STEP * VISC_KV) / (dz * dz), keep, rows(r))

    def pack_su(r):
        sug[rows(r), :] = pack([(0, k, su[k, rows(r), LEFT], su[k, rows(r), RIGHT]) for k in range(NL)])

    def solve_u(r):
        pack_su(jnp.maximum(r - 1, 0))
        implicit(0, su, gains, r)

    def solve_v(r):
        implicit(1, sv, gains2, r)

    def u_chunk(c):
        loop(c * (PER), (c + 1) * (PER), solve_u)
        out_copy(2, c).start()

    def v_chunk(c):
        loop(c * (PER), jnp.minimum((c + 1) * (PER), STRIPS - 1), solve_v)
        out_copy(3, c).start()

    solve_v(STRIPS - 1)
    loop(0, NCH, u_chunk)
    pack_su(STRIPS - 1)
    for k in range(NL):
        edge_row(vrn, 0, k, sv, NR - 1)
    fifth = [send(sug, gu_o, 23, to_x), send(vrn, grv_o, 24, to_n)]
    loop(0, NCH, v_chunk)
    receive_ext(fourth, gc, (FX, FY, SU))
    out_ext1 = pltpu.make_async_copy(ext.at[pl.ds(5, 4)], ext_o.at[pl.ds(5, 4)], outs_sem.at[1])
    out_ext1.start()
    out_sts = pltpu.make_async_copy(sts, sts_o, outs_sem.at[2])
    out_sts.start()

    def drain(c):
        for i in range(4):
            out_copy(i, c).wait()

    loop(0, NCH, drain)
    for c in third:
        c.wait()
    for c in fifth:
        c.wait()
    out_ext0.wait()
    out_ext1.wait()
    out_sts.wait()


def finish_kernel(
    tide, su_h, sv_h, tm_h, sm_h, ext_h, gts_h, gu_h, grts_h, grtn_h, grv_h, sts_h,
    eta_o, tu_o, tv_o, u_o, v_o, t_o, s_o,
    ub, vb, tb, sb, ext, cof, cnt, avg, gts, gu, grts, grtn, grv, sts, fpt, fps, fxt, fxs, pkt, tg, sg,
    load_sem, small_sem, out_sem, outs_sem,
):
    early = pltpu.make_async_copy(ext_h, ext, small_sem.at[0])
    early.start()
    small = [
        pltpu.make_async_copy(a, b, small_sem.at[i + 1])
        for i, (a, b) in enumerate(((gts_h, gts), (gu_h, gu), (grts_h, grts), (grtn_h, grtn), (grv_h, grv), (sts_h, sts)))
    ]
    for c in small:
        c.start()
    big = [
        pltpu.make_async_copy(su_h, ub, load_sem.at[0]),
        pltpu.make_async_copy(sv_h, vb.at[:, pl.ds(8, NR), :], load_sem.at[1]),
        pltpu.make_async_copy(tm_h, tb.at[:, pl.ds(8, NR), :], load_sem.at[2]),
        pltpu.make_async_copy(sm_h, sb.at[:, pl.ds(8, NR), :], load_sem.at[3]),
    ]
    for c in big:
        c.start()
    early.wait()

    def faces(at, above):
        kc, kn = ext[KMT, at, :], ext[KMT, above, :]
        dz, dn = ext[DZ, at, :], ext[DZ, above, :]
        k_u = jnp.minimum(kc, east(kc))
        k_v = jnp.minimum(kc, north(kc, kn))
        return kc, k_u, k_v, k_u * (0.5 * (dz + east(dz))), k_v * (0.5 * (dz + north(dz, dn)))

    for t in range(TILES):
        at = rows(t)
        kc, k_u, k_v, h_u, h_v = faces(at, rows(min(t + 1, TILES - 1)))
        for i, (count, h) in enumerate(((k_u, h_u), (k_v, h_v))):
            cof[i, at, :] = (DTB * DTB) * h
            cnt[i, at, :] = count
            ext[FX + i, at, :] = (DTB * DTB) * ext[FX + i, at, :]
            avg[i, at, :] = jnp.zeros((8, EC), F32)
        for f, count, scale in ((ETA, kc, 1.0), (TU, k_u, DTB), (TV, k_v, DTB)):
            ext[f, at, :] = jnp.where(count > ZERO, scale * ext[f, at, :], ZERO)

    norm = 6.0 / (NSUB * (NSUB + 1) * (NSUB + 2)) / DTB

    def subcycle(n, lo, hi):
        tide_x, tide_y = tide[0, n], tide[1, n]
        weight = norm * ((n + 1) * (NSUB - n)).astype(F32)
        v_prev = ext[TV, rows(max(lo - 1, 0)), :]
        eta_prev = None
        u_keep = v_keep = None
        for t in range(lo, hi + 1):
            if t < hi:
                at = rows(t)
                u, v = ext[TU, at, :], ext[TV, at, :]
                eta = ext[ETA, at, :] - ((u - west(u)) + (v - south(v, v_prev)))
                ext[ETA, at, :] = eta
            if t > lo:
                b = rows(t - 1)
                slope_x = east(eta_prev) - eta_prev
                slope_y = north(eta_prev, eta) - eta_prev
                u_new = u_keep + (cof[0, b, :] * (tide_x - slope_x) + ext[FX, b, :])
                v_new = v_keep + (cof[1, b, :] * (tide_y - slope_y) + ext[FY, b, :])
                ext[TU, b, :] = u_new
                ext[TV, b, :] = v_new
                if 2 <= t - 1 < 19:
                    avg[0, b, :] = avg[0, b, :] + weight * u_new
                    avg[1, b, :] = avg[1, b, :] + weight * v_new
            eta_prev, u_keep, v_keep, v_prev = eta, u, v, v

    tiles = TILES
    loop(0, 4, functools.partial(subcycle, lo=0, hi=tiles))
    loop(4, 12, functools.partial(subcycle, lo=1, hi=tiles - 1))
    loop(12, NSUB, functools.partial(subcycle, lo=2, hi=tiles - 2))

    for r in range(STRIPS):
        at = rows(r, HR)
        for f in (TU, TV):
            ext[f, at, :] = (1.0 / DTB) * ext[f, at, :]
    planes = [
        pltpu.make_async_copy(ext.at[2 + i, pl.ds(HR, NR), pl.ds(0, NC)], o, outs_sem.at[i])
        for i, o in enumerate((eta_o, tu_o, tv_o))
    ]
    for c in planes:
        c.start()
    for c in small:
        c.wait()
    for c in big:
        c.wait()
    for k in range(NL):
        vb[k, 7:8, :] = grv[k : k + 1, :]
        for i, ref in enumerate((tb, sb)):
            ref[k, 7:8, :] = grts[24 * i + k : 24 * i + k + 1, :]
            ref[k, NR + 8 : NR + 9, :] = grtn[24 * i + k : 24 * i + k + 1, :]

    for r in range(-1, STRIPS):
        at = rows(r, HR)
        for i, f in enumerate((SU, SV)):
            h = cof[i, at, :]
            avg[i, at, :] = (DTB * DTB) * (avg[i, at, :] - ext[f, at, :]) / jnp.where(h > ZERO, h, 1.0)

    def strip(r):
        at = rows(r, HR)
        return [x[at, BODY] for x in (ext.at[KMT], cnt.at[0], cnt.at[1], avg.at[0], avg.at[1])]

    def flux_y(r, k, k_v, d_v):
        vc = jnp.where(k_v > k, vb[k, rows(r, 8), :] + d_v, ZERO)
        out = [vc]
        for ref in (tb, sb):
            here = ref[k, rows(r, 8), :]
            out.append(here)
            out.append(vc * (here + north(here, ref[k, rows(r, 16), :])))
        return out

    _, _, k_v, _, d_v = strip(-1)
    for k in range(NL):
        _, _, a, _, b = flux_y(-1, k, k_v, d_v)
        fpt[k] = a
        fps[k] = b

    lane = iota((8, 128), 1)
    level = (((lane + 1) % 128) // 2).astype(F32)
    for r in range(STRIPS):
        at = rows(r, HR)
        count, add = (jnp.broadcast_to(x[0, at, EC - 1 : EC], (8, 128)) for x in (cnt, avg))
        uc = jnp.where(count > level, gu[rows(r), :] + add, ZERO)
        uc = jnp.where((lane < 39) | (lane == 127), uc, turn(uc, 40))
        g = gts[rows(r), :]
        pkt[rows(r), :] = even_odd(turn(uc * (g + turn(sts[rows(r), :], -1)), 1), turn(g, -1))

    def spread(i):
        for j in range(4):
            at = rows(4 * i + j)
            g = pkt[at, :]
            for k in range(NL):
                tg[k, at, :] = unpack(g, 0, k)
                sg[k, at, :] = unpack(g, 1, k)

    loop(0, STRIPS // 4, spread)

    def advect(r):
        kc, k_u, k_v, d_u, d_v = strip(r)
        for k in range(NL):
            vc, t, y_t, s, y_s = flux_y(r, k, k_v, d_v)
            vb[k, rows(r, 8), :] = vc
            uc = jnp.where(k_u > k, ub[k, rows(r), :] + d_u, ZERO)
            ub[k, rows(r), :] = uc
            for ref, ghost, prev, keep, x, y in ((tb, tg, fpt, fxt, t, y_t), (sb, sg, fps, fxs, s, y_s)):
                fx = uc * (x + east_of(x, ghost[k, rows(r), :]))
                keep[k] = fx
                ref[k, rows(r, 8), :] = x - (0.5 * TIME_STEP) * (fx + (y - south(y, prev[k])))
                prev[k] = y
        for k in range(NL):
            for ref, ghost, keep in ((tb, tg, fxt), (sb, sg, fxs)):
                x = ref[k, rows(r, 8), :] + (0.5 * TIME_STEP) * west_of(keep[k], ghost[k, rows(r), :])
                ref[k, rows(r, 8), :] = jnp.where(kc > k, x, ZERO)

    def out_copy(i, c):
        src = (ub, vb, tb, sb)[i]
        dst = (u_o, v_o, t_o, s_o)[i]
        at = pl.ds(pl.multiple_of(c * CH, CH), CH)
        frm = pl.ds(pl.multiple_of(c * CH + (8 if i else 0), 8), CH)
        return pltpu.make_async_copy(src.at[:, frm, :], dst.at[:, at, :], out_sem.at[i, c])

    def advect_chunk(c):
        loop(c * (PER), (c + 1) * (PER), advect)
        for i in range(4):
            out_copy(i, c).start()

    loop(0, NCH, advect_chunk)

    def drain(c):
        for i in range(4):
            out_copy(i, c).wait()

    loop(0, NCH, drain)
    for c in planes:
        c.wait()


def vmem(*shape):
    return pltpu.VMEM(shape, F32)


def solution(mesh):
    any_spec = pl.BlockSpec(memory_space=pl.ANY)
    cube = jax.ShapeDtypeStruct((NL, NR, NC), F32)
    plane = jax.ShapeDtypeStruct((NR, NC), F32)

    tile, ghost, strip = vmem(NR, 128), vmem(ER, 128), vmem(NL, 8, NC)

    def arr(*shape):
        return jax.ShapeDtypeStruct(shape, F32)

    def local_step(vel_u, vel_v, temperature, salinity, sea_level, trans_u, trans_v, bathymetry, kmt_levels, tide_force):
        mid = pl.pallas_call(
            predict_kernel,
            name="predict",
            out_shape=(
                cube, cube, cube, cube, arr(9, ER, EC), arr(NR, 128), arr(NR, 128), arr(48, NC), arr(48, NC), arr(24, NC),
                arr(NR, 128),
            ),
            in_specs=[any_spec] * 9,
            out_specs=(any_spec,) * 11,
            scratch_shapes=[
                *([vmem(NL, NR + 16, NC)] * 3), *([vmem(NL, NR, NC)] * 4),
                vmem(9, ER, EC), pltpu.VMEM((NR, NC), jnp.int32), vmem(NR, NC),
                *([tile] * 3), *([ghost] * 3), vmem(NR + 8, 128), tile, *([vmem(NL, NR, 128)] * 2), strip, *([vmem(NR + 16, 128)] * 2),
                vmem(48, NC), vmem(72, NC), vmem(48, NC), vmem(72, NC),
                tile, vmem(48, NC), vmem(48, NC), tile, vmem(24, NC), *([strip] * 3), vmem(4, NR, NC), vmem(2, NR, NC), strip, strip,
                pltpu.SemaphoreType.DMA((4, NCH)), pltpu.SemaphoreType.DMA((5,)), pltpu.SemaphoreType.DMA((4, NCH)),
                pltpu.SemaphoreType.DMA((3,)), pltpu.SemaphoreType.DMA((26,)), pltpu.SemaphoreType.DMA((26,)),
            ],
            compiler_params=pltpu.CompilerParams(collective_id=0, has_side_effects=True, vmem_limit_bytes=63 * 2**20),
        )(vel_u, vel_v, temperature, salinity, sea_level, trans_u, trans_v, bathymetry, kmt_levels)
        return pl.pallas_call(
            finish_kernel,
            name="finish",
            out_shape=(plane, plane, plane, cube, cube, cube, cube),
            in_specs=[pl.BlockSpec(memory_space=pltpu.SMEM)] + [any_spec] * 11,
            out_specs=(any_spec,) * 7,
            scratch_shapes=[
                vmem(NL, NR, NC), vmem(NL, NR + 8, NC), vmem(NL, NR + 16, NC), vmem(NL, NR + 16, NC),
                vmem(9, ER, EC), *([vmem(2, ER, EC)] * 3),
                vmem(NR, 128), vmem(NR, 128), vmem(48, NC), vmem(48, NC), vmem(24, NC), tile, *([strip] * 4), tile, *([vmem(NL, NR, 128)] * 2),
                pltpu.SemaphoreType.DMA((4,)), pltpu.SemaphoreType.DMA((7,)), pltpu.SemaphoreType.DMA((4, NCH)),
                pltpu.SemaphoreType.DMA((3,)),
            ],
            compiler_params=pltpu.CompilerParams(vmem_limit_bytes=60 * 2**20),
        )(tide_force.T, *mid)

    spec_cube = P(None, "row", "col")
    spec_plane = P("row", "col")
    return jax.shard_map(
        local_step,
        mesh=mesh,
        in_specs=(spec_cube,) * 4 + (spec_plane,) * 5 + (P(None, None),),
        out_specs=(spec_plane,) * 3 + (spec_cube,) * 4,
        check_vma=False,
    )
```

```python
import functools

import jax
import jax.numpy as jnp
from jax import lax
from jax.experimental import pallas as pl
from jax.experimental.pallas import tpu as pltpu
from jax.sharding import PartitionSpec as P

TIME_STEP = 4.0
ALPHA_T = 0.02
BETA_S = 0.015
VISC_KV = 0.001
DIFF_KT = 0.0005

NL = 20
NSUB = 20
NR, NC = 128, 512
HR = 24
ER, EC = NR + 2 * HR, NC + 128
NCH = 16
CH = NR // NCH
STRIPS, TILES = NR // 8, ER // 8
PAIR, TRIPLE = 2, 3
NORTH = 2 * PAIR
EARLY = 4
DTB = TIME_STEP / NSUB
HALF_DT = 0.5 * TIME_STEP
F32 = jnp.float32
ZERO = 0.0
BODY = slice(0, NC)
LEFT = slice(0, 128)
RIGHT = slice(NC - 128, NC)
GHOST = slice(NC, EC)
KMT, DZ, ETA, TU, TV, FX, FY, SV, SU = range(9)
KU, KV, DU, DV = range(4)
WIDE = 42
MESH = pl.DeviceIdType.MESH


def loop(lo, hi, body, per=1):
    def step(i, carry):
        for j in range(per):
            body(lo + per * i + j)
        return carry

    lax.fori_loop(0, (hi - lo) // per, step, 0)


def rows(r, off=0):
    start = 8 * r + off
    if isinstance(start, int):
        return pl.ds(start, 8)
    return pl.ds(pl.multiple_of(start, 8), 8)


def iota(shape, axis):
    return lax.broadcasted_iota(jnp.int32, shape, axis)


def east(x):
    return pltpu.roll(x, x.shape[1] - 1, 1)


def west(x):
    return pltpu.roll(x, 1, 1)


def north(here, above):
    return pltpu.roll(jnp.where(iota(here.shape, 0) == 0, above, here), 7, 0)


def south(here, below):
    return pltpu.roll(jnp.where(iota(here.shape, 0) == 7, below, here), 1, 0)


def lane_tiles(x):
    return [x[:, 128 * c : 128 * (c + 1)] for c in range(NC // 128)]


def east_of(x, ghost):
    moved = [pltpu.roll(t, 127, 1) for t in lane_tiles(x)] + [ghost]
    last = iota((8, 128), 1) == 127
    return jnp.concatenate([jnp.where(last, b, a) for a, b in zip(moved, moved[1:])], 1)


def west_of(x, ghost):
    moved = [ghost] + [pltpu.roll(t, 1, 1) for t in lane_tiles(x)]
    first = iota((8, 128), 1) == 0
    return jnp.concatenate([jnp.where(first, a, b) for a, b in zip(moved, moved[1:])], 1)


def turn(x, by):
    return pltpu.roll(x, by % 128, 1)


def even_odd(a, b):
    return jnp.where(iota((8, 128), 1) % 2 == 0, a, b)


def lane_of(slot, k):
    return 2 * k + 40 * slot


def unpack(ghost, slot, k):
    shift = (128 - lane_of(slot, k)) % 128
    return pltpu.roll(ghost, shift, 1) if shift else ghost


def pack(tiles):
    lane = iota((8, 128), 1)
    acc = None
    first = None
    for slot, k, low, high in tiles:
        both = jnp.where(lane == 127, high, low)
        at = lane_of(slot, k)
        moved = pltpu.roll(both, at, 1) if at else both
        if acc is None:
            acc = moved
            if at == 0:
                first = moved
        else:
            acc = jnp.where(lane >= at - 1, moved, acc)
    if first is not None:
        acc = jnp.where(lane == 127, first, acc)
    return acc


def pack_wide(planes):
    lane = iota((8, 128), 1)
    acc = None
    for q, x in enumerate(planes):
        edge = jnp.where(lane < 64, x[:, LEFT], x[:, RIGHT])
        if acc is None:
            acc = edge
        else:
            acc = jnp.where(lane >= WIDE * q - WIDE // 2, pltpu.roll(edge, WIDE * q, 1), acc)
    if len(planes) == 1:
        return acc
    first = jnp.where(lane < 64, planes[0][:, LEFT], planes[0][:, RIGHT])
    return jnp.where(lane >= 128 - WIDE // 2, first, acc)


def unpack_wide(tile, q):
    lane = iota(tile.shape, 1)
    moved = pltpu.roll(tile, 128 - WIDE * q, 1) if q else tile
    return jnp.where((lane < WIDE // 2) | (lane >= 128 - WIDE // 2), moved, ZERO)


def packed_lanes():
    lane = iota((8, 128), 1)
    in_first = (lane < 39) | (lane == 127)
    return lane, in_first, jnp.where(lane == 127, ZERO, (((lane + 1) % 40) // 2).astype(F32))


def solve(refs, masked, count, coef, gains, at):
    low = None
    rest = 1.0
    parts = [None] * len(refs)
    for k in range(NL):
        up = jnp.where(count > k + 1.0, coef, ZERO) if k < NL - 1 else ZERO
        inv = 1.0 / (rest + up)
        for i, ref in enumerate(refs):
            src = ref[k, at, :]
            if not masked:
                src = jnp.where(count > k, src, ZERO)
            parts[i] = src * inv if k == 0 else (src + low * parts[i]) * inv
            if k < NL - 1:
                ref[k, at, :] = parts[i]
        if k < NL - 1:
            gain = up * inv
            gains[k] = gain
            rest = 1.0 + gain * rest
        low = up
    for i, ref in enumerate(refs):
        ref[NL - 1, at, :] = parts[i]
    for k in range(NL - 2, -1, -1):
        gain = gains[k]
        for i, ref in enumerate(refs):
            parts[i] = ref[k, at, :] + gain * parts[i]
            ref[k, at, :] = parts[i]


def predict_kernel(
    u_h, v_h, t_h, s_h, eta_h, tu_h, tv_h, dep_h, kmt_h,
    su_o, sv_o, tm_o, sm_o, ext_o, gts_o, gu_o, grts_o, grtn_o, grv_o, sts_o,
    ub, vb, pb, tb, sb, su, sv, ext, ktmp, htmp, pa, pb_, pc, ga, gb, gc, pka, pkb, ga2, gb2, dup, sp, gx, prn, prs, grs, grn, sts, trn, trs, sug, vrn, fp, fsp, csp, geo, wet_g, wet_o, tot, gains, gains2,
    load_sem, small_sem, out_sem, outs_sem, send_sem, recv_sem,
):
    col = lax.axis_index("col")
    row = lax.axis_index("row")
    n_row = 8
    side = 1 - col
    up_row = lax.rem(row + 1, n_row)
    down_row = lax.rem(row + n_row - 1, n_row)
    to_x = {"col": side, "row": row}
    to_n = {"col": col, "row": up_row}
    to_s = {"col": col, "row": down_row}
    to_dn = {"col": side, "row": up_row}
    to_ds = {"col": side, "row": down_row}

    barrier = pltpu.get_barrier_semaphore()
    for dev in (to_x, to_n, to_s, to_dn, to_ds):
        pl.semaphore_signal(barrier, inc=1, device_id=dev, device_id_type=MESH)

    small = [
        pltpu.make_async_copy(kmt_h, ktmp, small_sem.at[0]),
        pltpu.make_async_copy(dep_h, htmp, small_sem.at[1]),
        pltpu.make_async_copy(eta_h, ext.at[2, pl.ds(HR, NR), pl.ds(0, NC)], small_sem.at[2]),
        pltpu.make_async_copy(tu_h, ext.at[3, pl.ds(HR, NR), pl.ds(0, NC)], small_sem.at[3]),
        pltpu.make_async_copy(tv_h, ext.at[4, pl.ds(HR, NR), pl.ds(0, NC)], small_sem.at[4]),
    ]
    for c in small:
        c.start()

    def load(i, c):
        src = (t_h, s_h, u_h, v_h)[i]
        dst = (tb, sb, ub, vb)[i]
        at = pl.ds(pl.multiple_of(c * CH, CH), CH)
        to = pl.ds(pl.multiple_of(c * CH + (8 if i >= 2 else 0), 8), CH)
        return pltpu.make_async_copy(src.at[:, at, :], dst.at[:, to, :], load_sem.at[i, c])

    def start_loads(pair):
        def body(c):
            for i in pair:
                load(i, c).start()

        loop(0, NCH, body)

    start_loads((0, 1))
    start_loads((2, 3))

    def send(src, dst, idx, dev):
        c = remote(src, dst, idx, dev)
        c.start()
        return c

    def remote(src, dst, idx, dev):
        return pltpu.make_async_remote_copy(
            src_ref=src, dst_ref=dst, send_sem=send_sem.at[idx], recv_sem=recv_sem.at[idx], device_id=dev, device_id_type=MESH
        )

    lane, in_first, level = packed_lanes()
    for c in small:
        c.wait()
    for r in range(STRIPS):
        kf = ktmp[rows(r), :].astype(F32)
        dz = htmp[rows(r), :] / jnp.maximum(kf, 1.0)
        ext[KMT, rows(r, HR), BODY] = kf
        ext[DZ, rows(r, HR), BODY] = dz
        eta, tu, tv = (ext[f, rows(r, HR), BODY] for f in (ETA, TU, TV))
        pa[rows(r), :] = pack_wide((kf, dz, eta))
        pb_[rows(r), :] = pack_wide((tu, tv))
    pl.semaphore_wait(barrier, 5)

    def start(copies):
        for c in copies:
            c.start()

    def send_ext(lo, n, tile, ghost, base):
        at = pl.ds(lo, n)
        low, high, mid = pl.ds(0, HR), pl.ds(HR + NR, HR), pl.ds(HR, NR)
        body = pl.ds(0, NC)
        parts = (
            (ext.at[at, pl.ds(NR, HR), body], ext.at[at, low, body], to_n),
            (tile.at[pl.ds(NR - HR, HR), :], ghost.at[low, :], to_dn),
            (tile, ghost.at[mid, :], to_x),
            (ext.at[at, pl.ds(HR, HR), body], ext.at[at, high, body], to_s),
            (tile.at[low, :], ghost.at[high, :], to_ds),
        )
        return [remote(a, b, base + i, dev) for i, (a, b, dev) in enumerate(parts)]

    def receive_ext(copies, ghost, fields):
        for c in copies:
            c.wait()

        for q, f in enumerate(fields):
            ext[f, :, GHOST] = unpack_wide(ghost[...], q)

    first = send_ext(KMT, 3, pa, ga, 0)
    start(first)

    def pressure(r):
        kc = ext[KMT, rows(r, HR), BODY]
        dz = ext[DZ, rows(r, HR), BODY]
        total = jnp.zeros((8, NC), F32)
        scale = TIME_STEP * dz
        for k in range(NL):
            half = (0.5 * BETA_S) * (sb[k, rows(r), :] - 1.0) - (0.5 * ALPHA_T) * (tb[k, rows(r), :] - 1.0)
            half = jnp.where(kc > k, half, ZERO)
            middle = total + half
            total = middle + half
            pb[k, rows(r, 8), :] = scale * middle

    def pressure_chunk(c):
        load(0, c).wait()
        load(1, c).wait()
        pressure(c)


    def out_copy(i, c):
        src = (tb, sb, su, sv)[i]
        dst = (tm_o, sm_o, su_o, sv_o)[i]
        at = pl.ds(pl.multiple_of(c * CH, CH), CH)
        return pltpu.make_async_copy(src.at[:, at, :], dst.at[:, at, :], out_sem.at[i, c])

    def pack_ts(r):
        tiles = []
        for slot, ref in enumerate((tb, sb)):
            for k in range(NL):
                tiles.append((slot, k, ref[k, rows(r), LEFT], ref[k, rows(r), RIGHT]))
        sts[rows(r), :] = pack(tiles)

    def mix(r):
        pack_ts(jnp.maximum(r - 1, 0))
        kc = ext[KMT, rows(r, HR), BODY]
        dz = ext[DZ, rows(r, HR), BODY]
        solve((tb, sb), False, kc, (TIME_STEP * DIFF_KT) / (dz * dz), gains, rows(r))

    def mix_chunk(c):
        mix(c)
        out_copy(0, c).start()
        out_copy(1, c).start()

    def both_chunk(c):
        pressure_chunk(c)
        mix_chunk(c)

    loop(0, EARLY, both_chunk, PAIR)
    loop(EARLY, NCH, pressure_chunk, PAIR)

    def pack_uvp(r):
        tiles = []
        for slot, ref in enumerate((ub, vb, pb)):
            for k in range(NL):
                x = [ref[k, rows(r, 8), LEFT], ref[k, rows(r, 8), RIGHT]]
                tiles.append((slot, k, *x))
        sp[rows(r, 8), :] = pack(tiles)

    def pack_chunk(c):
        load(2, c).wait()
        load(3, c).wait()
        pack_uvp(c)

    loop(0, NCH, pack_chunk, PAIR)

    def edge_row(dst, i, k, ref, at):
        dst[24 * i + k : 24 * i + k + 1, :] = ref[k, at : at + 1, :]

    def ghost_row(ref, k, at, src, i):
        x = src[24 * i + k : 24 * i + k + 1, :]
        ref[k, at : at + 1, :] = jnp.where(geo[i, at : at + 1, :] > k, x, ZERO) if i < 2 else x

    for k in range(NL):
        for i, ref in enumerate((ub, vb, pb)):
            edge_row(prs, i, k, ref, 8)
            if i < 2:
                edge_row(prn, i, k, ref, NR + 7)
    low, high = pl.ds(8, 8), pl.ds(NR, 8)
    second = [
        send(sp.at[pl.ds(8, NR), :], gx.at[pl.ds(8, NR), :], 10, to_x),
        send(prn, grs, 11, to_n),
        send(prs, grn, 12, to_s),
        send(sp.at[high, :], gx.at[pl.ds(0, 8), :], 13, to_dn),
        send(sp.at[low, :], gx.at[pl.ds(NR + 8, 8), :], 14, to_ds),
        send(sp.at[high, :], sp.at[pl.ds(0, 8), :], 25, to_n),
    ]

    later = send_ext(TU, 2, pb_, gb, 5)
    start(later)

    loop(EARLY, NCH, mix_chunk, PAIR)
    pack_ts(STRIPS - 1)
    for k in range(NL):
        for i, ref in enumerate((tb, sb)):
            edge_row(trs, i, k, ref, 0)
            edge_row(trn, i, k, ref, NR - 1)
    third = [send(sts, gts_o, 15, to_x), send(trn, grts_o, 16, to_n), send(trs, grtn_o, 17, to_s)]

    receive_ext(first, ga, (KMT, DZ, ETA))
    has_south = (row > 0).astype(F32)
    has_north = (row < n_row - 1).astype(F32)
    ext[KMT, 0:HR, :] = ext[KMT, 0:HR, :] * has_south
    ext[KMT, HR + NR :, :] = ext[KMT, HR + NR :, :] * has_north

    for r in range(-1, STRIPS + 1):
        at, above = rows(r, HR), rows(r, HR + 8)
        kc, dz = ext[KMT, at, :], ext[DZ, at, :]
        k_u = jnp.minimum(kc, east(kc))
        k_v = jnp.minimum(kc, north(kc, ext[KMT, above, :]))
        geo[KU, rows(r, 8), :] = k_u[:, BODY]
        geo[KV, rows(r, 8), :] = k_v[:, BODY]
        geo[DU, rows(r, 8), :] = 0.5 * (dz + east(dz))[:, BODY]
        geo[DV, rows(r, 8), :] = 0.5 * (dz + north(dz, ext[DZ, above, :]))[:, BODY]
        (u_w, u_e, u_l), (v_w, v_e, v_f) = (
            [jnp.broadcast_to(x[:, i : i + 1], (8, 128)) for i in at]
            for x, at in ((k_u, (EC - 1, NC, NC - 1)), (k_v, (EC - 1, NC, 0)))
        )
        top = jnp.where(lane < 2 * 40 - 1, even_odd(v_e, v_w), 1.0 * NL)
        wet_g[rows(r, 8), :] = jnp.where(in_first, even_odd(u_e, u_w), top)
        wet_o[rows(r, 8), :] = jnp.where(in_first, u_l, v_f)

    def mask(r):
        for slot, ref in enumerate((ub, vb)):
            count = geo[slot, rows(r, 8), :]
            total = jnp.zeros((8, NC), F32)
            for k in range(NL):
                x = jnp.where(count > k, ref[k, rows(r, 8), :], ZERO)
                ref[k, rows(r, 8), :] = x
                total = total + x
            tot[slot, rows(r), :] = total

    loop(0, STRIPS, mask, PAIR)
    for c in second:
        c.wait()

    def wet(x, count, t):
        return jnp.where(count[rows(t), :] > level, x[rows(t), :], ZERO)

    corner_w = None
    for t in range(STRIPS + 1, 0, -1):
        g, own, below = wet(gx, wet_g, t), wet(sp, wet_o, t), t - 1
        g_s, own_s = south(g, wet(gx, wet_g, below)), south(own, wet(sp, wet_o, below))
        pka[rows(t - 1), :] = even_odd(turn(g, 1), turn(g_s, -41))
        flux = (turn(g_s, -39) + turn(own_s, -40)) * turn(g_s + g, 1)
        if corner_w is not None:
            d = own + turn(g, -1)
            pkb[rows(t - 1), :] = even_odd(north(flux, corner_w), d * d + turn(g, -81))
        corner_w = flux

    def spread(i):
        for j in range(4):
            at = rows(4 * i + j)
            a, b = pka[at, :], pkb[at, :]
            for k in range(NL):
                ga2[k, at, :] = unpack(a, 0, k)
                gb2[k, at, :] = unpack(b, 0, k)

    loop(0, STRIPS // 4, spread)
    for k in range(NL):
        for i, ref in enumerate((ub, vb)):
            ghost_row(ref, k, 7, grs, i)
        for i, ref in enumerate((ub, vb, pb)):
            ghost_row(ref, k, NR + 8, grn, i)

    def corner(r, k, ghost):
        u, v, p = (ref[k, rows(r, 8), :] for ref in (ub, vb, pb))
        u_s = south(u, ub[k, rows(r), :])
        v_s = south(v, vb[k, rows(r), :])
        f_s = (v_s + east_of(v_s, ghost)) * (u_s + u)
        c = v + v_s
        return u, p, f_s, c * c + p

    for k in range(NL):
        fsp[k], csp[k] = corner(STRIPS, k, unpack(pka[NR : NR + 8, :], 0, k))[2:]

    def tendency(i):
        r = STRIPS - 1 - i
        at = rows(r)
        for k in range(NL):
            ghost = ga2[k, at, :]
            u, p, f_s, c = corner(r, k, ghost)
            f = north(f_s, fsp[k])
            c_n = north(c, csp[k])
            fsp[k], csp[k] = f_s, c
            d = u + west_of(u, ghost)
            d = d * d + p
            fp[k], dup[k] = f, d
            su[k, at, :] = (f_s - f) + d
            sv[k, at, :] = (c - c_n) - f
        k_u, k_v, dz_u, dz_v = (geo[i, rows(r, 8), :] for i in (KU, KV, DU, DV))
        sum_u = sum_v = jnp.zeros((8, NC), F32)
        for k in range(NL):
            ghost = gb2[k, at, :]
            t_u = su[k, at, :] - east_of(dup[k], ghost)
            t_v = sv[k, at, :] + west_of(fp[k], ghost)
            u = jnp.where(k_u > k, ub[k, rows(r, 8), :] + t_u, ZERO)
            v = jnp.where(k_v > k, vb[k, rows(r, 8), :] + t_v, ZERO)
            su[k, at, :], sv[k, at, :] = u, v
            sum_u, sum_v = sum_u + u, sum_v + v
        ext[FX, rows(r, HR), BODY] = (dz_u / TIME_STEP) * (sum_u - tot[KU, at, :])
        ext[FY, rows(r, HR), BODY] = (dz_v / TIME_STEP) * (sum_v - tot[KV, at, :])
        ext[SU, rows(r, HR), BODY] = dz_u * sum_u
        ext[SV, rows(r, HR), BODY] = dz_v * sum_v

    def pack_forcing(lo, hi):
        for r in range(lo, hi):
            pc[rows(r), :] = pack_wide([ext[f, rows(r, HR), BODY] for f in (FX, FY, SU)])

    fourth = send_ext(FX, 3, pc, gc, 18)

    def leave_north():
        pack_forcing(STRIPS - NORTH, STRIPS)
        start(fourth[:2])

    def tendency_pair(i):
        for j in range(PAIR):
            tendency(PAIR * i + j)
        pl.when(i == NORTH // PAIR - 1)(leave_north)

    loop(0, STRIPS // PAIR, tendency_pair)
    pack_forcing(0, STRIPS - NORTH)
    start(fourth[2:])
    receive_ext(later, gb, (TU, TV))
    out_ext0 = pltpu.make_async_copy(ext.at[pl.ds(0, 5)], ext_o.at[pl.ds(0, 5)], outs_sem.at[0])
    out_ext0.start()

    def implicit(i, ref, keep, r):
        dz = geo[DU + i, rows(r, 8), :]
        solve((ref,), True, geo[i, rows(r, 8), :], (TIME_STEP * VISC_KV) / (dz * dz), keep, rows(r))

    def pack_su(r):
        sug[rows(r), :] = pack([(0, k, su[k, rows(r), LEFT], su[k, rows(r), RIGHT]) for k in range(NL)])

    def solve_u(r):
        pack_su(jnp.maximum(r - 1, 0))
        implicit(0, su, gains, r)

    def solve_v(r):
        implicit(1, sv, gains2, r)

    def u_chunk(c):
        solve_u(c)
        out_copy(2, c).start()

    def v_chunk(c):
        solve_v(c)
        out_copy(3, c).start()

    v_chunk(NCH - 1)
    loop(0, NCH, u_chunk, PAIR)
    pack_su(STRIPS - 1)
    for k in range(NL):
        edge_row(vrn, 0, k, sv, NR - 1)
    fifth = [send(sug, gu_o, 23, to_x), send(vrn, grv_o, 24, to_n)]
    out_ext1 = pltpu.make_async_copy(ext.at[pl.ds(5, 4)], ext_o.at[pl.ds(5, 4)], outs_sem.at[1])

    def take_forcing():
        receive_ext(fourth, gc, (FX, FY, SU))
        out_ext1.start()

    def v_triple(i):
        for j in range(TRIPLE):
            v_chunk(TRIPLE * i + j)
        pl.when(i == TRIPLE - 1)(take_forcing)

    loop(0, STRIPS // TRIPLE, v_triple)
    out_sts = pltpu.make_async_copy(sts, sts_o, outs_sem.at[2])
    out_sts.start()

    def drain(c):
        for i in range(4):
            out_copy(i, c).wait()

    loop(0, NCH, drain)
    for c in third:
        c.wait()
    for c in fifth:
        c.wait()
    out_ext0.wait()
    out_ext1.wait()
    out_sts.wait()


def finish_kernel(
    tide, su_h, sv_h, tm_h, sm_h, ext_h, gts_h, gu_h, grts_h, grtn_h, grv_h, sts_h,
    eta_o, tu_o, tv_o, u_o, v_o, t_o, s_o,
    ub, vb, tb, sb, ext, cof, cnt, avg, gts, gu, grts, grtn, grv, sts, fpt, fps, fxt, fxs, pkt, tg, sg,
    load_sem, small_sem, out_sem, outs_sem,
):
    early, late = (
        pltpu.make_async_copy(ext_h.at[at], ext.at[at], small_sem.at[i])
        for i, at in enumerate((pl.ds(KMT, SV), pl.ds(SV, 2)))
    )
    early.start()
    small = [
        pltpu.make_async_copy(a, b, small_sem.at[i + 2])
        for i, (a, b) in enumerate(((gts_h, gts), (gu_h, gu), (grts_h, grts), (grtn_h, grtn), (grv_h, grv), (sts_h, sts)))
    ]
    late.start()
    for c in small:
        c.start()
    big = [
        pltpu.make_async_copy(su_h, ub, load_sem.at[0]),
        pltpu.make_async_copy(sv_h, vb.at[:, pl.ds(8, NR), :], load_sem.at[1]),
        pltpu.make_async_copy(tm_h, tb.at[:, pl.ds(8, NR), :], load_sem.at[2]),
        pltpu.make_async_copy(sm_h, sb.at[:, pl.ds(8, NR), :], load_sem.at[3]),
    ]
    for c in big:
        c.start()
    early.wait()

    def faces(at, above):
        kc, kn = ext[KMT, at, :], ext[KMT, above, :]
        dz, dn = ext[DZ, at, :], ext[DZ, above, :]
        k_u = jnp.minimum(kc, east(kc))
        k_v = jnp.minimum(kc, north(kc, kn))
        return kc, k_u, k_v, k_u * (0.5 * (dz + east(dz))), k_v * (0.5 * (dz + north(dz, dn)))

    for t in range(TILES):
        at = rows(t)
        kc, k_u, k_v, h_u, h_v = faces(at, rows(min(t + 1, TILES - 1)))
        for i, (count, h) in enumerate(((k_u, h_u), (k_v, h_v))):
            cof[i, at, :] = (DTB * DTB) * h
            cnt[i, at, :] = count
            ext[FX + i, at, :] = (DTB * DTB) * ext[FX + i, at, :]
            avg[i, at, :] = jnp.zeros((8, EC), F32)
        for f, count, scale in ((ETA, kc, 1.0), (TU, k_u, DTB), (TV, k_v, DTB)):
            ext[f, at, :] = jnp.where(count > ZERO, scale * ext[f, at, :], ZERO)

    norm = 6.0 / (NSUB * (NSUB + 1) * (NSUB + 2)) / DTB

    def subcycle(n, lo, hi):
        tide_x, tide_y = tide[0, n], tide[1, n]
        weight = norm * ((n + 1) * (NSUB - n)).astype(F32)
        v_prev = ext[TV, rows(max(lo - 1, 0)), :]
        eta_prev = None
        u_keep = v_keep = None
        for t in range(lo, hi + 1):
            if t < hi:
                at = rows(t)
                u, v = ext[TU, at, :], ext[TV, at, :]
                eta = ext[ETA, at, :] - ((u - west(u)) + (v - south(v, v_prev)))
                ext[ETA, at, :] = eta
            if t > lo:
                b = rows(t - 1)
                slope_x = east(eta_prev) - eta_prev
                slope_y = north(eta_prev, eta) - eta_prev
                u_new = u_keep + (cof[0, b, :] * (tide_x - slope_x) + ext[FX, b, :])
                v_new = v_keep + (cof[1, b, :] * (tide_y - slope_y) + ext[FY, b, :])
                ext[TU, b, :] = u_new
                ext[TV, b, :] = v_new
                if 2 <= t - 1 < 19:
                    avg[0, b, :] = avg[0, b, :] + weight * u_new
                    avg[1, b, :] = avg[1, b, :] + weight * v_new
            eta_prev, u_keep, v_keep, v_prev = eta, u, v, v

    tiles = TILES
    loop(0, 4, functools.partial(subcycle, lo=0, hi=tiles))
    loop(4, 12, functools.partial(subcycle, lo=1, hi=tiles - 1))
    loop(12, NSUB, functools.partial(subcycle, lo=2, hi=tiles - 2))

    for r in range(STRIPS):
        at = rows(r, HR)
        for f in (TU, TV):
            ext[f, at, :] = (1.0 / DTB) * ext[f, at, :]
    planes = [
        pltpu.make_async_copy(ext.at[2 + i, pl.ds(HR, NR), pl.ds(0, NC)], o, outs_sem.at[i])
        for i, o in enumerate((eta_o, tu_o, tv_o))
    ]
    for c in planes:
        c.start()
    late.wait()
    for c in small:
        c.wait()
    for c in big:
        c.wait()
    for k in range(NL):
        vb[k, 7:8, :] = grv[k : k + 1, :]
        for i, ref in enumerate((tb, sb)):
            ref[k, 7:8, :] = grts[24 * i + k : 24 * i + k + 1, :]
            ref[k, NR + 8 : NR + 9, :] = grtn[24 * i + k : 24 * i + k + 1, :]

    for r in range(-1, STRIPS):
        at = rows(r, HR)
        for i, f in enumerate((SU, SV)):
            h = cof[i, at, :]
            avg[i, at, :] = (DTB * DTB) * (avg[i, at, :] - ext[f, at, :]) / jnp.where(h > ZERO, h, 1.0)

    def strip(r):
        at = rows(r, HR)
        return [x[at, BODY] for x in (ext.at[KMT], cnt.at[0], cnt.at[1], avg.at[0], avg.at[1])]

    def flux_y(r, k, k_v, d_v):
        vc = jnp.where(k_v > k, vb[k, rows(r, 8), :] + d_v, ZERO)
        out = [vc]
        for ref in (tb, sb):
            here = ref[k, rows(r, 8), :]
            out.append(here)
            out.append(vc * (here + north(here, ref[k, rows(r, 16), :])))
        return out

    _, _, k_v, _, d_v = strip(-1)
    for k in range(NL):
        _, _, a, _, b = flux_y(-1, k, k_v, d_v)
        fpt[k] = a
        fps[k] = b

    _, in_first, level = packed_lanes()
    for r in range(STRIPS):
        at = rows(r, HR)
        count, add = (jnp.broadcast_to(x[0, at, EC - 1 : EC], (8, 128)) for x in (cnt, avg))
        uc = jnp.where(count > level, gu[rows(r), :] + add, ZERO)
        uc = jnp.where(in_first, uc, turn(uc, 40))
        g = gts[rows(r), :]
        pkt[rows(r), :] = even_odd(turn(uc * (g + turn(sts[rows(r), :], -1)), 1), turn(g, -1))

    def spread(i):
        for j in range(4):
            at = rows(4 * i + j)
            g = pkt[at, :]
            for k in range(NL):
                tg[k, at, :] = unpack(g, 0, k)
                sg[k, at, :] = unpack(g, 1, k)

    loop(0, STRIPS // 4, spread)

    def advect(r):
        kc, k_u, k_v, d_u, d_v = strip(r)
        for k in range(NL):
            vc, t, y_t, s, y_s = flux_y(r, k, k_v, d_v)
            vb[k, rows(r, 8), :] = vc
            uc = jnp.where(k_u > k, ub[k, rows(r), :] + d_u, ZERO)
            ub[k, rows(r), :] = uc
            for ref, ghost, prev, keep, x, y in ((tb, tg, fpt, fxt, t, y_t), (sb, sg, fps, fxs, s, y_s)):
                fx = uc * (x + east_of(x, ghost[k, rows(r), :]))
                keep[k] = fx
                ref[k, rows(r, 8), :] = x - HALF_DT * (fx + (y - south(y, prev[k])))
                prev[k] = y
        for k in range(NL):
            for ref, ghost, keep in ((tb, tg, fxt), (sb, sg, fxs)):
                x = ref[k, rows(r, 8), :] + HALF_DT * west_of(keep[k], ghost[k, rows(r), :])
                ref[k, rows(r, 8), :] = jnp.where(kc > k, x, ZERO)

    def out_copy(i, c):
        src = (ub, vb, tb, sb)[i]
        dst = (u_o, v_o, t_o, s_o)[i]
        at = pl.ds(pl.multiple_of(c * CH, CH), CH)
        frm = pl.ds(pl.multiple_of(c * CH + (8 if i else 0), 8), CH)
        return pltpu.make_async_copy(src.at[:, frm, :], dst.at[:, at, :], out_sem.at[i, c])

    def advect_chunk(c):
        advect(c)
        for i in range(4):
            out_copy(i, c).start()

    loop(0, NCH, advect_chunk, PAIR)

    def drain(c):
        for i in range(4):
            out_copy(i, c).wait()

    loop(0, NCH, drain)
    for c in planes:
        c.wait()


def vmem(*shape):
    return pltpu.VMEM(shape, F32)


def solution(mesh):
    any_spec = pl.BlockSpec(memory_space=pl.ANY)
    cube = jax.ShapeDtypeStruct((NL, NR, NC), F32)
    plane = jax.ShapeDtypeStruct((NR, NC), F32)

    tile, ghost, strip = vmem(NR, 128), vmem(ER, 128), vmem(NL, 8, NC)

    def arr(*shape):
        return jax.ShapeDtypeStruct(shape, F32)

    def local_step(vel_u, vel_v, temperature, salinity, sea_level, trans_u, trans_v, bathymetry, kmt_levels, tide_force):
        mid = pl.pallas_call(
            predict_kernel,
            name="predict",
            out_shape=(
                cube, cube, cube, cube, arr(9, ER, EC), arr(NR, 128), arr(NR, 128), arr(48, NC), arr(48, NC), arr(24, NC),
                arr(NR, 128),
            ),
            in_specs=[any_spec] * 9,
            out_specs=(any_spec,) * 11,
            scratch_shapes=[
                *([vmem(NL, NR + 16, NC)] * 3), *([vmem(NL, NR, NC)] * 4),
                vmem(9, ER, EC), pltpu.VMEM((NR, NC), jnp.int32), vmem(NR, NC),
                *([tile] * 3), *([ghost] * 3), vmem(NR + 8, 128), tile, *([vmem(NL, NR, 128)] * 2), strip, *([vmem(NR + 16, 128)] * 2),
                vmem(48, NC), vmem(72, NC), vmem(48, NC), vmem(72, NC),
                tile, vmem(48, NC), vmem(48, NC), tile, vmem(24, NC), *([strip] * 3), vmem(4, NR + 16, NC), *([vmem(NR + 16, 128)] * 2), vmem(2, NR, NC), strip, strip,
                pltpu.SemaphoreType.DMA((4, NCH)), pltpu.SemaphoreType.DMA((5,)), pltpu.SemaphoreType.DMA((4, NCH)),
                pltpu.SemaphoreType.DMA((3,)), pltpu.SemaphoreType.DMA((26,)), pltpu.SemaphoreType.DMA((26,)),
            ],
            compiler_params=pltpu.CompilerParams(collective_id=0, has_side_effects=True, vmem_limit_bytes=63 * 2**20),
        )(vel_u, vel_v, temperature, salinity, sea_level, trans_u, trans_v, bathymetry, kmt_levels)
        return pl.pallas_call(
            finish_kernel,
            name="finish",
            out_shape=(plane, plane, plane, cube, cube, cube, cube),
            in_specs=[pl.BlockSpec(memory_space=pltpu.SMEM)] + [any_spec] * 11,
            out_specs=(any_spec,) * 7,
            scratch_shapes=[
                vmem(NL, NR, NC), vmem(NL, NR + 8, NC), vmem(NL, NR + 16, NC), vmem(NL, NR + 16, NC),
                vmem(9, ER, EC), *([vmem(2, ER, EC)] * 3),
                vmem(NR, 128), vmem(NR, 128), vmem(48, NC), vmem(48, NC), vmem(24, NC), tile, *([strip] * 4), tile, *([vmem(NL, NR, 128)] * 2),
                pltpu.SemaphoreType.DMA((4,)), pltpu.SemaphoreType.DMA((8,)), pltpu.SemaphoreType.DMA((4, NCH)),
                pltpu.SemaphoreType.DMA((3,)),
            ],
            compiler_params=pltpu.CompilerParams(vmem_limit_bytes=60 * 2**20),
        )(tide_force.T, *mid)

    spec_cube = P(None, "row", "col")
    spec_plane = P("row", "col")
    return jax.shard_map(
        local_step,
        mesh=mesh,
        in_specs=(spec_cube,) * 4 + (spec_plane,) * 5 + (P(None, None),),
        out_specs=(spec_plane,) * 3 + (spec_cube,) * 4,
        check_vma=False,
    )
```

```python
import functools

import jax
import jax.numpy as jnp
from jax import lax
from jax.experimental import pallas as pl
from jax.experimental.pallas import tpu as pltpu
from jax.sharding import PartitionSpec as P

TIME_STEP = 4.0
ALPHA_T = 0.02
BETA_S = 0.015
VISC_KV = 0.001
DIFF_KT = 0.0005

NL = 20
NSUB = 20
NR, NC = 128, 512
HR = 24
ER, EC = NR + 2 * HR, NC + 128
NCH = 16
CH = NR // NCH
STRIPS, TILES = NR // 8, ER // 8
PAIR, TRIPLE = 2, 3
NORTH = 2 * PAIR
EARLY = 4
DTB = TIME_STEP / NSUB
HALF_DT = 0.5 * TIME_STEP
F32 = jnp.float32
ZERO = 0.0
BODY = slice(0, NC)
LEFT = slice(0, 128)
RIGHT = slice(NC - 128, NC)
GHOST = slice(NC, EC)
KMT, DZ, ETA, TU, TV, FX, FY, SV, SU = range(9)
KU, KV, DU, DV = range(4)
WIDE = 42
MESH = pl.DeviceIdType.MESH


def loop(lo, hi, body, per=1):
    def step(i, carry):
        for j in range(per):
            body(lo + per * i + j)
        return carry

    lax.fori_loop(0, (hi - lo) // per, step, 0)


def rows(r, off=0):
    start = 8 * r + off
    if isinstance(start, int):
        return pl.ds(start, 8)
    return pl.ds(pl.multiple_of(start, 8), 8)


def iota(shape, axis):
    return lax.broadcasted_iota(jnp.int32, shape, axis)


def east(x):
    return pltpu.roll(x, x.shape[1] - 1, 1)


def west(x):
    return pltpu.roll(x, 1, 1)


def north(here, above):
    return pltpu.roll(jnp.where(iota(here.shape, 0) == 0, above, here), 7, 0)


def south(here, below):
    return pltpu.roll(jnp.where(iota(here.shape, 0) == 7, below, here), 1, 0)


def lane_tiles(x):
    return [x[:, 128 * c : 128 * (c + 1)] for c in range(NC // 128)]


def east_of(x, ghost):
    moved = [pltpu.roll(t, 127, 1) for t in lane_tiles(x)] + [ghost]
    last = iota((8, 128), 1) == 127
    return jnp.concatenate([jnp.where(last, b, a) for a, b in zip(moved, moved[1:])], 1)


def west_of(x, ghost):
    moved = [ghost] + [pltpu.roll(t, 1, 1) for t in lane_tiles(x)]
    first = iota((8, 128), 1) == 0
    return jnp.concatenate([jnp.where(first, a, b) for a, b in zip(moved, moved[1:])], 1)


def turn(x, by):
    return pltpu.roll(x, by % 128, 1)


def even_odd(a, b):
    return jnp.where(iota((8, 128), 1) % 2 == 0, a, b)


def lane_of(slot, k):
    return 2 * k + 40 * slot


def unpack(ghost, slot, k):
    shift = (128 - lane_of(slot, k)) % 128
    return pltpu.roll(ghost, shift, 1) if shift else ghost


def pack(tiles):
    lane = iota((8, 128), 1)
    acc = None
    first = None
    for slot, k, low, high in tiles:
        both = jnp.where(lane == 127, high, low)
        at = lane_of(slot, k)
        moved = pltpu.roll(both, at, 1) if at else both
        if acc is None:
            acc = moved
            if at == 0:
                first = moved
        else:
            acc = jnp.where(lane >= at - 1, moved, acc)
    if first is not None:
        acc = jnp.where(lane == 127, first, acc)
    return acc


def pack_wide(planes):
    lane = iota((8, 128), 1)
    acc = None
    for q, x in enumerate(planes):
        edge = jnp.where(lane < 64, x[:, LEFT], x[:, RIGHT])
        if acc is None:
            acc = edge
        else:
            acc = jnp.where(lane >= WIDE * q - WIDE // 2, pltpu.roll(edge, WIDE * q, 1), acc)
    if len(planes) == 1:
        return acc
    first = jnp.where(lane < 64, planes[0][:, LEFT], planes[0][:, RIGHT])
    return jnp.where(lane >= 128 - WIDE // 2, first, acc)


def unpack_wide(tile, q):
    lane = iota(tile.shape, 1)
    moved = pltpu.roll(tile, 128 - WIDE * q, 1) if q else tile
    return jnp.where((lane < WIDE // 2) | (lane >= 128 - WIDE // 2), moved, ZERO)


def packed_lanes():
    lane = iota((8, 128), 1)
    in_first = (lane < 39) | (lane == 127)
    return lane, in_first, jnp.where(lane == 127, ZERO, (((lane + 1) % 40) // 2).astype(F32))


def solve(refs, masked, count, coef, gains, at):
    low = None
    rest = 1.0
    parts = [None] * len(refs)
    for k in range(NL):
        up = jnp.where(count > k + 1.0, coef, ZERO) if k < NL - 1 else ZERO
        inv = 1.0 / (rest + up)
        for i, ref in enumerate(refs):
            src = ref[k, at, :]
            if not masked:
                src = jnp.where(count > k, src, ZERO)
            parts[i] = src * inv if k == 0 else (src + low * parts[i]) * inv
            if k < NL - 1:
                ref[k, at, :] = parts[i]
        if k < NL - 1:
            gain = up * inv
            gains[k] = gain
            rest = 1.0 + gain * rest
        low = up
    for i, ref in enumerate(refs):
        ref[NL - 1, at, :] = parts[i]
    for k in range(NL - 2, -1, -1):
        gain = gains[k]
        for i, ref in enumerate(refs):
            parts[i] = ref[k, at, :] + gain * parts[i]
            ref[k, at, :] = parts[i]


def predict_kernel(
    u_h, v_h, t_h, s_h, eta_h, tu_h, tv_h, dep_h, kmt_h,
    su_o, sv_o, tm_o, sm_o, ext_o, gts_o, gu_o, grts_o, grtn_o, grv_o, sts_o,
    ub, vb, pb, tb, sb, su, sv, ext, ktmp, htmp, pa, pb_, pc, ga, gb, gc, pka, pkb, dup, sp, gx, prn, prs, grs, grn, sts, trn, trs, sug, vrn, fp, fsp, csp, geo, wet_g, wet_o, tot, gains, gains2,
    load_sem, small_sem, out_sem, outs_sem, send_sem, recv_sem,
):
    col = lax.axis_index("col")
    row = lax.axis_index("row")
    n_row = 8
    side = 1 - col
    up_row = lax.rem(row + 1, n_row)
    down_row = lax.rem(row + n_row - 1, n_row)
    to_x = {"col": side, "row": row}
    to_n = {"col": col, "row": up_row}
    to_s = {"col": col, "row": down_row}
    to_dn = {"col": side, "row": up_row}
    to_ds = {"col": side, "row": down_row}

    barrier = pltpu.get_barrier_semaphore()
    for dev in (to_x, to_n, to_s, to_dn, to_ds):
        pl.semaphore_signal(barrier, inc=1, device_id=dev, device_id_type=MESH)

    small = [
        pltpu.make_async_copy(kmt_h, ktmp, small_sem.at[0]),
        pltpu.make_async_copy(dep_h, htmp, small_sem.at[1]),
        pltpu.make_async_copy(eta_h, ext.at[2, pl.ds(HR, NR), pl.ds(0, NC)], small_sem.at[2]),
        pltpu.make_async_copy(tu_h, ext.at[3, pl.ds(HR, NR), pl.ds(0, NC)], small_sem.at[3]),
        pltpu.make_async_copy(tv_h, ext.at[4, pl.ds(HR, NR), pl.ds(0, NC)], small_sem.at[4]),
    ]
    for c in small:
        c.start()

    def load(i, c):
        src = (t_h, s_h, u_h, v_h)[i]
        dst = (tb, sb, ub, vb)[i]
        at = pl.ds(pl.multiple_of(c * CH, CH), CH)
        to = pl.ds(pl.multiple_of(c * CH + (8 if i >= 2 else 0), 8), CH)
        return pltpu.make_async_copy(src.at[:, at, :], dst.at[:, to, :], load_sem.at[i, c])

    def start_loads(pair):
        def body(c):
            for i in pair:
                load(i, c).start()

        loop(0, NCH, body)

    start_loads((0, 1))
    start_loads((2, 3))

    def send(src, dst, idx, dev):
        c = remote(src, dst, idx, dev)
        c.start()
        return c

    def remote(src, dst, idx, dev):
        return pltpu.make_async_remote_copy(
            src_ref=src, dst_ref=dst, send_sem=send_sem.at[idx], recv_sem=recv_sem.at[idx], device_id=dev, device_id_type=MESH
        )

    lane, in_first, level = packed_lanes()
    for c in small:
        c.wait()
    for r in range(STRIPS):
        kf = ktmp[rows(r), :].astype(F32)
        dz = htmp[rows(r), :] / jnp.maximum(kf, 1.0)
        ext[KMT, rows(r, HR), BODY] = kf
        ext[DZ, rows(r, HR), BODY] = dz
        eta, tu, tv = (ext[f, rows(r, HR), BODY] for f in (ETA, TU, TV))
        pa[rows(r), :] = pack_wide((kf, dz, eta))
        pb_[rows(r), :] = pack_wide((tu, tv))
    pl.semaphore_wait(barrier, 5)

    def start(copies):
        for c in copies:
            c.start()

    def send_ext(lo, n, tile, ghost, base):
        at = pl.ds(lo, n)
        low, high, mid = pl.ds(0, HR), pl.ds(HR + NR, HR), pl.ds(HR, NR)
        body = pl.ds(0, NC)
        parts = (
            (ext.at[at, pl.ds(NR, HR), body], ext.at[at, low, body], to_n),
            (tile.at[pl.ds(NR - HR, HR), :], ghost.at[low, :], to_dn),
            (tile, ghost.at[mid, :], to_x),
            (ext.at[at, pl.ds(HR, HR), body], ext.at[at, high, body], to_s),
            (tile.at[low, :], ghost.at[high, :], to_ds),
        )
        return [remote(a, b, base + i, dev) for i, (a, b, dev) in enumerate(parts)]

    def receive_ext(copies, ghost, fields):
        for c in copies:
            c.wait()

        for q, f in enumerate(fields):
            ext[f, :, GHOST] = unpack_wide(ghost[...], q)

    first = send_ext(KMT, 3, pa, ga, 0)
    start(first)

    def pressure(r):
        kc = ext[KMT, rows(r, HR), BODY]
        dz = ext[DZ, rows(r, HR), BODY]
        total = jnp.zeros((8, NC), F32)
        scale = TIME_STEP * dz
        for k in range(NL):
            half = (0.5 * BETA_S) * (sb[k, rows(r), :] - 1.0) - (0.5 * ALPHA_T) * (tb[k, rows(r), :] - 1.0)
            half = jnp.where(kc > k, half, ZERO)
            middle = total + half
            total = middle + half
            pb[k, rows(r, 8), :] = scale * middle

    def pressure_chunk(c):
        load(0, c).wait()
        load(1, c).wait()
        pressure(c)


    def out_copy(i, c):
        src = (tb, sb, su, sv)[i]
        dst = (tm_o, sm_o, su_o, sv_o)[i]
        at = pl.ds(pl.multiple_of(c * CH, CH), CH)
        return pltpu.make_async_copy(src.at[:, at, :], dst.at[:, at, :], out_sem.at[i, c])

    def pack_ts(r):
        tiles = []
        for slot, ref in enumerate((tb, sb)):
            for k in range(NL):
                tiles.append((slot, k, ref[k, rows(r), LEFT], ref[k, rows(r), RIGHT]))
        sts[rows(r), :] = pack(tiles)

    def mix(r):
        pack_ts(jnp.maximum(r - 1, 0))
        kc = ext[KMT, rows(r, HR), BODY]
        dz = ext[DZ, rows(r, HR), BODY]
        solve((tb, sb), False, kc, (TIME_STEP * DIFF_KT) / (dz * dz), gains, rows(r))

    def mix_chunk(c):
        mix(c)
        out_copy(0, c).start()
        out_copy(1, c).start()

    def both_chunk(c):
        pressure_chunk(c)
        mix_chunk(c)

    loop(0, EARLY, both_chunk, PAIR)
    loop(EARLY, NCH, pressure_chunk, PAIR)

    def pack_uvp(r):
        tiles = []
        for slot, ref in enumerate((ub, vb, pb)):
            for k in range(NL):
                x = [ref[k, rows(r, 8), LEFT], ref[k, rows(r, 8), RIGHT]]
                tiles.append((slot, k, *x))
        sp[rows(r, 8), :] = pack(tiles)

    def pack_chunk(c):
        load(2, c).wait()
        load(3, c).wait()
        pack_uvp(c)

    loop(0, NCH, pack_chunk, PAIR)

    def edge_row(dst, i, k, ref, at):
        dst[24 * i + k : 24 * i + k + 1, :] = ref[k, at : at + 1, :]

    def ghost_row(ref, k, at, src, i):
        x = src[24 * i + k : 24 * i + k + 1, :]
        ref[k, at : at + 1, :] = jnp.where(geo[i, at : at + 1, :] > k, x, ZERO) if i < 2 else x

    for k in range(NL):
        for i, ref in enumerate((ub, vb, pb)):
            edge_row(prs, i, k, ref, 8)
            if i < 2:
                edge_row(prn, i, k, ref, NR + 7)
    low, high = pl.ds(8, 8), pl.ds(NR, 8)
    second = [
        send(sp.at[pl.ds(8, NR), :], gx.at[pl.ds(8, NR), :], 10, to_x),
        send(prn, grs, 11, to_n),
        send(prs, grn, 12, to_s),
        send(sp.at[high, :], gx.at[pl.ds(0, 8), :], 13, to_dn),
        send(sp.at[low, :], gx.at[pl.ds(NR + 8, 8), :], 14, to_ds),
        send(sp.at[high, :], sp.at[pl.ds(0, 8), :], 25, to_n),
    ]

    later = send_ext(TU, 2, pb_, gb, 5)
    start(later)

    loop(EARLY, NCH, mix_chunk, PAIR)
    pack_ts(STRIPS - 1)
    for k in range(NL):
        for i, ref in enumerate((tb, sb)):
            edge_row(trs, i, k, ref, 0)
            edge_row(trn, i, k, ref, NR - 1)
    third = [send(sts, gts_o, 15, to_x), send(trn, grts_o, 16, to_n), send(trs, grtn_o, 17, to_s)]

    receive_ext(first, ga, (KMT, DZ, ETA))
    has_south = (row > 0).astype(F32)
    has_north = (row < n_row - 1).astype(F32)
    ext[KMT, 0:HR, :] = ext[KMT, 0:HR, :] * has_south
    ext[KMT, HR + NR :, :] = ext[KMT, HR + NR :, :] * has_north

    for r in range(-1, STRIPS + 1):
        at, above = rows(r, HR), rows(r, HR + 8)
        kc, dz = ext[KMT, at, :], ext[DZ, at, :]
        k_u = jnp.minimum(kc, east(kc))
        k_v = jnp.minimum(kc, north(kc, ext[KMT, above, :]))
        geo[KU, rows(r, 8), :] = k_u[:, BODY]
        geo[KV, rows(r, 8), :] = k_v[:, BODY]
        geo[DU, rows(r, 8), :] = 0.5 * (dz + east(dz))[:, BODY]
        geo[DV, rows(r, 8), :] = 0.5 * (dz + north(dz, ext[DZ, above, :]))[:, BODY]
        (u_w, u_e, u_l), (v_w, v_e, v_f) = (
            [jnp.broadcast_to(x[:, i : i + 1], (8, 128)) for i in at]
            for x, at in ((k_u, (EC - 1, NC, NC - 1)), (k_v, (EC - 1, NC, 0)))
        )
        top = jnp.where(lane < 2 * 40 - 1, even_odd(v_e, v_w), 1.0 * NL)
        wet_g[rows(r, 8), :] = jnp.where(in_first, even_odd(u_e, u_w), top)
        wet_o[rows(r, 8), :] = jnp.where(in_first, u_l, v_f)

    def mask(r):
        for slot, ref in enumerate((ub, vb)):
            count = geo[slot, rows(r, 8), :]
            total = jnp.zeros((8, NC), F32)
            for k in range(NL):
                x = jnp.where(count > k, ref[k, rows(r, 8), :], ZERO)
                ref[k, rows(r, 8), :] = x
                total = total + x
            tot[slot, rows(r), :] = total

    loop(0, STRIPS, mask, PAIR)
    for c in second:
        c.wait()

    def wet(x, count, t):
        return jnp.where(count[rows(t), :] > level, x[rows(t), :], ZERO)

    corner_w = None
    for t in range(STRIPS + 1, 0, -1):
        g, own, below = wet(gx, wet_g, t), wet(sp, wet_o, t), t - 1
        g_s, own_s = south(g, wet(gx, wet_g, below)), south(own, wet(sp, wet_o, below))
        pka[rows(t - 1), :] = even_odd(turn(g, 1), turn(g_s, -41))
        flux = (turn(g_s, -39) + turn(own_s, -40)) * turn(g_s + g, 1)
        if corner_w is not None:
            d = own + turn(g, -1)
            pkb[rows(t - 1), :] = even_odd(north(flux, corner_w), d * d + turn(g, -81))
        corner_w = flux

    for k in range(NL):
        for i, ref in enumerate((ub, vb)):
            ghost_row(ref, k, 7, grs, i)
        for i, ref in enumerate((ub, vb, pb)):
            ghost_row(ref, k, NR + 8, grn, i)

    def corner(r, k, ghost):
        u, v, p = (ref[k, rows(r, 8), :] for ref in (ub, vb, pb))
        u_s = south(u, ub[k, rows(r), :])
        v_s = south(v, vb[k, rows(r), :])
        f_s = (v_s + east_of(v_s, ghost)) * (u_s + u)
        c = v + v_s
        return u, p, f_s, c * c + p

    for k in range(NL):
        fsp[k], csp[k] = corner(STRIPS, k, unpack(pka[NR : NR + 8, :], 0, k))[2:]

    def tendency(i):
        r = STRIPS - 1 - i
        at = rows(r)
        near, far = pka[at, :], pkb[at, :]
        for k in range(NL):
            ghost = unpack(near, 0, k)
            u, p, f_s, c = corner(r, k, ghost)
            f = north(f_s, fsp[k])
            c_n = north(c, csp[k])
            fsp[k], csp[k] = f_s, c
            d = u + west_of(u, ghost)
            d = d * d + p
            fp[k], dup[k] = f, d
            su[k, at, :] = (f_s - f) + d
            sv[k, at, :] = (c - c_n) - f
        k_u, k_v, dz_u, dz_v = (geo[i, rows(r, 8), :] for i in (KU, KV, DU, DV))
        sum_u = sum_v = jnp.zeros((8, NC), F32)
        for k in range(NL):
            ghost = unpack(far, 0, k)
            t_u = su[k, at, :] - east_of(dup[k], ghost)
            t_v = sv[k, at, :] + west_of(fp[k], ghost)
            u = jnp.where(k_u > k, ub[k, rows(r, 8), :] + t_u, ZERO)
            v = jnp.where(k_v > k, vb[k, rows(r, 8), :] + t_v, ZERO)
            su[k, at, :], sv[k, at, :] = u, v
            sum_u, sum_v = sum_u + u, sum_v + v
        ext[FX, rows(r, HR), BODY] = (dz_u / TIME_STEP) * (sum_u - tot[KU, at, :])
        ext[FY, rows(r, HR), BODY] = (dz_v / TIME_STEP) * (sum_v - tot[KV, at, :])
        ext[SU, rows(r, HR), BODY] = dz_u * sum_u
        ext[SV, rows(r, HR), BODY] = dz_v * sum_v

    def pack_forcing(lo, hi):
        for r in range(lo, hi):
            pc[rows(r), :] = pack_wide([ext[f, rows(r, HR), BODY] for f in (FX, FY, SU)])

    fourth = send_ext(FX, 3, pc, gc, 18)

    def leave_north():
        pack_forcing(STRIPS - NORTH, STRIPS)
        start(fourth[:2])

    def tendency_pair(i):
        for j in range(PAIR):
            tendency(PAIR * i + j)
        pl.when(i == NORTH // PAIR - 1)(leave_north)

    loop(0, STRIPS // PAIR, tendency_pair)
    pack_forcing(0, STRIPS - NORTH)
    start(fourth[2:])
    receive_ext(later, gb, (TU, TV))
    out_ext0 = pltpu.make_async_copy(ext.at[pl.ds(0, 5)], ext_o.at[pl.ds(0, 5)], outs_sem.at[0])
    out_ext0.start()

    def implicit(i, ref, keep, r):
        dz = geo[DU + i, rows(r, 8), :]
        solve((ref,), True, geo[i, rows(r, 8), :], (TIME_STEP * VISC_KV) / (dz * dz), keep, rows(r))

    def pack_su(r):
        sug[rows(r), :] = pack([(0, k, su[k, rows(r), LEFT], su[k, rows(r), RIGHT]) for k in range(NL)])

    def solve_u(r):
        pack_su(jnp.maximum(r - 1, 0))
        implicit(0, su, gains, r)

    def solve_v(r):
        implicit(1, sv, gains2, r)

    def u_chunk(c):
        solve_u(c)
        out_copy(2, c).start()

    def v_chunk(c):
        solve_v(c)
        out_copy(3, c).start()

    v_chunk(NCH - 1)
    loop(0, NCH, u_chunk, PAIR)
    pack_su(STRIPS - 1)
    for k in range(NL):
        edge_row(vrn, 0, k, sv, NR - 1)
    fifth = [send(sug, gu_o, 23, to_x), send(vrn, grv_o, 24, to_n)]
    out_ext1 = pltpu.make_async_copy(ext.at[pl.ds(5, 4)], ext_o.at[pl.ds(5, 4)], outs_sem.at[1])

    def take_forcing():
        receive_ext(fourth, gc, (FX, FY, SU))
        out_ext1.start()

    def v_triple(i):
        for j in range(TRIPLE):
            v_chunk(TRIPLE * i + j)
        pl.when(i == TRIPLE - 1)(take_forcing)

    loop(0, STRIPS // TRIPLE, v_triple)
    out_sts = pltpu.make_async_copy(sts, sts_o, outs_sem.at[2])
    out_sts.start()

    def drain(c):
        for i in range(4):
            out_copy(i, c).wait()

    loop(0, NCH, drain)
    for c in third:
        c.wait()
    for c in fifth:
        c.wait()
    out_ext0.wait()
    out_ext1.wait()
    out_sts.wait()


def finish_kernel(
    tide, su_h, sv_h, tm_h, sm_h, ext_h, gts_h, gu_h, grts_h, grtn_h, grv_h, sts_h,
    eta_o, tu_o, tv_o, u_o, v_o, t_o, s_o,
    ub, vb, tb, sb, ext, cof, cnt, avg, gts, gu, grts, grtn, grv, sts, fpt, fps, fxt, fxs, pkt, tg, sg,
    load_sem, small_sem, out_sem, outs_sem,
):
    early, late = (
        pltpu.make_async_copy(ext_h.at[at], ext.at[at], small_sem.at[i])
        for i, at in enumerate((pl.ds(KMT, SV), pl.ds(SV, 2)))
    )
    early.start()
    small = [
        pltpu.make_async_copy(a, b, small_sem.at[i + 2])
        for i, (a, b) in enumerate(((gts_h, gts), (gu_h, gu), (grts_h, grts), (grtn_h, grtn), (grv_h, grv), (sts_h, sts)))
    ]
    late.start()
    for c in small:
        c.start()
    big = [
        pltpu.make_async_copy(su_h, ub, load_sem.at[0]),
        pltpu.make_async_copy(sv_h, vb.at[:, pl.ds(8, NR), :], load_sem.at[1]),
        pltpu.make_async_copy(tm_h, tb.at[:, pl.ds(8, NR), :], load_sem.at[2]),
        pltpu.make_async_copy(sm_h, sb.at[:, pl.ds(8, NR), :], load_sem.at[3]),
    ]
    for c in big:
        c.start()
    early.wait()

    def faces(at, above):
        kc, kn = ext[KMT, at, :], ext[KMT, above, :]
        dz, dn = ext[DZ, at, :], ext[DZ, above, :]
        k_u = jnp.minimum(kc, east(kc))
        k_v = jnp.minimum(kc, north(kc, kn))
        return kc, k_u, k_v, k_u * (0.5 * (dz + east(dz))), k_v * (0.5 * (dz + north(dz, dn)))

    for t in range(TILES):
        at = rows(t)
        kc, k_u, k_v, h_u, h_v = faces(at, rows(min(t + 1, TILES - 1)))
        for i, (count, h) in enumerate(((k_u, h_u), (k_v, h_v))):
            cof[i, at, :] = (DTB * DTB) * h
            cnt[i, at, :] = count
            ext[FX + i, at, :] = (DTB * DTB) * ext[FX + i, at, :]
            avg[i, at, :] = jnp.zeros((8, EC), F32)
        for f, count, scale in ((ETA, kc, 1.0), (TU, k_u, DTB), (TV, k_v, DTB)):
            ext[f, at, :] = jnp.where(count > ZERO, scale * ext[f, at, :], ZERO)

    norm = 6.0 / (NSUB * (NSUB + 1) * (NSUB + 2)) / DTB

    def subcycle(n, lo, hi):
        tide_x, tide_y = tide[0, n], tide[1, n]
        weight = norm * ((n + 1) * (NSUB - n)).astype(F32)
        v_prev = ext[TV, rows(max(lo - 1, 0)), :]
        eta_prev = None
        u_keep = v_keep = None
        for t in range(lo, hi + 1):
            if t < hi:
                at = rows(t)
                u, v = ext[TU, at, :], ext[TV, at, :]
                eta = ext[ETA, at, :] - ((u - west(u)) + (v - south(v, v_prev)))
                ext[ETA, at, :] = eta
            if t > lo:
                b = rows(t - 1)
                slope_x = east(eta_prev) - eta_prev
                slope_y = north(eta_prev, eta) - eta_prev
                u_new = u_keep + (cof[0, b, :] * (tide_x - slope_x) + ext[FX, b, :])
                v_new = v_keep + (cof[1, b, :] * (tide_y - slope_y) + ext[FY, b, :])
                ext[TU, b, :] = u_new
                ext[TV, b, :] = v_new
                if 2 <= t - 1 < 19:
                    avg[0, b, :] = avg[0, b, :] + weight * u_new
                    avg[1, b, :] = avg[1, b, :] + weight * v_new
            eta_prev, u_keep, v_keep, v_prev = eta, u, v, v

    tiles = TILES
    loop(0, 4, functools.partial(subcycle, lo=0, hi=tiles))
    loop(4, 12, functools.partial(subcycle, lo=1, hi=tiles - 1))
    loop(12, NSUB, functools.partial(subcycle, lo=2, hi=tiles - 2))

    for r in range(STRIPS):
        at = rows(r, HR)
        for f in (TU, TV):
            ext[f, at, :] = (1.0 / DTB) * ext[f, at, :]
    planes = [
        pltpu.make_async_copy(ext.at[2 + i, pl.ds(HR, NR), pl.ds(0, NC)], o, outs_sem.at[i])
        for i, o in enumerate((eta_o, tu_o, tv_o))
    ]
    for c in planes:
        c.start()
    late.wait()
    for c in small:
        c.wait()
    for c in big:
        c.wait()
    for k in range(NL):
        vb[k, 7:8, :] = grv[k : k + 1, :]
        for i, ref in enumerate((tb, sb)):
            ref[k, 7:8, :] = grts[24 * i + k : 24 * i + k + 1, :]
            ref[k, NR + 8 : NR + 9, :] = grtn[24 * i + k : 24 * i + k + 1, :]

    for r in range(-1, STRIPS):
        at = rows(r, HR)
        for i, f in enumerate((SU, SV)):
            h = cof[i, at, :]
            avg[i, at, :] = (DTB * DTB) * (avg[i, at, :] - ext[f, at, :]) / jnp.where(h > ZERO, h, 1.0)

    def strip(r):
        at = rows(r, HR)
        return [x[at, BODY] for x in (ext.at[KMT], cnt.at[0], cnt.at[1], avg.at[0], avg.at[1])]

    def flux_y(r, k, k_v, d_v):
        vc = jnp.where(k_v > k, vb[k, rows(r, 8), :] + d_v, ZERO)
        out = [vc]
        for ref in (tb, sb):
            here = ref[k, rows(r, 8), :]
            out.append(here)
            out.append(vc * (here + north(here, ref[k, rows(r, 16), :])))
        return out

    _, _, k_v, _, d_v = strip(-1)
    for k in range(NL):
        _, _, a, _, b = flux_y(-1, k, k_v, d_v)
        fpt[k] = a
        fps[k] = b

    _, in_first, level = packed_lanes()
    for r in range(STRIPS):
        at = rows(r, HR)
        count, add = (jnp.broadcast_to(x[0, at, EC - 1 : EC], (8, 128)) for x in (cnt, avg))
        uc = jnp.where(count > level, gu[rows(r), :] + add, ZERO)
        uc = jnp.where(in_first, uc, turn(uc, 40))
        g = gts[rows(r), :]
        pkt[rows(r), :] = even_odd(turn(uc * (g + turn(sts[rows(r), :], -1)), 1), turn(g, -1))

    def advect(r):
        kc, k_u, k_v, d_u, d_v = strip(r)
        edges = pkt[rows(r), :]
        for k in range(NL):
            vc, t, y_t, s, y_s = flux_y(r, k, k_v, d_v)
            vb[k, rows(r, 8), :] = vc
            uc = jnp.where(k_u > k, ub[k, rows(r), :] + d_u, ZERO)
            ub[k, rows(r), :] = uc
            for slot, (ref, edge, prev, keep, x, y) in enumerate(((tb, tg, fpt, fxt, t, y_t), (sb, sg, fps, fxs, s, y_s))):
                ghost = unpack(edges, slot, k)
                edge[k] = ghost
                fx = uc * (x + east_of(x, ghost))
                keep[k] = fx
                ref[k, rows(r, 8), :] = x - HALF_DT * (fx + (y - south(y, prev[k])))
                prev[k] = y
        for k in range(NL):
            for ref, edge, keep in ((tb, tg, fxt), (sb, sg, fxs)):
                x = ref[k, rows(r, 8), :] + HALF_DT * west_of(keep[k], edge[k])
                ref[k, rows(r, 8), :] = jnp.where(kc > k, x, ZERO)

    def out_copy(i, c):
        src = (ub, vb, tb, sb)[i]
        dst = (u_o, v_o, t_o, s_o)[i]
        at = pl.ds(pl.multiple_of(c * CH, CH), CH)
        frm = pl.ds(pl.multiple_of(c * CH + (8 if i else 0), 8), CH)
        return pltpu.make_async_copy(src.at[:, frm, :], dst.at[:, at, :], out_sem.at[i, c])

    def advect_chunk(c):
        advect(c)
        for i in range(4):
            out_copy(i, c).start()

    loop(0, NCH, advect_chunk)

    def drain(c):
        for i in range(4):
            out_copy(i, c).wait()

    loop(0, NCH, drain)
    for c in planes:
        c.wait()


def vmem(*shape):
    return pltpu.VMEM(shape, F32)


def solution(mesh):
    any_spec = pl.BlockSpec(memory_space=pl.ANY)
    cube = jax.ShapeDtypeStruct((NL, NR, NC), F32)
    plane = jax.ShapeDtypeStruct((NR, NC), F32)

    tile, ghost, strip = vmem(NR, 128), vmem(ER, 128), vmem(NL, 8, NC)

    def arr(*shape):
        return jax.ShapeDtypeStruct(shape, F32)

    def local_step(vel_u, vel_v, temperature, salinity, sea_level, trans_u, trans_v, bathymetry, kmt_levels, tide_force):
        mid = pl.pallas_call(
            predict_kernel,
            name="predict",
            out_shape=(
                cube, cube, cube, cube, arr(9, ER, EC), arr(NR, 128), arr(NR, 128), arr(48, NC), arr(48, NC), arr(24, NC),
                arr(NR, 128),
            ),
            in_specs=[any_spec] * 9,
            out_specs=(any_spec,) * 11,
            scratch_shapes=[
                *([vmem(NL, NR + 16, NC)] * 3), *([vmem(NL, NR, NC)] * 4),
                vmem(9, ER, EC), pltpu.VMEM((NR, NC), jnp.int32), vmem(NR, NC),
                *([tile] * 3), *([ghost] * 3), vmem(NR + 8, 128), tile, strip, *([vmem(NR + 16, 128)] * 2),
                vmem(48, NC), vmem(72, NC), vmem(48, NC), vmem(72, NC),
                tile, vmem(48, NC), vmem(48, NC), tile, vmem(24, NC), *([strip] * 3), vmem(4, NR + 16, NC), *([vmem(NR + 16, 128)] * 2), vmem(2, NR, NC), strip, strip,
                pltpu.SemaphoreType.DMA((4, NCH)), pltpu.SemaphoreType.DMA((5,)), pltpu.SemaphoreType.DMA((4, NCH)),
                pltpu.SemaphoreType.DMA((3,)), pltpu.SemaphoreType.DMA((26,)), pltpu.SemaphoreType.DMA((26,)),
            ],
            compiler_params=pltpu.CompilerParams(collective_id=0, has_side_effects=True, vmem_limit_bytes=63 * 2**20),
        )(vel_u, vel_v, temperature, salinity, sea_level, trans_u, trans_v, bathymetry, kmt_levels)
        return pl.pallas_call(
            finish_kernel,
            name="finish",
            out_shape=(plane, plane, plane, cube, cube, cube, cube),
            in_specs=[pl.BlockSpec(memory_space=pltpu.SMEM)] + [any_spec] * 11,
            out_specs=(any_spec,) * 7,
            scratch_shapes=[
                vmem(NL, NR, NC), vmem(NL, NR + 8, NC), vmem(NL, NR + 16, NC), vmem(NL, NR + 16, NC),
                vmem(9, ER, EC), *([vmem(2, ER, EC)] * 3),
                vmem(NR, 128), vmem(NR, 128), vmem(48, NC), vmem(48, NC), vmem(24, NC), tile, *([strip] * 4), tile, *([vmem(NL, 8, 128)] * 2),
                pltpu.SemaphoreType.DMA((4,)), pltpu.SemaphoreType.DMA((8,)), pltpu.SemaphoreType.DMA((4, NCH)),
                pltpu.SemaphoreType.DMA((3,)),
            ],
            compiler_params=pltpu.CompilerParams(vmem_limit_bytes=60 * 2**20),
        )(tide_force.T, *mid)

    spec_cube = P(None, "row", "col")
    spec_plane = P("row", "col")
    return jax.shard_map(
        local_step,
        mesh=mesh,
        in_specs=(spec_cube,) * 4 + (spec_plane,) * 5 + (P(None, None),),
        out_specs=(spec_plane,) * 3 + (spec_cube,) * 4,
        check_vma=False,
    )
```

```python
import functools

import jax
import jax.numpy as jnp
from jax import lax
from jax.experimental import pallas as pl
from jax.experimental.pallas import tpu as pltpu
from jax.sharding import PartitionSpec as P

TIME_STEP = 4.0
ALPHA_T = 0.02
BETA_S = 0.015
VISC_KV = 0.001
DIFF_KT = 0.0005

NL = 20
NSUB = 20
NR, NC = 128, 512
HR = 24
ER, EC = NR + 2 * HR, NC + 128
NCH = 16
CH = NR // NCH
STRIPS, TILES = NR // 8, ER // 8
PAIR, TRIPLE = 2, 3
NORTH = 2 * PAIR
EARLY = 2
DTB = TIME_STEP / NSUB
HALF_DT = 0.5 * TIME_STEP
F32 = jnp.float32
ZERO = 0.0
BODY = slice(0, NC)
LEFT = slice(0, 128)
RIGHT = slice(NC - 128, NC)
GHOST = slice(NC, EC)
KMT, DZ, ETA, TU, TV, FX, FY, SV, SU = range(9)
KU, KV, DU, DV = range(4)
WIDE = 42
MESH = pl.DeviceIdType.MESH


def loop(lo, hi, body, per=1):
    def step(i, carry):
        for j in range(per):
            body(lo + per * i + j)
        return carry

    lax.fori_loop(0, (hi - lo) // per, step, 0)


def rows(r, off=0):
    start = 8 * r + off
    if isinstance(start, int):
        return pl.ds(start, 8)
    return pl.ds(pl.multiple_of(start, 8), 8)


def iota(shape, axis):
    return lax.broadcasted_iota(jnp.int32, shape, axis)


def east(x):
    return pltpu.roll(x, x.shape[1] - 1, 1)


def west(x):
    return pltpu.roll(x, 1, 1)


def north(here, above):
    return pltpu.roll(jnp.where(iota(here.shape, 0) == 0, above, here), 7, 0)


def south(here, below):
    return pltpu.roll(jnp.where(iota(here.shape, 0) == 7, below, here), 1, 0)


def lane_tiles(x):
    return [x[:, 128 * c : 128 * (c + 1)] for c in range(NC // 128)]


def east_of(x, ghost):
    moved = [pltpu.roll(t, 127, 1) for t in lane_tiles(x)] + [ghost]
    last = iota((8, 128), 1) == 127
    return jnp.concatenate([jnp.where(last, b, a) for a, b in zip(moved, moved[1:])], 1)


def west_of(x, ghost):
    moved = [ghost] + [pltpu.roll(t, 1, 1) for t in lane_tiles(x)]
    first = iota((8, 128), 1) == 0
    return jnp.concatenate([jnp.where(first, a, b) for a, b in zip(moved, moved[1:])], 1)


def turn(x, by):
    return pltpu.roll(x, by % 128, 1)


def even_odd(a, b):
    return jnp.where(iota((8, 128), 1) % 2 == 0, a, b)


def lane_of(slot, k):
    return 2 * k + 40 * slot


def unpack(ghost, slot, k):
    shift = (128 - lane_of(slot, k)) % 128
    return pltpu.roll(ghost, shift, 1) if shift else ghost


def pack(tiles):
    lane = iota((8, 128), 1)
    acc = None
    first = None
    for slot, k, low, high in tiles:
        both = jnp.where(lane == 127, high, low)
        at = lane_of(slot, k)
        moved = pltpu.roll(both, at, 1) if at else both
        if acc is None:
            acc = moved
            if at == 0:
                first = moved
        else:
            acc = jnp.where(lane >= at - 1, moved, acc)
    if first is not None:
        acc = jnp.where(lane == 127, first, acc)
    return acc


def pack_wide(planes):
    lane = iota((8, 128), 1)
    acc = None
    for q, x in enumerate(planes):
        edge = jnp.where(lane < 64, x[:, LEFT], x[:, RIGHT])
        if acc is None:
            acc = edge
        else:
            acc = jnp.where(lane >= WIDE * q - WIDE // 2, pltpu.roll(edge, WIDE * q, 1), acc)
    if len(planes) == 1:
        return acc
    first = jnp.where(lane < 64, planes[0][:, LEFT], planes[0][:, RIGHT])
    return jnp.where(lane >= 128 - WIDE // 2, first, acc)


def unpack_wide(tile, q):
    lane = iota(tile.shape, 1)
    moved = pltpu.roll(tile, 128 - WIDE * q, 1) if q else tile
    return jnp.where((lane < WIDE // 2) | (lane >= 128 - WIDE // 2), moved, ZERO)


def packed_lanes():
    lane = iota((8, 128), 1)
    in_first = (lane < 39) | (lane == 127)
    return lane, in_first, jnp.where(lane == 127, ZERO, (((lane + 1) % 40) // 2).astype(F32))


def solve(refs, masked, count, coef, gains, at):
    low = None
    rest = 1.0
    parts = [None] * len(refs)
    for k in range(NL):
        up = jnp.where(count > k + 1.0, coef, ZERO) if k < NL - 1 else ZERO
        inv = 1.0 / (rest + up)
        for i, ref in enumerate(refs):
            src = ref[k, at, :]
            if not masked:
                src = jnp.where(count > k, src, ZERO)
            parts[i] = src * inv if k == 0 else (src + low * parts[i]) * inv
            if k < NL - 1:
                ref[k, at, :] = parts[i]
        if k < NL - 1:
            gain = up * inv
            gains[k] = gain
            rest = 1.0 + gain * rest
        low = up
    for i, ref in enumerate(refs):
        ref[NL - 1, at, :] = parts[i]
    for k in range(NL - 2, -1, -1):
        gain = gains[k]
        for i, ref in enumerate(refs):
            parts[i] = ref[k, at, :] + gain * parts[i]
            ref[k, at, :] = parts[i]


def predict_kernel(
    u_h, v_h, t_h, s_h, eta_h, tu_h, tv_h, dep_h, kmt_h,
    su_o, sv_o, tm_o, sm_o, ext_o, gts_o, gu_o, grts_o, grtn_o, grv_o, sts_o,
    ub, vb, pb, tb, sb, su, sv, ext, ktmp, htmp, pa, pb_, pc, ga, gb, gc, pka, pkb, dup, sp, gx, prn, prs, grs, grn, sts, trn, trs, sug, vrn, fp, fsp, csp, geo, wet_g, wet_o, tot, gains, gains2,
    load_sem, small_sem, out_sem, outs_sem, send_sem, recv_sem,
):
    col = lax.axis_index("col")
    row = lax.axis_index("row")
    n_row = 8
    side = 1 - col
    up_row = lax.rem(row + 1, n_row)
    down_row = lax.rem(row + n_row - 1, n_row)
    to_x = {"col": side, "row": row}
    to_n = {"col": col, "row": up_row}
    to_s = {"col": col, "row": down_row}
    to_dn = {"col": side, "row": up_row}
    to_ds = {"col": side, "row": down_row}

    barrier = pltpu.get_barrier_semaphore()
    for dev in (to_x, to_n, to_s, to_dn, to_ds):
        pl.semaphore_signal(barrier, inc=1, device_id=dev, device_id_type=MESH)

    small = [
        pltpu.make_async_copy(kmt_h, ktmp, small_sem.at[0]),
        pltpu.make_async_copy(dep_h, htmp, small_sem.at[1]),
        pltpu.make_async_copy(eta_h, ext.at[2, pl.ds(HR, NR), pl.ds(0, NC)], small_sem.at[2]),
        pltpu.make_async_copy(tu_h, ext.at[3, pl.ds(HR, NR), pl.ds(0, NC)], small_sem.at[3]),
        pltpu.make_async_copy(tv_h, ext.at[4, pl.ds(HR, NR), pl.ds(0, NC)], small_sem.at[4]),
    ]
    for c in small:
        c.start()

    def load(i, c):
        src = (t_h, s_h, u_h, v_h)[i]
        dst = (tb, sb, ub, vb)[i]
        at = pl.ds(pl.multiple_of(c * CH, CH), CH)
        to = pl.ds(pl.multiple_of(c * CH + (8 if i >= 2 else 0), 8), CH)
        return pltpu.make_async_copy(src.at[:, at, :], dst.at[:, to, :], load_sem.at[i, c])

    def start_loads(pair):
        def body(c):
            for i in pair:
                load(i, c).start()

        loop(0, NCH, body)

    start_loads((0, 1))
    start_loads((2, 3))

    def send(src, dst, idx, dev):
        c = remote(src, dst, idx, dev)
        c.start()
        return c

    def remote(src, dst, idx, dev):
        return pltpu.make_async_remote_copy(
            src_ref=src, dst_ref=dst, send_sem=send_sem.at[idx], recv_sem=recv_sem.at[idx], device_id=dev, device_id_type=MESH
        )

    lane, in_first, level = packed_lanes()
    for c in small:
        c.wait()
    for r in range(STRIPS):
        kf = ktmp[rows(r), :].astype(F32)
        dz = htmp[rows(r), :] / jnp.maximum(kf, 1.0)
        ext[KMT, rows(r, HR), BODY] = kf
        ext[DZ, rows(r, HR), BODY] = dz
        eta, tu, tv = (ext[f, rows(r, HR), BODY] for f in (ETA, TU, TV))
        pa[rows(r), :] = pack_wide((kf, dz, eta))
        pb_[rows(r), :] = pack_wide((tu, tv))
    pl.semaphore_wait(barrier, 5)

    def start(copies):
        for c in copies:
            c.start()

    def send_ext(lo, n, tile, ghost, base):
        at = pl.ds(lo, n)
        low, high, mid = pl.ds(0, HR), pl.ds(HR + NR, HR), pl.ds(HR, NR)
        body = pl.ds(0, NC)
        parts = (
            (ext.at[at, pl.ds(NR, HR), body], ext.at[at, low, body], to_n),
            (tile.at[pl.ds(NR - HR, HR), :], ghost.at[low, :], to_dn),
            (tile, ghost.at[mid, :], to_x),
            (ext.at[at, pl.ds(HR, HR), body], ext.at[at, high, body], to_s),
            (tile.at[low, :], ghost.at[high, :], to_ds),
        )
        return [remote(a, b, base + i, dev) for i, (a, b, dev) in enumerate(parts)]

    def receive_ext(copies, ghost, fields):
        for c in copies:
            c.wait()

        for q, f in enumerate(fields):
            ext[f, :, GHOST] = unpack_wide(ghost[...], q)

    first = send_ext(KMT, 3, pa, ga, 0)
    start(first)

    def pressure(r):
        kc = ext[KMT, rows(r, HR), BODY]
        dz = ext[DZ, rows(r, HR), BODY]
        total = jnp.zeros((8, NC), F32)
        scale = TIME_STEP * dz
        for k in range(NL):
            half = (0.5 * BETA_S) * (sb[k, rows(r), :] - 1.0) - (0.5 * ALPHA_T) * (tb[k, rows(r), :] - 1.0)
            half = jnp.where(kc > k, half, ZERO)
            middle = total + half
            total = middle + half
            pb[k, rows(r, 8), :] = scale * middle

    def pressure_chunk(c):
        load(0, c).wait()
        load(1, c).wait()
        pressure(c)


    def out_copy(i, c):
        src = (tb, sb, su, sv)[i]
        dst = (tm_o, sm_o, su_o, sv_o)[i]
        at = pl.ds(pl.multiple_of(c * CH, CH), CH)
        return pltpu.make_async_copy(src.at[:, at, :], dst.at[:, at, :], out_sem.at[i, c])

    def pack_ts(r):
        tiles = []
        for slot, ref in enumerate((tb, sb)):
            for k in range(NL):
                tiles.append((slot, k, ref[k, rows(r), LEFT], ref[k, rows(r), RIGHT]))
        sts[rows(r), :] = pack(tiles)

    def mix(r):
        pack_ts(jnp.maximum(r - 1, 0))
        kc = ext[KMT, rows(r, HR), BODY]
        dz = ext[DZ, rows(r, HR), BODY]
        solve((tb, sb), False, kc, (TIME_STEP * DIFF_KT) / (dz * dz), gains, rows(r))

    def mix_chunk(c):
        mix(c)
        out_copy(0, c).start()
        out_copy(1, c).start()

    def both_chunk(c):
        pressure_chunk(c)
        mix_chunk(c)

    loop(0, EARLY, both_chunk, PAIR)
    loop(EARLY, NCH, pressure_chunk, PAIR)

    def pack_uvp(r):
        tiles = []
        for slot, ref in enumerate((ub, vb, pb)):
            for k in range(NL):
                x = [ref[k, rows(r, 8), LEFT], ref[k, rows(r, 8), RIGHT]]
                tiles.append((slot, k, *x))
        sp[rows(r, 8), :] = pack(tiles)

    def pack_chunk(c):
        load(2, c).wait()
        load(3, c).wait()
        pack_uvp(c)

    loop(0, NCH, pack_chunk, PAIR)

    def edge_row(dst, i, k, ref, at):
        dst[24 * i + k : 24 * i + k + 1, :] = ref[k, at : at + 1, :]

    def ghost_row(ref, k, at, src, i):
        x = src[24 * i + k : 24 * i + k + 1, :]
        ref[k, at : at + 1, :] = jnp.where(geo[i, at : at + 1, :] > k, x, ZERO) if i < 2 else x

    for k in range(NL):
        for i, ref in enumerate((ub, vb, pb)):
            edge_row(prs, i, k, ref, 8)
            if i < 2:
                edge_row(prn, i, k, ref, NR + 7)
    low, high = pl.ds(8, 8), pl.ds(NR, 8)
    second = [
        send(sp.at[pl.ds(8, NR), :], gx.at[pl.ds(8, NR), :], 10, to_x),
        send(prn, grs, 11, to_n),
        send(prs, grn, 12, to_s),
        send(sp.at[high, :], gx.at[pl.ds(0, 8), :], 13, to_dn),
        send(sp.at[low, :], gx.at[pl.ds(NR + 8, 8), :], 14, to_ds),
        send(sp.at[high, :], sp.at[pl.ds(0, 8), :], 25, to_n),
    ]

    later = send_ext(TU, 2, pb_, gb, 5)
    start(later)

    loop(EARLY, NCH, mix_chunk, PAIR)
    pack_ts(STRIPS - 1)
    for k in range(NL):
        for i, ref in enumerate((tb, sb)):
            edge_row(trs, i, k, ref, 0)
            edge_row(trn, i, k, ref, NR - 1)
    third = [send(sts, gts_o, 15, to_x), send(trn, grts_o, 16, to_n), send(trs, grtn_o, 17, to_s)]

    receive_ext(first, ga, (KMT, DZ, ETA))
    has_south = (row > 0).astype(F32)
    has_north = (row < n_row - 1).astype(F32)
    ext[KMT, 0:HR, :] = ext[KMT, 0:HR, :] * has_south
    ext[KMT, HR + NR :, :] = ext[KMT, HR + NR :, :] * has_north

    for r in range(-1, STRIPS + 1):
        at, above = rows(r, HR), rows(r, HR + 8)
        kc, dz = ext[KMT, at, :], ext[DZ, at, :]
        k_u = jnp.minimum(kc, east(kc))
        k_v = jnp.minimum(kc, north(kc, ext[KMT, above, :]))
        geo[KU, rows(r, 8), :] = k_u[:, BODY]
        geo[KV, rows(r, 8), :] = k_v[:, BODY]
        geo[DU, rows(r, 8), :] = 0.5 * (dz + east(dz))[:, BODY]
        geo[DV, rows(r, 8), :] = 0.5 * (dz + north(dz, ext[DZ, above, :]))[:, BODY]
        (u_w, u_e, u_l), (v_w, v_e, v_f) = (
            [jnp.broadcast_to(x[:, i : i + 1], (8, 128)) for i in at]
            for x, at in ((k_u, (EC - 1, NC, NC - 1)), (k_v, (EC - 1, NC, 0)))
        )
        top = jnp.where(lane < 2 * 40 - 1, even_odd(v_e, v_w), 1.0 * NL)
        wet_g[rows(r, 8), :] = jnp.where(in_first, even_odd(u_e, u_w), top)
        wet_o[rows(r, 8), :] = jnp.where(in_first, u_l, v_f)

    def mask(r):
        for slot, ref in enumerate((ub, vb)):
            count = geo[slot, rows(r, 8), :]
            total = jnp.zeros((8, NC), F32)
            for k in range(NL):
                x = jnp.where(count > k, ref[k, rows(r, 8), :], ZERO)
                ref[k, rows(r, 8), :] = x
                total = total + x
            tot[slot, rows(r), :] = total

    loop(0, STRIPS, mask, PAIR)
    for c in second:
        c.wait()

    def wet(x, count, t):
        return jnp.where(count[rows(t), :] > level, x[rows(t), :], ZERO)

    corner_w = None
    for t in range(STRIPS + 1, 0, -1):
        g, own, below = wet(gx, wet_g, t), wet(sp, wet_o, t), t - 1
        g_s, own_s = south(g, wet(gx, wet_g, below)), south(own, wet(sp, wet_o, below))
        pka[rows(t - 1), :] = even_odd(turn(g, 1), turn(g_s, -41))
        flux = (turn(g_s, -39) + turn(own_s, -40)) * turn(g_s + g, 1)
        if corner_w is not None:
            d = own + turn(g, -1)
            pkb[rows(t - 1), :] = even_odd(north(flux, corner_w), d * d + turn(g, -81))
        corner_w = flux

    for k in range(NL):
        for i, ref in enumerate((ub, vb)):
            ghost_row(ref, k, 7, grs, i)
        for i, ref in enumerate((ub, vb, pb)):
            ghost_row(ref, k, NR + 8, grn, i)

    def corner(r, k, ghost):
        u, v, p = (ref[k, rows(r, 8), :] for ref in (ub, vb, pb))
        u_s = south(u, ub[k, rows(r), :])
        v_s = south(v, vb[k, rows(r), :])
        f_s = (v_s + east_of(v_s, ghost)) * (u_s + u)
        c = v + v_s
        return u, p, f_s, c * c + p

    for k in range(NL):
        fsp[k], csp[k] = corner(STRIPS, k, unpack(pka[NR : NR + 8, :], 0, k))[2:]

    def tendency(i):
        r = STRIPS - 1 - i
        at = rows(r)
        near, far = pka[at, :], pkb[at, :]
        for k in range(NL):
            ghost = unpack(near, 0, k)
            u, p, f_s, c = corner(r, k, ghost)
            f = north(f_s, fsp[k])
            c_n = north(c, csp[k])
            fsp[k], csp[k] = f_s, c
            d = u + west_of(u, ghost)
            d = d * d + p
            fp[k], dup[k] = f, d
            su[k, at, :] = (f_s - f) + d
            sv[k, at, :] = (c - c_n) - f
        k_u, k_v, dz_u, dz_v = (geo[i, rows(r, 8), :] for i in (KU, KV, DU, DV))
        sum_u = sum_v = jnp.zeros((8, NC), F32)
        for k in range(NL):
            ghost = unpack(far, 0, k)
            t_u = su[k, at, :] - east_of(dup[k], ghost)
            t_v = sv[k, at, :] + west_of(fp[k], ghost)
            u = jnp.where(k_u > k, ub[k, rows(r, 8), :] + t_u, ZERO)
            v = jnp.where(k_v > k, vb[k, rows(r, 8), :] + t_v, ZERO)
            su[k, at, :], sv[k, at, :] = u, v
            sum_u, sum_v = sum_u + u, sum_v + v
        ext[FX, rows(r, HR), BODY] = (dz_u / TIME_STEP) * (sum_u - tot[KU, at, :])
        ext[FY, rows(r, HR), BODY] = (dz_v / TIME_STEP) * (sum_v - tot[KV, at, :])
        ext[SU, rows(r, HR), BODY] = dz_u * sum_u
        ext[SV, rows(r, HR), BODY] = dz_v * sum_v

    def pack_forcing(lo, hi):
        for r in range(lo, hi):
            pc[rows(r), :] = pack_wide([ext[f, rows(r, HR), BODY] for f in (FX, FY, SU)])

    fourth = send_ext(FX, 3, pc, gc, 18)

    def leave_north():
        pack_forcing(STRIPS - NORTH, STRIPS)
        start(fourth[:2])

    def tendency_pair(i):
        for j in range(PAIR):
            tendency(PAIR * i + j)
        pl.when(i == NORTH // PAIR - 1)(leave_north)

    loop(0, STRIPS // PAIR, tendency_pair)
    pack_forcing(0, STRIPS - NORTH)
    start(fourth[2:])
    receive_ext(later, gb, (TU, TV))
    out_ext0 = pltpu.make_async_copy(ext.at[pl.ds(0, 5)], ext_o.at[pl.ds(0, 5)], outs_sem.at[0])
    out_ext0.start()

    def implicit(i, ref, keep, r):
        dz = geo[DU + i, rows(r, 8), :]
        solve((ref,), True, geo[i, rows(r, 8), :], (TIME_STEP * VISC_KV) / (dz * dz), keep, rows(r))

    def pack_su(r):
        sug[rows(r), :] = pack([(0, k, su[k, rows(r), LEFT], su[k, rows(r), RIGHT]) for k in range(NL)])

    def solve_u(r):
        pack_su(jnp.maximum(r - 1, 0))
        implicit(0, su, gains, r)

    def solve_v(r):
        implicit(1, sv, gains2, r)

    def u_chunk(c):
        solve_u(c)
        out_copy(2, c).start()

    def v_chunk(c):
        solve_v(c)
        out_copy(3, c).start()

    v_chunk(NCH - 1)
    loop(0, NCH, u_chunk, PAIR)
    pack_su(STRIPS - 1)
    for k in range(NL):
        edge_row(vrn, 0, k, sv, NR - 1)
    fifth = [send(sug, gu_o, 23, to_x), send(vrn, grv_o, 24, to_n)]
    out_ext1 = pltpu.make_async_copy(ext.at[pl.ds(5, 4)], ext_o.at[pl.ds(5, 4)], outs_sem.at[1])

    def take_forcing():
        receive_ext(fourth, gc, (FX, FY, SU))
        out_ext1.start()

    def v_triple(i):
        for j in range(TRIPLE):
            v_chunk(TRIPLE * i + j)
        pl.when(i == TRIPLE - 1)(take_forcing)

    loop(0, STRIPS // TRIPLE, v_triple)
    out_sts = pltpu.make_async_copy(sts, sts_o, outs_sem.at[2])
    out_sts.start()

    def drain(c):
        for i in range(4):
            out_copy(i, c).wait()

    loop(0, NCH, drain)
    for c in third:
        c.wait()
    for c in fifth:
        c.wait()
    out_ext0.wait()
    out_ext1.wait()
    out_sts.wait()


def finish_kernel(
    tide, su_h, sv_h, tm_h, sm_h, ext_h, gts_h, gu_h, grts_h, grtn_h, grv_h, sts_h,
    eta_o, tu_o, tv_o, u_o, v_o, t_o, s_o,
    ub, vb, tb, sb, ext, cof, cnt, avg, gts, gu, grts, grtn, grv, sts, fpt, fps, fxt, fxs, pkt, tg, sg,
    load_sem, small_sem, out_sem, outs_sem,
):
    early, late = (
        pltpu.make_async_copy(ext_h.at[at], ext.at[at], small_sem.at[i])
        for i, at in enumerate((pl.ds(KMT, SV), pl.ds(SV, 2)))
    )
    early.start()
    small = [
        pltpu.make_async_copy(a, b, small_sem.at[i + 2])
        for i, (a, b) in enumerate(((gts_h, gts), (gu_h, gu), (grts_h, grts), (grtn_h, grtn), (grv_h, grv), (sts_h, sts)))
    ]
    late.start()
    for c in small:
        c.start()
    big = [
        pltpu.make_async_copy(su_h, ub, load_sem.at[0]),
        pltpu.make_async_copy(sv_h, vb.at[:, pl.ds(8, NR), :], load_sem.at[1]),
        pltpu.make_async_copy(tm_h, tb.at[:, pl.ds(8, NR), :], load_sem.at[2]),
        pltpu.make_async_copy(sm_h, sb.at[:, pl.ds(8, NR), :], load_sem.at[3]),
    ]
    for c in big:
        c.start()
    early.wait()

    def faces(at, above):
        kc, kn = ext[KMT, at, :], ext[KMT, above, :]
        dz, dn = ext[DZ, at, :], ext[DZ, above, :]
        k_u = jnp.minimum(kc, east(kc))
        k_v = jnp.minimum(kc, north(kc, kn))
        return kc, k_u, k_v, k_u * (0.5 * (dz + east(dz))), k_v * (0.5 * (dz + north(dz, dn)))

    for t in range(TILES):
        at = rows(t)
        kc, k_u, k_v, h_u, h_v = faces(at, rows(min(t + 1, TILES - 1)))
        for i, (count, h) in enumerate(((k_u, h_u), (k_v, h_v))):
            cof[i, at, :] = (DTB * DTB) * h
            cnt[i, at, :] = count
            ext[FX + i, at, :] = (DTB * DTB) * ext[FX + i, at, :]
            avg[i, at, :] = jnp.zeros((8, EC), F32)
        for f, count, scale in ((ETA, kc, 1.0), (TU, k_u, DTB), (TV, k_v, DTB)):
            ext[f, at, :] = jnp.where(count > ZERO, scale * ext[f, at, :], ZERO)

    norm = 6.0 / (NSUB * (NSUB + 1) * (NSUB + 2)) / DTB

    def subcycle(n, lo, hi):
        tide_x, tide_y = tide[0, n], tide[1, n]
        weight = norm * ((n + 1) * (NSUB - n)).astype(F32)
        v_prev = ext[TV, rows(max(lo - 1, 0)), :]
        eta_prev = None
        u_keep = v_keep = None
        for t in range(lo, hi + 1):
            if t < hi:
                at = rows(t)
                u, v = ext[TU, at, :], ext[TV, at, :]
                eta = ext[ETA, at, :] - ((u - west(u)) + (v - south(v, v_prev)))
                ext[ETA, at, :] = eta
            if t > lo:
                b = rows(t - 1)
                slope_x = east(eta_prev) - eta_prev
                slope_y = north(eta_prev, eta) - eta_prev
                u_new = u_keep + (cof[0, b, :] * (tide_x - slope_x) + ext[FX, b, :])
                v_new = v_keep + (cof[1, b, :] * (tide_y - slope_y) + ext[FY, b, :])
                ext[TU, b, :] = u_new
                ext[TV, b, :] = v_new
                if 2 <= t - 1 < 19:
                    avg[0, b, :] = avg[0, b, :] + weight * u_new
                    avg[1, b, :] = avg[1, b, :] + weight * v_new
            eta_prev, u_keep, v_keep, v_prev = eta, u, v, v

    tiles = TILES
    loop(0, 4, functools.partial(subcycle, lo=0, hi=tiles))
    loop(4, 12, functools.partial(subcycle, lo=1, hi=tiles - 1))
    loop(12, NSUB, functools.partial(subcycle, lo=2, hi=tiles - 2))

    for r in range(STRIPS):
        at = rows(r, HR)
        for f in (TU, TV):
            ext[f, at, :] = (1.0 / DTB) * ext[f, at, :]
    planes = [
        pltpu.make_async_copy(ext.at[2 + i, pl.ds(HR, NR), pl.ds(0, NC)], o, outs_sem.at[i])
        for i, o in enumerate((eta_o, tu_o, tv_o))
    ]
    for c in planes:
        c.start()
    late.wait()
    for c in small:
        c.wait()
    for c in big:
        c.wait()
    for k in range(NL):
        vb[k, 7:8, :] = grv[k : k + 1, :]
        for i, ref in enumerate((tb, sb)):
            ref[k, 7:8, :] = grts[24 * i + k : 24 * i + k + 1, :]
            ref[k, NR + 8 : NR + 9, :] = grtn[24 * i + k : 24 * i + k + 1, :]

    for r in range(-1, STRIPS):
        at = rows(r, HR)
        for i, f in enumerate((SU, SV)):
            h = cof[i, at, :]
            avg[i, at, :] = (DTB * DTB) * (avg[i, at, :] - ext[f, at, :]) / jnp.where(h > ZERO, h, 1.0)

    def strip(r):
        at = rows(r, HR)
        return [x[at, BODY] for x in (ext.at[KMT], cnt.at[0], cnt.at[1], avg.at[0], avg.at[1])]

    def flux_y(r, k, k_v, d_v):
        vc = jnp.where(k_v > k, vb[k, rows(r, 8), :] + d_v, ZERO)
        out = [vc]
        for ref in (tb, sb):
            here = ref[k, rows(r, 8), :]
            out.append(here)
            out.append(vc * (here + north(here, ref[k, rows(r, 16), :])))
        return out

    _, _, k_v, _, d_v = strip(-1)
    for k in range(NL):
        _, _, a, _, b = flux_y(-1, k, k_v, d_v)
        fpt[k] = a
        fps[k] = b

    _, in_first, level = packed_lanes()
    for r in range(STRIPS):
        at = rows(r, HR)
        count, add = (jnp.broadcast_to(x[0, at, EC - 1 : EC], (8, 128)) for x in (cnt, avg))
        uc = jnp.where(count > level, gu[rows(r), :] + add, ZERO)
        uc = jnp.where(in_first, uc, turn(uc, 40))
        g = gts[rows(r), :]
        pkt[rows(r), :] = even_odd(turn(uc * (g + turn(sts[rows(r), :], -1)), 1), turn(g, -1))

    def advect(r):
        kc, k_u, k_v, d_u, d_v = strip(r)
        edges = pkt[rows(r), :]
        for k in range(NL):
            vc, t, y_t, s, y_s = flux_y(r, k, k_v, d_v)
            vb[k, rows(r, 8), :] = vc
            uc = jnp.where(k_u > k, ub[k, rows(r), :] + d_u, ZERO)
            ub[k, rows(r), :] = uc
            for slot, (ref, edge, prev, keep, x, y) in enumerate(((tb, tg, fpt, fxt, t, y_t), (sb, sg, fps, fxs, s, y_s))):
                ghost = unpack(edges, slot, k)
                edge[k] = ghost
                fx = uc * (x + east_of(x, ghost))
                keep[k] = fx
                ref[k, rows(r, 8), :] = x - HALF_DT * (fx + (y - south(y, prev[k])))
                prev[k] = y
        for k in range(NL):
            for ref, edge, keep in ((tb, tg, fxt), (sb, sg, fxs)):
                x = ref[k, rows(r, 8), :] + HALF_DT * west_of(keep[k], edge[k])
                ref[k, rows(r, 8), :] = jnp.where(kc > k, x, ZERO)

    def out_copy(i, c):
        src = (ub, vb, tb, sb)[i]
        dst = (u_o, v_o, t_o, s_o)[i]
        at = pl.ds(pl.multiple_of(c * CH, CH), CH)
        frm = pl.ds(pl.multiple_of(c * CH + (8 if i else 0), 8), CH)
        return pltpu.make_async_copy(src.at[:, frm, :], dst.at[:, at, :], out_sem.at[i, c])

    def advect_chunk(c):
        advect(c)
        for i in range(4):
            out_copy(i, c).start()

    loop(0, NCH, advect_chunk)

    def drain(c):
        for i in range(4):
            out_copy(i, c).wait()

    loop(0, NCH, drain)
    for c in planes:
        c.wait()


def vmem(*shape):
    return pltpu.VMEM(shape, F32)


def solution(mesh):
    any_spec = pl.BlockSpec(memory_space=pl.ANY)
    cube = jax.ShapeDtypeStruct((NL, NR, NC), F32)
    plane = jax.ShapeDtypeStruct((NR, NC), F32)

    tile, ghost, strip = vmem(NR, 128), vmem(ER, 128), vmem(NL, 8, NC)

    def arr(*shape):
        return jax.ShapeDtypeStruct(shape, F32)

    def local_step(vel_u, vel_v, temperature, salinity, sea_level, trans_u, trans_v, bathymetry, kmt_levels, tide_force):
        mid = pl.pallas_call(
            predict_kernel,
            name="predict",
            out_shape=(
                cube, cube, cube, cube, arr(9, ER, EC), arr(NR, 128), arr(NR, 128), arr(48, NC), arr(48, NC), arr(24, NC),
                arr(NR, 128),
            ),
            in_specs=[any_spec] * 9,
            out_specs=(any_spec,) * 11,
            scratch_shapes=[
                *([vmem(NL, NR + 16, NC)] * 3), *([vmem(NL, NR, NC)] * 4),
                vmem(9, ER, EC), pltpu.VMEM((NR, NC), jnp.int32), vmem(NR, NC),
                *([tile] * 3), *([ghost] * 3), vmem(NR + 8, 128), tile, strip, *([vmem(NR + 16, 128)] * 2),
                vmem(48, NC), vmem(72, NC), vmem(48, NC), vmem(72, NC),
                tile, vmem(48, NC), vmem(48, NC), tile, vmem(24, NC), *([strip] * 3), vmem(4, NR + 16, NC), *([vmem(NR + 16, 128)] * 2), vmem(2, NR, NC), strip, strip,
                pltpu.SemaphoreType.DMA((4, NCH)), pltpu.SemaphoreType.DMA((5,)), pltpu.SemaphoreType.DMA((4, NCH)),
                pltpu.SemaphoreType.DMA((3,)), pltpu.SemaphoreType.DMA((26,)), pltpu.SemaphoreType.DMA((26,)),
            ],
            compiler_params=pltpu.CompilerParams(collective_id=0, has_side_effects=True, vmem_limit_bytes=63 * 2**20),
        )(vel_u, vel_v, temperature, salinity, sea_level, trans_u, trans_v, bathymetry, kmt_levels)
        return pl.pallas_call(
            finish_kernel,
            name="finish",
            out_shape=(plane, plane, plane, cube, cube, cube, cube),
            in_specs=[pl.BlockSpec(memory_space=pltpu.SMEM)] + [any_spec] * 11,
            out_specs=(any_spec,) * 7,
            scratch_shapes=[
                vmem(NL, NR, NC), vmem(NL, NR + 8, NC), vmem(NL, NR + 16, NC), vmem(NL, NR + 16, NC),
                vmem(9, ER, EC), *([vmem(2, ER, EC)] * 3),
                vmem(NR, 128), vmem(NR, 128), vmem(48, NC), vmem(48, NC), vmem(24, NC), tile, *([strip] * 4), tile, *([vmem(NL, 8, 128)] * 2),
                pltpu.SemaphoreType.DMA((4,)), pltpu.SemaphoreType.DMA((8,)), pltpu.SemaphoreType.DMA((4, NCH)),
                pltpu.SemaphoreType.DMA((3,)),
            ],
            compiler_params=pltpu.CompilerParams(
                vmem_limit_bytes=60 * 2**20
            ),
        )(tide_force.T, *mid)

    spec_cube = P(None, "row", "col")
    spec_plane = P("row", "col")
    return jax.shard_map(
        local_step,
        mesh=mesh,
        in_specs=(spec_cube,) * 4 + (spec_plane,) * 5 + (P(None, None),),
        out_specs=(spec_plane,) * 3 + (spec_cube,) * 4,
        check_vma=False,
    )
```

```python
import functools

import jax
import jax.numpy as jnp
from jax import lax
from jax.experimental import pallas as pl
from jax.experimental.pallas import tpu as pltpu
from jax.sharding import PartitionSpec as P

TIME_STEP = 4.0
ALPHA_T = 0.02
BETA_S = 0.015
VISC_KV = 0.001
DIFF_KT = 0.0005

NL = 20
NSUB = 20
NR, NC = 128, 512
HR = 24
ER, EC = NR + 2 * HR, NC + 128
NCH = 16
CH = NR // NCH
STRIPS, TILES = NR // 8, ER // 8
PAIR, TRIPLE = 2, 3
NORTH = 2 * PAIR
EARLY = 0
DTB = TIME_STEP / NSUB
HALF_DT = 0.5 * TIME_STEP
F32 = jnp.float32
ZERO = 0.0
BODY = slice(0, NC)
LEFT = slice(0, 128)
RIGHT = slice(NC - 128, NC)
GHOST = slice(NC, EC)
KMT, DZ, ETA, TU, TV, FX, FY, SV, SU = range(9)
KU, KV, DU, DV = range(4)
WIDE = 42
MESH = pl.DeviceIdType.MESH


def loop(lo, hi, body, per=1):
    def step(i, carry):
        for j in range(per):
            body(lo + per * i + j)
        return carry

    lax.fori_loop(0, (hi - lo) // per, step, 0)


def rows(r, off=0):
    start = 8 * r + off
    if isinstance(start, int):
        return pl.ds(start, 8)
    return pl.ds(pl.multiple_of(start, 8), 8)


def iota(shape, axis):
    return lax.broadcasted_iota(jnp.int32, shape, axis)


def east(x):
    return pltpu.roll(x, x.shape[1] - 1, 1)


def west(x):
    return pltpu.roll(x, 1, 1)


def north(here, above):
    return pltpu.roll(jnp.where(iota(here.shape, 0) == 0, above, here), 7, 0)


def south(here, below):
    return pltpu.roll(jnp.where(iota(here.shape, 0) == 7, below, here), 1, 0)


def lane_tiles(x):
    return [x[:, 128 * c : 128 * (c + 1)] for c in range(NC // 128)]


def east_of(x, ghost):
    moved = [pltpu.roll(t, 127, 1) for t in lane_tiles(x)] + [ghost]
    last = iota((8, 128), 1) == 127
    return jnp.concatenate([jnp.where(last, b, a) for a, b in zip(moved, moved[1:])], 1)


def west_of(x, ghost):
    moved = [ghost] + [pltpu.roll(t, 1, 1) for t in lane_tiles(x)]
    first = iota((8, 128), 1) == 0
    return jnp.concatenate([jnp.where(first, a, b) for a, b in zip(moved, moved[1:])], 1)


def turn(x, by):
    return pltpu.roll(x, by % 128, 1)


def even_odd(a, b):
    return jnp.where(iota((8, 128), 1) % 2 == 0, a, b)


def lane_of(slot, k):
    return 2 * k + 40 * slot


def unpack(ghost, slot, k):
    shift = (128 - lane_of(slot, k)) % 128
    return pltpu.roll(ghost, shift, 1) if shift else ghost


def pack(tiles):
    lane = iota((8, 128), 1)
    acc = None
    first = None
    for slot, k, low, high in tiles:
        both = jnp.where(lane == 127, high, low)
        at = lane_of(slot, k)
        moved = pltpu.roll(both, at, 1) if at else both
        if acc is None:
            acc = moved
            if at == 0:
                first = moved
        else:
            acc = jnp.where(lane >= at - 1, moved, acc)
    if first is not None:
        acc = jnp.where(lane == 127, first, acc)
    return acc


def pack_wide(planes):
    lane = iota((8, 128), 1)
    acc = None
    for q, x in enumerate(planes):
        edge = jnp.where(lane < 64, x[:, LEFT], x[:, RIGHT])
        if acc is None:
            acc = edge
        else:
            acc = jnp.where(lane >= WIDE * q - WIDE // 2, pltpu.roll(edge, WIDE * q, 1), acc)
    if len(planes) == 1:
        return acc
    first = jnp.where(lane < 64, planes[0][:, LEFT], planes[0][:, RIGHT])
    return jnp.where(lane >= 128 - WIDE // 2, first, acc)


def unpack_wide(tile, q):
    lane = iota(tile.shape, 1)
    moved = pltpu.roll(tile, 128 - WIDE * q, 1) if q else tile
    return jnp.where((lane < WIDE // 2) | (lane >= 128 - WIDE // 2), moved, ZERO)


def packed_lanes():
    lane = iota((8, 128), 1)
    in_first = (lane < 39) | (lane == 127)
    return lane, in_first, jnp.where(lane == 127, ZERO, (((lane + 1) % 40) // 2).astype(F32))


def solve(refs, masked, count, coef, gains, at):
    low = None
    rest = 1.0
    parts = [None] * len(refs)
    for k in range(NL):
        up = jnp.where(count > k + 1.0, coef, ZERO) if k < NL - 1 else ZERO
        inv = 1.0 / (rest + up)
        for i, ref in enumerate(refs):
            src = ref[k, at, :]
            if not masked:
                src = jnp.where(count > k, src, ZERO)
            parts[i] = src * inv if k == 0 else (src + low * parts[i]) * inv
            if k < NL - 1:
                ref[k, at, :] = parts[i]
        if k < NL - 1:
            gain = up * inv
            gains[k] = gain
            rest = 1.0 + gain * rest
        low = up
    for i, ref in enumerate(refs):
        ref[NL - 1, at, :] = parts[i]
    for k in range(NL - 2, -1, -1):
        gain = gains[k]
        for i, ref in enumerate(refs):
            parts[i] = ref[k, at, :] + gain * parts[i]
            ref[k, at, :] = parts[i]


def predict_kernel(
    u_h, v_h, t_h, s_h, eta_h, tu_h, tv_h, dep_h, kmt_h,
    su_o, sv_o, tm_o, sm_o, ext_o, gts_o, gu_o, grts_o, grtn_o, grv_o, sts_o,
    ub, vb, pb, tb, sb, su, sv, ext, ktmp, htmp, pa, pb_, pc, ga, gb, gc, pka, pkb, dup, sp, gx, prn, prs, grs, grn, sts, trn, trs, sug, vrn, fp, fsp, csp, geo, wet_g, wet_o, tot, gains, gains2,
    load_sem, small_sem, out_sem, outs_sem, send_sem, recv_sem,
):
    col = lax.axis_index("col")
    row = lax.axis_index("row")
    n_row = 8
    side = 1 - col
    up_row = lax.rem(row + 1, n_row)
    down_row = lax.rem(row + n_row - 1, n_row)
    to_x = {"col": side, "row": row}
    to_n = {"col": col, "row": up_row}
    to_s = {"col": col, "row": down_row}
    to_dn = {"col": side, "row": up_row}
    to_ds = {"col": side, "row": down_row}

    barrier = pltpu.get_barrier_semaphore()
    for dev in (to_x, to_n, to_s, to_dn, to_ds):
        pl.semaphore_signal(barrier, inc=1, device_id=dev, device_id_type=MESH)

    small = [
        pltpu.make_async_copy(kmt_h, ktmp, small_sem.at[0]),
        pltpu.make_async_copy(dep_h, htmp, small_sem.at[1]),
        pltpu.make_async_copy(eta_h, ext.at[2, pl.ds(HR, NR), pl.ds(0, NC)], small_sem.at[2]),
        pltpu.make_async_copy(tu_h, ext.at[3, pl.ds(HR, NR), pl.ds(0, NC)], small_sem.at[3]),
        pltpu.make_async_copy(tv_h, ext.at[4, pl.ds(HR, NR), pl.ds(0, NC)], small_sem.at[4]),
    ]
    for c in small:
        c.start()

    def load(i, c):
        src = (t_h, s_h, u_h, v_h)[i]
        dst = (tb, sb, ub, vb)[i]
        at = pl.ds(pl.multiple_of(c * CH, CH), CH)
        to = pl.ds(pl.multiple_of(c * CH + (8 if i >= 2 else 0), 8), CH)
        return pltpu.make_async_copy(src.at[:, at, :], dst.at[:, to, :], load_sem.at[i, c])

    def start_loads(pair):
        def body(c):
            for i in pair:
                load(i, c).start()

        loop(0, NCH, body)

    start_loads((0, 1))
    start_loads((2, 3))

    def send(src, dst, idx, dev):
        c = remote(src, dst, idx, dev)
        c.start()
        return c

    def remote(src, dst, idx, dev):
        return pltpu.make_async_remote_copy(
            src_ref=src, dst_ref=dst, send_sem=send_sem.at[idx], recv_sem=recv_sem.at[idx], device_id=dev, device_id_type=MESH
        )

    lane, in_first, level = packed_lanes()
    for c in small:
        c.wait()
    for r in range(STRIPS):
        kf = ktmp[rows(r), :].astype(F32)
        dz = htmp[rows(r), :] / jnp.maximum(kf, 1.0)
        ext[KMT, rows(r, HR), BODY] = kf
        ext[DZ, rows(r, HR), BODY] = dz
        eta, tu, tv = (ext[f, rows(r, HR), BODY] for f in (ETA, TU, TV))
        pa[rows(r), :] = pack_wide((kf, dz, eta))
        pb_[rows(r), :] = pack_wide((tu, tv))
    pl.semaphore_wait(barrier, 5)

    def start(copies):
        for c in copies:
            c.start()

    def send_ext(lo, n, tile, ghost, base):
        at = pl.ds(lo, n)
        low, high, mid = pl.ds(0, HR), pl.ds(HR + NR, HR), pl.ds(HR, NR)
        body = pl.ds(0, NC)
        parts = (
            (ext.at[at, pl.ds(NR, HR), body], ext.at[at, low, body], to_n),
            (tile.at[pl.ds(NR - HR, HR), :], ghost.at[low, :], to_dn),
            (tile, ghost.at[mid, :], to_x),
            (ext.at[at, pl.ds(HR, HR), body], ext.at[at, high, body], to_s),
            (tile.at[low, :], ghost.at[high, :], to_ds),
        )
        return [remote(a, b, base + i, dev) for i, (a, b, dev) in enumerate(parts)]

    def receive_ext(copies, ghost, fields):
        for c in copies:
            c.wait()

        for q, f in enumerate(fields):
            ext[f, :, GHOST] = unpack_wide(ghost[...], q)

    first = send_ext(KMT, 3, pa, ga, 0)
    start(first)

    def pressure(r):
        kc = ext[KMT, rows(r, HR), BODY]
        dz = ext[DZ, rows(r, HR), BODY]
        total = jnp.zeros((8, NC), F32)
        scale = TIME_STEP * dz
        for k in range(NL):
            half = (0.5 * BETA_S) * (sb[k, rows(r), :] - 1.0) - (0.5 * ALPHA_T) * (tb[k, rows(r), :] - 1.0)
            half = jnp.where(kc > k, half, ZERO)
            middle = total + half
            total = middle + half
            pb[k, rows(r, 8), :] = scale * middle

    def pressure_chunk(c):
        load(0, c).wait()
        load(1, c).wait()
        pressure(c)


    def out_copy(i, c):
        src = (tb, sb, su, sv)[i]
        dst = (tm_o, sm_o, su_o, sv_o)[i]
        at = pl.ds(pl.multiple_of(c * CH, CH), CH)
        return pltpu.make_async_copy(src.at[:, at, :], dst.at[:, at, :], out_sem.at[i, c])

    def pack_ts(r):
        tiles = []
        for slot, ref in enumerate((tb, sb)):
            for k in range(NL):
                tiles.append((slot, k, ref[k, rows(r), LEFT], ref[k, rows(r), RIGHT]))
        sts[rows(r), :] = pack(tiles)

    def mix(r):
        pack_ts(jnp.maximum(r - 1, 0))
        kc = ext[KMT, rows(r, HR), BODY]
        dz = ext[DZ, rows(r, HR), BODY]
        solve((tb, sb), False, kc, (TIME_STEP * DIFF_KT) / (dz * dz), gains, rows(r))

    def mix_chunk(c):
        mix(c)
        out_copy(0, c).start()
        out_copy(1, c).start()

    loop(EARLY, NCH, pressure_chunk, PAIR)

    def pack_uvp(r):
        tiles = []
        for slot, ref in enumerate((ub, vb, pb)):
            for k in range(NL):
                x = [ref[k, rows(r, 8), LEFT], ref[k, rows(r, 8), RIGHT]]
                tiles.append((slot, k, *x))
        sp[rows(r, 8), :] = pack(tiles)

    def pack_chunk(c):
        load(2, c).wait()
        load(3, c).wait()
        pack_uvp(c)

    loop(0, NCH, pack_chunk, PAIR)

    def edge_row(dst, i, k, ref, at):
        dst[24 * i + k : 24 * i + k + 1, :] = ref[k, at : at + 1, :]

    def ghost_row(ref, k, at, src, i):
        x = src[24 * i + k : 24 * i + k + 1, :]
        ref[k, at : at + 1, :] = jnp.where(geo[i, at : at + 1, :] > k, x, ZERO) if i < 2 else x

    for k in range(NL):
        for i, ref in enumerate((ub, vb, pb)):
            edge_row(prs, i, k, ref, 8)
            if i < 2:
                edge_row(prn, i, k, ref, NR + 7)
    low, high = pl.ds(8, 8), pl.ds(NR, 8)
    second = [
        send(sp.at[pl.ds(8, NR), :], gx.at[pl.ds(8, NR), :], 10, to_x),
        send(prn, grs, 11, to_n),
        send(prs, grn, 12, to_s),
        send(sp.at[high, :], gx.at[pl.ds(0, 8), :], 13, to_dn),
        send(sp.at[low, :], gx.at[pl.ds(NR + 8, 8), :], 14, to_ds),
        send(sp.at[high, :], sp.at[pl.ds(0, 8), :], 25, to_n),
    ]

    later = send_ext(TU, 2, pb_, gb, 5)
    start(later)

    loop(EARLY, NCH, mix_chunk, PAIR)
    pack_ts(STRIPS - 1)
    for k in range(NL):
        for i, ref in enumerate((tb, sb)):
            edge_row(trs, i, k, ref, 0)
            edge_row(trn, i, k, ref, NR - 1)
    third = [send(sts, gts_o, 15, to_x), send(trn, grts_o, 16, to_n), send(trs, grtn_o, 17, to_s)]

    receive_ext(first, ga, (KMT, DZ, ETA))
    has_south = (row > 0).astype(F32)
    has_north = (row < n_row - 1).astype(F32)
    ext[KMT, 0:HR, :] = ext[KMT, 0:HR, :] * has_south
    ext[KMT, HR + NR :, :] = ext[KMT, HR + NR :, :] * has_north

    for r in range(-1, STRIPS + 1):
        at, above = rows(r, HR), rows(r, HR + 8)
        kc, dz = ext[KMT, at, :], ext[DZ, at, :]
        k_u = jnp.minimum(kc, east(kc))
        k_v = jnp.minimum(kc, north(kc, ext[KMT, above, :]))
        geo[KU, rows(r, 8), :] = k_u[:, BODY]
        geo[KV, rows(r, 8), :] = k_v[:, BODY]
        geo[DU, rows(r, 8), :] = 0.5 * (dz + east(dz))[:, BODY]
        geo[DV, rows(r, 8), :] = 0.5 * (dz + north(dz, ext[DZ, above, :]))[:, BODY]
        (u_w, u_e, u_l), (v_w, v_e, v_f) = (
            [jnp.broadcast_to(x[:, i : i + 1], (8, 128)) for i in at]
            for x, at in ((k_u, (EC - 1, NC, NC - 1)), (k_v, (EC - 1, NC, 0)))
        )
        top = jnp.where(lane < 2 * 40 - 1, even_odd(v_e, v_w), 1.0 * NL)
        wet_g[rows(r, 8), :] = jnp.where(in_first, even_odd(u_e, u_w), top)
        wet_o[rows(r, 8), :] = jnp.where(in_first, u_l, v_f)

    def mask(r):
        for slot, ref in enumerate((ub, vb)):
            count = geo[slot, rows(r, 8), :]
            total = jnp.zeros((8, NC), F32)
            for k in range(NL):
                x = jnp.where(count > k, ref[k, rows(r, 8), :], ZERO)
                ref[k, rows(r, 8), :] = x
                total = total + x
            tot[slot, rows(r), :] = total

    loop(0, STRIPS, mask, PAIR)
    for c in second:
        c.wait()

    def wet(x, count, t):
        return jnp.where(count[rows(t), :] > level, x[rows(t), :], ZERO)

    corner_w = None
    for t in range(STRIPS + 1, 0, -1):
        g, own, below = wet(gx, wet_g, t), wet(sp, wet_o, t), t - 1
        g_s, own_s = south(g, wet(gx, wet_g, below)), south(own, wet(sp, wet_o, below))
        pka[rows(t - 1), :] = even_odd(turn(g, 1), turn(g_s, -41))
        flux = (turn(g_s, -39) + turn(own_s, -40)) * turn(g_s + g, 1)
        if corner_w is not None:
            d = own + turn(g, -1)
            pkb[rows(t - 1), :] = even_odd(north(flux, corner_w), d * d + turn(g, -81))
        corner_w = flux

    for k in range(NL):
        for i, ref in enumerate((ub, vb)):
            ghost_row(ref, k, 7, grs, i)
        for i, ref in enumerate((ub, vb, pb)):
            ghost_row(ref, k, NR + 8, grn, i)

    def corner(r, k, ghost):
        u, v, p = (ref[k, rows(r, 8), :] for ref in (ub, vb, pb))
        u_s = south(u, ub[k, rows(r), :])
        v_s = south(v, vb[k, rows(r), :])
        f_s = (v_s + east_of(v_s, ghost)) * (u_s + u)
        c = v + v_s
        return u, p, f_s, c * c + p

    for k in range(NL):
        fsp[k], csp[k] = corner(STRIPS, k, unpack(pka[NR : NR + 8, :], 0, k))[2:]

    def tendency(i):
        r = STRIPS - 1 - i
        at = rows(r)
        near, far = pka[at, :], pkb[at, :]
        for k in range(NL):
            ghost = unpack(near, 0, k)
            u, p, f_s, c = corner(r, k, ghost)
            f = north(f_s, fsp[k])
            c_n = north(c, csp[k])
            fsp[k], csp[k] = f_s, c
            d = u + west_of(u, ghost)
            d = d * d + p
            fp[k], dup[k] = f, d
            su[k, at, :] = (f_s - f) + d
            sv[k, at, :] = (c - c_n) - f
        k_u, k_v, dz_u, dz_v = (geo[i, rows(r, 8), :] for i in (KU, KV, DU, DV))
        sum_u = sum_v = jnp.zeros((8, NC), F32)
        for k in range(NL):
            ghost = unpack(far, 0, k)
            t_u = su[k, at, :] - east_of(dup[k], ghost)
            t_v = sv[k, at, :] + west_of(fp[k], ghost)
            u = jnp.where(k_u > k, ub[k, rows(r, 8), :] + t_u, ZERO)
            v = jnp.where(k_v > k, vb[k, rows(r, 8), :] + t_v, ZERO)
            su[k, at, :], sv[k, at, :] = u, v
            sum_u, sum_v = sum_u + u, sum_v + v
        ext[FX, rows(r, HR), BODY] = (dz_u / TIME_STEP) * (sum_u - tot[KU, at, :])
        ext[FY, rows(r, HR), BODY] = (dz_v / TIME_STEP) * (sum_v - tot[KV, at, :])
        ext[SU, rows(r, HR), BODY] = dz_u * sum_u
        ext[SV, rows(r, HR), BODY] = dz_v * sum_v

    def pack_forcing(lo, hi):
        for r in range(lo, hi):
            pc[rows(r), :] = pack_wide([ext[f, rows(r, HR), BODY] for f in (FX, FY, SU)])

    fourth = send_ext(FX, 3, pc, gc, 18)

    def leave_north():
        pack_forcing(STRIPS - NORTH, STRIPS)
        start(fourth[:2])

    def tendency_pair(i):
        for j in range(PAIR):
            tendency(PAIR * i + j)
        pl.when(i == NORTH // PAIR - 1)(leave_north)

    loop(0, STRIPS // PAIR, tendency_pair)
    pack_forcing(0, STRIPS - NORTH)
    start(fourth[2:])
    receive_ext(later, gb, (TU, TV))
    out_ext0 = pltpu.make_async_copy(ext.at[pl.ds(0, 5)], ext_o.at[pl.ds(0, 5)], outs_sem.at[0])
    out_ext0.start()

    def implicit(i, ref, keep, r):
        dz = geo[DU + i, rows(r, 8), :]
        solve((ref,), True, geo[i, rows(r, 8), :], (TIME_STEP * VISC_KV) / (dz * dz), keep, rows(r))

    def pack_su(r):
        sug[rows(r), :] = pack([(0, k, su[k, rows(r), LEFT], su[k, rows(r), RIGHT]) for k in range(NL)])

    def solve_u(r):
        pack_su(jnp.maximum(r - 1, 0))
        implicit(0, su, gains, r)

    def solve_v(r):
        implicit(1, sv, gains2, r)

    def u_chunk(c):
        solve_u(c)
        out_copy(2, c).start()

    def v_chunk(c):
        solve_v(c)
        out_copy(3, c).start()

    v_chunk(NCH - 1)
    loop(0, NCH, u_chunk, PAIR)
    pack_su(STRIPS - 1)
    for k in range(NL):
        edge_row(vrn, 0, k, sv, NR - 1)
    fifth = [send(sug, gu_o, 23, to_x), send(vrn, grv_o, 24, to_n)]
    out_ext1 = pltpu.make_async_copy(ext.at[pl.ds(5, 4)], ext_o.at[pl.ds(5, 4)], outs_sem.at[1])

    def take_forcing():
        receive_ext(fourth, gc, (FX, FY, SU))
        out_ext1.start()

    def v_triple(i):
        for j in range(TRIPLE):
            v_chunk(TRIPLE * i + j)
        pl.when(i == TRIPLE - 1)(take_forcing)

    loop(0, STRIPS // TRIPLE, v_triple)
    out_sts = pltpu.make_async_copy(sts, sts_o, outs_sem.at[2])
    out_sts.start()

    def drain(c):
        for i in range(4):
            out_copy(i, c).wait()

    loop(0, NCH, drain)
    for c in third:
        c.wait()
    for c in fifth:
        c.wait()
    out_ext0.wait()
    out_ext1.wait()
    out_sts.wait()


def finish_kernel(
    tide, su_h, sv_h, tm_h, sm_h, ext_h, gts_h, gu_h, grts_h, grtn_h, grv_h, sts_h,
    eta_o, tu_o, tv_o, u_o, v_o, t_o, s_o,
    ub, vb, tb, sb, ext, cof, cnt, avg, gts, gu, grts, grtn, grv, sts, fpt, fps, fxt, fxs, pkt, tg, sg,
    load_sem, small_sem, out_sem, outs_sem,
):
    early, late = (
        pltpu.make_async_copy(ext_h.at[at], ext.at[at], small_sem.at[i])
        for i, at in enumerate((pl.ds(KMT, SV), pl.ds(SV, 2)))
    )
    early.start()
    small = [
        pltpu.make_async_copy(a, b, small_sem.at[i + 2])
        for i, (a, b) in enumerate(((gts_h, gts), (gu_h, gu), (grts_h, grts), (grtn_h, grtn), (grv_h, grv), (sts_h, sts)))
    ]
    late.start()
    for c in small:
        c.start()
    big = [
        pltpu.make_async_copy(su_h, ub, load_sem.at[0]),
        pltpu.make_async_copy(sv_h, vb.at[:, pl.ds(8, NR), :], load_sem.at[1]),
        pltpu.make_async_copy(tm_h, tb.at[:, pl.ds(8, NR), :], load_sem.at[2]),
        pltpu.make_async_copy(sm_h, sb.at[:, pl.ds(8, NR), :], load_sem.at[3]),
    ]
    for c in big:
        c.start()
    early.wait()

    def faces(at, above):
        kc, kn = ext[KMT, at, :], ext[KMT, above, :]
        dz, dn = ext[DZ, at, :], ext[DZ, above, :]
        k_u = jnp.minimum(kc, east(kc))
        k_v = jnp.minimum(kc, north(kc, kn))
        return kc, k_u, k_v, k_u * (0.5 * (dz + east(dz))), k_v * (0.5 * (dz + north(dz, dn)))

    for t in range(TILES):
        at = rows(t)
        kc, k_u, k_v, h_u, h_v = faces(at, rows(min(t + 1, TILES - 1)))
        for i, (count, h) in enumerate(((k_u, h_u), (k_v, h_v))):
            cof[i, at, :] = (DTB * DTB) * h
            cnt[i, at, :] = count
            ext[FX + i, at, :] = (DTB * DTB) * ext[FX + i, at, :]
            avg[i, at, :] = jnp.zeros((8, EC), F32)
        for f, count, scale in ((ETA, kc, 1.0), (TU, k_u, DTB), (TV, k_v, DTB)):
            ext[f, at, :] = jnp.where(count > ZERO, scale * ext[f, at, :], ZERO)

    norm = 6.0 / (NSUB * (NSUB + 1) * (NSUB + 2)) / DTB

    def subcycle(n, lo, hi):
        tide_x, tide_y = tide[0, n], tide[1, n]
        weight = norm * ((n + 1) * (NSUB - n)).astype(F32)
        v_prev = ext[TV, rows(max(lo - 1, 0)), :]
        eta_prev = None
        u_keep = v_keep = None
        for t in range(lo, hi + 1):
            if t < hi:
                at = rows(t)
                u, v = ext[TU, at, :], ext[TV, at, :]
                eta = ext[ETA, at, :] - ((u - west(u)) + (v - south(v, v_prev)))
                ext[ETA, at, :] = eta
            if t > lo:
                b = rows(t - 1)
                slope_x = east(eta_prev) - eta_prev
                slope_y = north(eta_prev, eta) - eta_prev
                u_new = u_keep + (cof[0, b, :] * (tide_x - slope_x) + ext[FX, b, :])
                v_new = v_keep + (cof[1, b, :] * (tide_y - slope_y) + ext[FY, b, :])
                ext[TU, b, :] = u_new
                ext[TV, b, :] = v_new
                if 2 <= t - 1 < 19:
                    avg[0, b, :] = avg[0, b, :] + weight * u_new
                    avg[1, b, :] = avg[1, b, :] + weight * v_new
            eta_prev, u_keep, v_keep, v_prev = eta, u, v, v

    tiles = TILES
    loop(0, 4, functools.partial(subcycle, lo=0, hi=tiles))
    loop(4, 12, functools.partial(subcycle, lo=1, hi=tiles - 1))
    loop(12, NSUB, functools.partial(subcycle, lo=2, hi=tiles - 2))

    for r in range(STRIPS):
        at = rows(r, HR)
        for f in (TU, TV):
            ext[f, at, :] = (1.0 / DTB) * ext[f, at, :]
    planes = [
        pltpu.make_async_copy(ext.at[2 + i, pl.ds(HR, NR), pl.ds(0, NC)], o, outs_sem.at[i])
        for i, o in enumerate((eta_o, tu_o, tv_o))
    ]
    for c in planes:
        c.start()
    late.wait()
    for c in small:
        c.wait()
    for c in big:
        c.wait()
    for k in range(NL):
        vb[k, 7:8, :] = grv[k : k + 1, :]
        for i, ref in enumerate((tb, sb)):
            ref[k, 7:8, :] = grts[24 * i + k : 24 * i + k + 1, :]
            ref[k, NR + 8 : NR + 9, :] = grtn[24 * i + k : 24 * i + k + 1, :]

    for r in range(-1, STRIPS):
        at = rows(r, HR)
        for i, f in enumerate((SU, SV)):
            h = cof[i, at, :]
            avg[i, at, :] = (DTB * DTB) * (avg[i, at, :] - ext[f, at, :]) / jnp.where(h > ZERO, h, 1.0)

    def strip(r):
        at = rows(r, HR)
        return [x[at, BODY] for x in (ext.at[KMT], cnt.at[0], cnt.at[1], avg.at[0], avg.at[1])]

    def flux_y(r, k, k_v, d_v):
        vc = jnp.where(k_v > k, vb[k, rows(r, 8), :] + d_v, ZERO)
        out = [vc]
        for ref in (tb, sb):
            here = ref[k, rows(r, 8), :]
            out.append(here)
            out.append(vc * (here + north(here, ref[k, rows(r, 16), :])))
        return out

    _, _, k_v, _, d_v = strip(-1)
    for k in range(NL):
        _, _, a, _, b = flux_y(-1, k, k_v, d_v)
        fpt[k] = a
        fps[k] = b

    _, in_first, level = packed_lanes()
    for r in range(STRIPS):
        at = rows(r, HR)
        count, add = (jnp.broadcast_to(x[0, at, EC - 1 : EC], (8, 128)) for x in (cnt, avg))
        uc = jnp.where(count > level, gu[rows(r), :] + add, ZERO)
        uc = jnp.where(in_first, uc, turn(uc, 40))
        g = gts[rows(r), :]
        pkt[rows(r), :] = even_odd(turn(uc * (g + turn(sts[rows(r), :], -1)), 1), turn(g, -1))

    def advect(r):
        kc, k_u, k_v, d_u, d_v = strip(r)
        edges = pkt[rows(r), :]
        for k in range(NL):
            vc, t, y_t, s, y_s = flux_y(r, k, k_v, d_v)
            vb[k, rows(r, 8), :] = vc
            uc = jnp.where(k_u > k, ub[k, rows(r), :] + d_u, ZERO)
            ub[k, rows(r), :] = uc
            for slot, (ref, edge, prev, keep, x, y) in enumerate(((tb, tg, fpt, fxt, t, y_t), (sb, sg, fps, fxs, s, y_s))):
                ghost = unpack(edges, slot, k)
                edge[k] = ghost
                fx = uc * (x + east_of(x, ghost))
                keep[k] = fx
                ref[k, rows(r, 8), :] = x - HALF_DT * (fx + (y - south(y, prev[k])))
                prev[k] = y
        for k in range(NL):
            for ref, edge, keep in ((tb, tg, fxt), (sb, sg, fxs)):
                x = ref[k, rows(r, 8), :] + HALF_DT * west_of(keep[k], edge[k])
                ref[k, rows(r, 8), :] = jnp.where(kc > k, x, ZERO)

    def out_copy(i, c):
        src = (ub, vb, tb, sb)[i]
        dst = (u_o, v_o, t_o, s_o)[i]
        at = pl.ds(pl.multiple_of(c * CH, CH), CH)
        frm = pl.ds(pl.multiple_of(c * CH + (8 if i else 0), 8), CH)
        return pltpu.make_async_copy(src.at[:, frm, :], dst.at[:, at, :], out_sem.at[i, c])

    def advect_chunk(c):
        advect(c)
        for i in range(4):
            out_copy(i, c).start()

    loop(0, NCH, advect_chunk)

    def drain(c):
        for i in range(4):
            out_copy(i, c).wait()

    loop(0, NCH, drain)
    for c in planes:
        c.wait()


def vmem(*shape):
    return pltpu.VMEM(shape, F32)


def solution(mesh):
    any_spec = pl.BlockSpec(memory_space=pl.ANY)
    cube = jax.ShapeDtypeStruct((NL, NR, NC), F32)
    plane = jax.ShapeDtypeStruct((NR, NC), F32)

    tile, ghost, strip = vmem(NR, 128), vmem(ER, 128), vmem(NL, 8, NC)

    def arr(*shape):
        return jax.ShapeDtypeStruct(shape, F32)

    def local_step(vel_u, vel_v, temperature, salinity, sea_level, trans_u, trans_v, bathymetry, kmt_levels, tide_force):
        mid = pl.pallas_call(
            predict_kernel,
            name="predict",
            out_shape=(
                cube, cube, cube, cube, arr(9, ER, EC), arr(NR, 128), arr(NR, 128), arr(48, NC), arr(48, NC), arr(24, NC),
                arr(NR, 128),
            ),
            in_specs=[any_spec] * 9,
            out_specs=(any_spec,) * 11,
            scratch_shapes=[
                *([vmem(NL, NR + 16, NC)] * 3), *([vmem(NL, NR, NC)] * 4),
                vmem(9, ER, EC), pltpu.VMEM((NR, NC), jnp.int32), vmem(NR, NC),
                *([tile] * 3), *([ghost] * 3), vmem(NR + 8, 128), tile, strip, *([vmem(NR + 16, 128)] * 2),
                vmem(48, NC), vmem(72, NC), vmem(48, NC), vmem(72, NC),
                tile, vmem(48, NC), vmem(48, NC), tile, vmem(24, NC), *([strip] * 3), vmem(4, NR + 16, NC), *([vmem(NR + 16, 128)] * 2), vmem(2, NR, NC), strip, strip,
                pltpu.SemaphoreType.DMA((4, NCH)), pltpu.SemaphoreType.DMA((5,)), pltpu.SemaphoreType.DMA((4, NCH)),
                pltpu.SemaphoreType.DMA((3,)), pltpu.SemaphoreType.DMA((26,)), pltpu.SemaphoreType.DMA((26,)),
            ],
            compiler_params=pltpu.CompilerParams(collective_id=0, has_side_effects=True, vmem_limit_bytes=63 * 2**20),
        )(vel_u, vel_v, temperature, salinity, sea_level, trans_u, trans_v, bathymetry, kmt_levels)
        return pl.pallas_call(
            finish_kernel,
            name="finish",
            out_shape=(plane, plane, plane, cube, cube, cube, cube),
            in_specs=[pl.BlockSpec(memory_space=pltpu.SMEM)] + [any_spec] * 11,
            out_specs=(any_spec,) * 7,
            scratch_shapes=[
                vmem(NL, NR, NC), vmem(NL, NR + 8, NC), vmem(NL, NR + 16, NC), vmem(NL, NR + 16, NC),
                vmem(9, ER, EC), *([vmem(2, ER, EC)] * 3),
                vmem(NR, 128), vmem(NR, 128), vmem(48, NC), vmem(48, NC), vmem(24, NC), tile, *([strip] * 4), tile, *([vmem(NL, 8, 128)] * 2),
                pltpu.SemaphoreType.DMA((4,)), pltpu.SemaphoreType.DMA((8,)), pltpu.SemaphoreType.DMA((4, NCH)),
                pltpu.SemaphoreType.DMA((3,)),
            ],
            compiler_params=pltpu.CompilerParams(
                vmem_limit_bytes=60 * 2**20
            ),
        )(tide_force.T, *mid)

    spec_cube = P(None, "row", "col")
    spec_plane = P("row", "col")
    return jax.shard_map(
        local_step,
        mesh=mesh,
        in_specs=(spec_cube,) * 4 + (spec_plane,) * 5 + (P(None, None),),
        out_specs=(spec_plane,) * 3 + (spec_cube,) * 4,
        check_vma=False,
    )
```
